32 devices in a mesh: dp: 2 (over x), dm: 4 (over z), tp: 4 (over y, core).
Axes of the slice: x: 2, y: 2, z: 4, core: 2. Of those that a mesh axis runs over, the one named last changes fastest.
Arguments:
- hidden: bfloat16 [128, 5120], P('dp', 'dm'), parts along dimension 0
- w_q: bfloat16 [5120, 40, 128], P('dm', 'tp')
- w_k: bfloat16 [5120, 40, 128], P('dm', 'tp')
- w_v: bfloat16 [5120, 40, 128], P('dm', 'tp')
- w_o: bfloat16 [40, 128, 5120], P('tp', None, 'dm')
- w_gate: bfloat16 [5120, 13824], P('dm', 'tp')
- w_up: bfloat16 [5120, 13824], P('dm', 'tp')
- w_down: bfloat16 [13824, 5120], P('tp', 'dm')
- norm_attn: bfloat16 [5120], P('dm')
- norm_mlp: bfloat16 [5120], P('dm')
- k_cache: bfloat16 [128, 128, 40, 128], P(('dp', 'dm'), None, 'tp'), parts along dimension 0
- v_cache: bfloat16 [128, 128, 40, 128], P(('dp', 'dm'), None, 'tp'), parts along dimension 0
- seq_lens: int32 [128], P(('dp', 'dm')), parts along dimension 0
- rope_cos: float32 [128, 64], P(('dp', 'dm')), parts along dimension 0
- rope_sin: float32 [128, 64], P(('dp', 'dm')), parts along dimension 0
Outputs:
- output 1: bfloat16 [128, 5120], P('dp', 'dm'), parts along dimension 0
- output 2: bfloat16 [128, 128, 40, 128], P(('dp', 'dm'), None, 'tp'), parts along dimension 0
- output 3: bfloat16 [128, 128, 40, 128], P(('dp', 'dm'), None, 'tp'), parts along dimension 0
There are 2 independent parts. The reference program is written for one: setup_inputs(seed, part) draws one part's arguments, and reference() takes and returns one part's arrays. A program takes and returns all parts, laid end to end along the dimension named above; an argument that names none is the same for every part.
All inputs are finite; a program needn't handle non-finite values.
Results may differ from the reference program's by a relative error of at most 0.0106486.
Values are sent between devices in bfloat16 or wider.
A program may use at most 1 GiB of HBM per device.

```python
import math
import jax
import jax.numpy as jnp
from jax import lax

D = 5120
HEADS = 40
KV_HEADS = 40
HEAD = 128
FF = 13824
BATCH = 64
SEQ = 128

GROUP = HEADS // KV_HEADS
HALF = HEAD // 2
EPS = 1e-6
ROPE_BASE = 10000.0
K_SCALE = math.sqrt(max(math.log(SEQ / 16.0), 1.0))


def rope_tables(seq_lens):
    inv_freq = ROPE_BASE ** (-2.0 * jnp.arange(HALF, dtype=jnp.float32) / HEAD)
    angles = seq_lens.astype(jnp.float32)[:, None] * inv_freq[None, :]
    return jnp.cos(angles), jnp.sin(angles)


def draw_lengths(key):
    lengths = jax.random.randint(key, (BATCH,), SEQ // 8, SEQ, dtype=jnp.int32)
    return lengths.at[0].set(SEQ - 1).at[BATCH - 1].set(SEQ // 8)


def setup_inputs(seed: int = 0, part: int = 0) -> dict:
    shared = jax.random.split(jax.random.key(seed), 9)
    local = jax.random.split(jax.random.fold_in(jax.random.key(seed), part), 4)
    w_q = (jax.random.normal(shared[0], (D, HEADS, HEAD), jnp.float32) * D ** -0.5).astype(jnp.bfloat16)
    w_k = (jax.random.normal(shared[1], (D, KV_HEADS, HEAD), jnp.float32) * (K_SCALE * D ** -0.5)).astype(jnp.bfloat16)
    w_v = (jax.random.normal(shared[2], (D, KV_HEADS, HEAD), jnp.float32) * D ** -0.5).astype(jnp.bfloat16)
    w_o = (jax.random.normal(shared[3], (HEADS, HEAD, D), jnp.float32) * (HEADS * HEAD) ** -0.5).astype(jnp.bfloat16)
    w_gate = (jax.random.normal(shared[4], (D, FF), jnp.float32) * D ** -0.5).astype(jnp.bfloat16)
    w_up = (jax.random.normal(shared[5], (D, FF), jnp.float32) * D ** -0.5).astype(jnp.bfloat16)
    w_down = (jax.random.normal(shared[6], (FF, D), jnp.float32) * FF ** -0.5).astype(jnp.bfloat16)
    norm_attn = (1.0 + 0.4 * jax.random.normal(shared[7], (D,), jnp.float32)).astype(jnp.bfloat16)
    norm_mlp = (1.0 + 0.4 * jax.random.normal(shared[8], (D,), jnp.float32)).astype(jnp.bfloat16)
    hidden = jax.random.normal(local[0], (BATCH, D), jnp.float32).astype(jnp.bfloat16)
    k_cache = (jax.random.normal(local[1], (BATCH, SEQ, KV_HEADS, HEAD), jnp.float32) * K_SCALE).astype(jnp.bfloat16)
    v_cache = jax.random.normal(local[2], (BATCH, SEQ, KV_HEADS, HEAD), jnp.float32).astype(jnp.bfloat16)
    seq_lens = draw_lengths(local[3])
    rope_cos, rope_sin = rope_tables(seq_lens)
    return dict(hidden=hidden, w_q=w_q, w_k=w_k, w_v=w_v, w_o=w_o, w_gate=w_gate, w_up=w_up, w_down=w_down, norm_attn=norm_attn, norm_mlp=norm_mlp, k_cache=k_cache, v_cache=v_cache, seq_lens=seq_lens, rope_cos=rope_cos, rope_sin=rope_sin)


def rms_norm(x, gain):
    x_f32 = x.astype(jnp.float32)
    scale = lax.rsqrt(jnp.mean(x_f32 * x_f32, axis=-1, keepdims=True) + EPS)
    return (x_f32 * scale * gain.astype(jnp.float32)).astype(jnp.bfloat16)


def apply_rope(x, rope_cos, rope_sin):
    first = x[..., :HALF]
    second = x[..., HALF:]
    cosine = rope_cos[:, None, :]
    sine = rope_sin[:, None, :]
    return jnp.concatenate([first * cosine - second * sine, second * cosine + first * sine], axis=-1).astype(jnp.bfloat16)


def project(x, weight):
    return jnp.dot(x, weight.reshape(D, -1), preferred_element_type=jnp.float32).reshape(BATCH, -1, HEAD)


def attend_row(row_args):
    q_row, k_row, v_row, length = row_args
    q_grp = q_row.reshape(KV_HEADS, GROUP, HEAD).astype(jnp.float32)
    scores = jnp.einsum('kgd,skd->kgs', q_grp, k_row.astype(jnp.float32)) / math.sqrt(HEAD)
    key_mask = jnp.arange(SEQ)[None, None, :] <= length
    scores = jnp.where(key_mask, scores, -1e30)
    attn_probs = jax.nn.softmax(scores, axis=-1).astype(jnp.bfloat16).astype(jnp.float32)
    heads = jnp.einsum('kgs,skd->kgd', attn_probs, v_row.astype(jnp.float32))
    return heads.reshape(HEADS, HEAD).astype(jnp.bfloat16)


def reference(hidden, w_q, w_k, w_v, w_o, w_gate, w_up, w_down, norm_attn, norm_mlp, k_cache, v_cache, seq_lens, rope_cos, rope_sin):
    x_norm = rms_norm(hidden, norm_attn)
    q_rot = apply_rope(project(x_norm, w_q), rope_cos, rope_sin)
    k_rot = apply_rope(project(x_norm, w_k), rope_cos, rope_sin)
    v_new = project(x_norm, w_v).astype(jnp.bfloat16)
    write_mask = (jnp.arange(SEQ)[None, :] == seq_lens[:, None])[:, :, None, None]
    k_out = jnp.where(write_mask, k_rot[:, None], k_cache)
    v_out = jnp.where(write_mask, v_new[:, None], v_cache)
    attn_heads = lax.map(attend_row, (q_rot, k_out, v_out, seq_lens))
    attn_out = jnp.dot(attn_heads.reshape(BATCH, HEADS * HEAD), w_o.reshape(HEADS * HEAD, D), preferred_element_type=jnp.float32).astype(jnp.bfloat16)
    h_mid = hidden + attn_out
    x_mlp = rms_norm(h_mid, norm_mlp)
    gate = jnp.dot(x_mlp, w_gate, preferred_element_type=jnp.float32)
    up_proj = jnp.dot(x_mlp, w_up, preferred_element_type=jnp.float32)
    gated_act = (jax.nn.silu(gate) * up_proj).astype(jnp.bfloat16)
    mlp_out = jnp.dot(gated_act, w_down, preferred_element_type=jnp.float32).astype(jnp.bfloat16)
    return (h_mid + mlp_out, k_out, v_out)
```

```python
import functools

import jax
import jax.numpy as jnp
from jax import lax
from jax.experimental import pallas as pl
from jax.experimental.pallas import tpu as pltpu
from jax.sharding import PartitionSpec as P

EPS = 1e-6
MESH = pl.DeviceIdType.MESH
F32 = jnp.float32
BF16 = jnp.bfloat16
NZ = 4
A_LAG = 2
E_LAG = 4
COL = 128
RCOL = 256


def remote(src, dst, send_sem, recv_sem, **where):
    return pltpu.make_async_remote_copy(src_ref=src, dst_ref=dst, send_sem=send_sem, recv_sem=recv_sem, device_id=where, device_id_type=MESH)


def barrier(z, tp):
    sem = pltpu.get_barrier_semaphore()
    count = 0
    for k in range(1, NZ):
        pl.semaphore_signal(sem, inc=1, device_id={'dm': lax.rem(z + k, NZ)}, device_id_type=MESH)
        count += 1
    if tp is not None:
        for k in (1, 2):
            pl.semaphore_signal(sem, inc=1, device_id={'tp': partner(tp, k)}, device_id_type=MESH)
            count += 1
    pl.semaphore_wait(sem, count)


def partner(tp, k):
    if k == 1:
        return tp + 1 - 2 * lax.rem(tp, 2)
    return lax.rem(tp + 2, 4)


def exchange_sq(z, x, sq_buf, send, recv):
    rows = x.shape[0]
    lane = lax.broadcasted_iota(jnp.int32, (rows, 128), 1)
    row = lax.broadcasted_iota(jnp.int32, (rows, 128), 0)
    col = jnp.sum(x * x, axis=-1, keepdims=True)
    packed = jnp.sum(jnp.where(lane == row, col, 0.0), axis=0, keepdims=True)
    sq_buf[z] = jnp.broadcast_to(packed, (8, 128))
    for k in range(1, NZ):
        peer = lax.rem(z + k, NZ)
        remote(sq_buf.at[z], sq_buf.at[z], send.at[peer], recv.at[z], dm=peer).start()
    for k in range(1, NZ):
        peer = lax.rem(z + k, NZ)
        cp = remote(sq_buf.at[peer], sq_buf.at[peer], send.at[peer], recv.at[peer], dm=peer)
        cp.wait_recv()
        cp.wait_send()
    total = (sq_buf[0] + sq_buf[1]) + (sq_buf[2] + sq_buf[3])
    wide = jnp.broadcast_to(total[0:1], (rows, 128))
    return jnp.sum(jnp.where(lane == row, wide, 0.0), axis=1, keepdims=True)


def qkv_kernel(hid, gain, wq, wk, wv, cos, sin, out, wbuf, part, rbuf, lbuf, x_buf, sq_buf, w_sem, sq_s, sq_r, rs, rr, ls, lr):
    z = lax.axis_index('dm')
    heads = wq.shape[0]
    width = hid.shape[1] * NZ
    for h in range(heads):
        for i, w in enumerate((wq, wk, wv)):
            pltpu.make_async_copy(w.at[h], wbuf.at[i, h], w_sem.at[i, h]).start()
    barrier(z, None)
    x = hid[...].astype(F32)
    sq = exchange_sq(z, x, sq_buf, sq_s, sq_r)
    x_buf[...] = (x * lax.rsqrt(sq / width + EPS) * gain[...].astype(F32)).astype(BF16)
    cos2 = jnp.concatenate([cos[...], cos[...]], axis=-1)
    sin2 = jnp.concatenate([-sin[...], sin[...]], axis=-1)

    def right(d, p):
        return remote(part.at[d, p], rbuf.at[d, p], rs.at[d, p], rr.at[d, p], dm=lax.rem(z + 1, NZ))

    def left(d, p):
        return remote(part.at[d, p], lbuf.at[d, p], ls.at[d, p], lr.at[d, p], dm=lax.rem(z + NZ - 1, NZ))

    def slot(t, carry):
        @pl.when(t < heads)
        def _():
            for i, w in enumerate((wq, wk, wv)):
                pltpu.make_async_copy(w.at[t], wbuf.at[i, t], w_sem.at[i, t]).wait()
                y = jnp.dot(x_buf[...], wbuf[i, t], preferred_element_type=F32)
                for d in range(NZ):
                    part[d, t, :, i * 128:(i + 1) * 128] = y[d * 16:(d + 1) * 16]

        p = t - A_LAG * z

        @pl.when((p >= 0) & (p < heads))
        def _():
            for d in (3, 2, 1):
                @pl.when((z > 0) & (z <= d))
                def _(d=d):
                    right(d, p).wait_recv()
                    part[d, p] = part[d, p] + rbuf[d, p]

                @pl.when(z < d)
                def _(d=d):
                    right(d, p).start()

        b = t - A_LAG * (NZ - 1 - z)

        @pl.when((b >= 0) & (b < heads))
        def _():
            for d in (0, 1, 2):
                @pl.when((z < NZ - 1) & (z >= d))
                def _(d=d):
                    left(d, b).wait_recv()
                    part[d, b] = part[d, b] + lbuf[d, b]

                @pl.when(z > d)
                def _(d=d):
                    left(d, b).start()

        f = t - A_LAG * jnp.maximum(z, NZ - 1 - z)

        @pl.when((f >= 0) & (f < heads))
        def _():
            q = part[z, f, :, 0:128]
            k = part[z, f, :, 128:256]
            out[0, f] = (q * cos2 + pltpu.roll(q, 64, 1) * sin2).astype(BF16)
            out[1, f] = (k * cos2 + pltpu.roll(k, 64, 1) * sin2).astype(BF16)
            out[2, f] = part[z, f, :, 256:384].astype(BF16)

        return carry

    lax.fori_loop(0, heads + A_LAG * (NZ - 1), slot, 0)

    def drain(p, carry):
        for d in range(NZ):
            @pl.when(z < d)
            def _(d=d):
                right(d, p).wait_send()

            @pl.when(z > d)
            def _(d=d):
                left(d, p).wait_send()

        return carry

    lax.fori_loop(0, heads, drain, 0)


def qkv_call(hid, gain, wq, wk, wv, cos, sin):
    heads, width, hd = wq.shape
    rows = hid.shape[0]
    vm = pl.BlockSpec(memory_space=pltpu.VMEM)
    hbm = pl.BlockSpec(memory_space=pltpu.HBM)
    dma = pltpu.SemaphoreType.DMA
    return pl.pallas_call(
        qkv_kernel,
        name='qkv_rs',
        out_shape=jax.ShapeDtypeStruct((3, heads, rows // NZ, hd), BF16),
        in_specs=[vm, vm, hbm, hbm, hbm, vm, vm],
        out_specs=vm,
        scratch_shapes=[
            pltpu.VMEM((3, heads, width, hd), BF16),
            pltpu.VMEM((NZ, heads, rows // NZ, 3 * hd), F32),
            pltpu.VMEM((NZ, heads, rows // NZ, 3 * hd), F32),
            pltpu.VMEM((NZ, heads, rows // NZ, 3 * hd), F32),
            pltpu.VMEM((rows, width), BF16),
            pltpu.VMEM((NZ, 8, 128), F32),
            dma((3, heads)),
            dma((NZ,)), dma((NZ,)),
            dma((NZ, heads)), dma((NZ, heads)), dma((NZ, heads)), dma((NZ, heads)),
        ],
        compiler_params=pltpu.CompilerParams(collective_id=0, has_side_effects=True, vmem_limit_bytes=20 * 2**20),
        cost_estimate=pl.CostEstimate(flops=2 * rows * width * heads * 3 * hd, bytes_accessed=80_000_000, transcendentals=0),
    )(hid, gain, wq, wk, wv, cos, sin)


def attn_kernel(lens, qkv, k_in, v_in, o, k_out, v_out):
    rows, heads, slots, hd = k_in.shape
    row = lax.broadcasted_iota(jnp.int32, (rows, slots), 0)
    pos = lax.broadcasted_iota(jnp.int32, (rows, slots), 1)
    tile_pos = lax.broadcasted_iota(jnp.int32, (16, hd), 0)
    length = jnp.zeros((rows, slots), jnp.int32)
    for r in range(rows):
        length = jnp.where(row == r, lens[r], length)
    at_len = pos == length
    seen = pos <= length

    def head(h, carry):
        q = qkv[0, h]
        k_new = qkv[1, h].astype(F32)
        v_new = qkv[2, h].astype(F32)
        s = jnp.zeros((rows, slots), F32)
        for r in range(rows):
            y = lax.dot_general(q, k_in[r, h], (((1,), (1,)), ((), ())), preferred_element_type=F32)
            s = jnp.where(row == r, y, s)
        s_new = jnp.sum(q.astype(F32) * k_new, axis=-1, keepdims=True)
        s = jnp.where(at_len, s_new, s) * (hd ** -0.5)
        s = jnp.where(seen, s, -1e30)
        e = jnp.exp(s - jnp.max(s, axis=-1, keepdims=True))
        prob = (e / jnp.sum(e, axis=-1, keepdims=True)).astype(BF16)
        prob32 = prob.astype(F32)
        p_new = jnp.sum(jnp.where(at_len, prob32, 0.0), axis=-1, keepdims=True)
        p_old = jnp.where(at_len, 0.0, prob32).astype(BF16)
        acc = jnp.zeros((rows, hd), F32)
        for r in range(rows):
            y = jnp.dot(p_old, v_in[r, h], preferred_element_type=F32)
            acc = jnp.where(row == r, y, acc)
        o[h] = (acc + p_new * v_new).astype(BF16)
        for r in range(rows):
            k_out[r, h] = k_in[r, h]
            v_out[r, h] = v_in[r, h]
            base = pl.multiple_of((lens[r] // 16) * 16, 16)
            hit = tile_pos == lens[r] - base
            old = k_in[r, h, pl.ds(base, 16), :].astype(F32)
            k_out[r, h, pl.ds(base, 16), :] = jnp.where(hit, k_new[r:r + 1], old).astype(BF16)
            old = v_in[r, h, pl.ds(base, 16), :].astype(F32)
            v_out[r, h, pl.ds(base, 16), :] = jnp.where(hit, v_new[r:r + 1], old).astype(BF16)
        return carry

    lax.fori_loop(0, heads, head, 0)


def attn_call(lens, qkv, k_cache, v_cache):
    rows, heads, slots, hd = k_cache.shape
    vm = pl.BlockSpec(memory_space=pltpu.VMEM)
    cache = jax.ShapeDtypeStruct(k_cache.shape, BF16)
    return pl.pallas_call(
        attn_kernel,
        name='attn',
        out_shape=[jax.ShapeDtypeStruct((heads, rows, hd), BF16), cache, cache],
        in_specs=[pl.BlockSpec(memory_space=pltpu.SMEM), vm, vm, vm],
        out_specs=[vm, vm, vm],
        compiler_params=pltpu.CompilerParams(vmem_limit_bytes=28 * 2**20),
        cost_estimate=pl.CostEstimate(flops=4 * rows * heads * slots * hd, bytes_accessed=8 * rows * heads * slots * hd, transcendentals=rows * heads * slots),
    )(lens, qkv, k_cache, v_cache)


def mlp_kernel(o_mine, hid, gain, wo, wg, wu, wd, out,
               wo_b, wg_b, wu_b, wd_b, o_all, part, r1, s_buf, r2, h_mid, x_buf, pbuf, rbuf, lbuf, mbuf, sq_buf,
               w_sem, g_sem, o_s, o_r, a_s, a_r, b_s, b_r, c_s, c_r, sq_s, sq_r,
               rs, rr, ls, lr, mr_s, mr_r, ml_s, ml_r):
    z = lax.axis_index('dm')
    tp = lax.axis_index('tp')
    rows, width = hid.shape
    half = rows // 2
    per = rows // NZ
    heads, hd = o_mine.shape[0], o_mine.shape[2]
    ff = wg.shape[1]
    n_col = ff // COL
    n_grp = g_sem.shape[1]
    grp = ff // n_grp
    n_red = width // RCOL
    core = lax.rem(tp, 2)
    sib, across = partner(tp, 1), partner(tp, 2)
    mine = pl.ds(pl.multiple_of(core * half, half), half)
    other = pl.ds(pl.multiple_of((1 - core) * half, half), half)

    load_o = pltpu.make_async_copy(wo, wo_b, w_sem.at[0])
    load_d = pltpu.make_async_copy(wd, wd_b, w_sem.at[1])

    def load(i, g):
        src, dst = ((wg, wg_b), (wu, wu_b))[i]
        cols = pl.ds(pl.multiple_of(g * grp, COL), grp)
        return pltpu.make_async_copy(src.at[:, cols], dst.at[:, cols], g_sem.at[i, g])

    load_o.start()
    for g in range(n_grp):
        load(0, g).start()
        load(1, g).start()
    load_d.start()
    barrier(z, tp)

    def o_copy(frm, to):
        return remote(o_mine, o_all.at[frm], o_s.at[to], o_r.at[frm], dm=to)

    for k in (2, 1, 3):
        o_copy(z, lax.rem(z + k, NZ)).start()
    o_all[z] = o_mine[...]
    for k in (1, 3, 2):
        o_copy(lax.rem(z + k, NZ), lax.rem(z + k, NZ)).wait_recv()

    def reduce_tp(step, lhs, w_ref, base, dst, add):
        def a_copy(j):
            return remote(part.at[j, other], r1.at[step, j], a_s.at[step, j], a_r.at[step, j], tp=sib)

        def b_copy(j):
            return remote(s_buf.at[step, j], r2.at[step, j], b_s.at[step, j], b_r.at[step, j], tp=across)

        def c_copy(j):
            view = dst.at[mine, pl.ds(j * RCOL, RCOL)]
            return remote(view, view, c_s.at[step, j], c_r.at[step, j], tp=sib)

        def c_arrival(j):
            view = dst.at[other, pl.ds(j * RCOL, RCOL)]
            return remote(view, view, c_s.at[step, j], c_r.at[step, j], tp=sib)

        for j in range(n_red):
            part[j] = jnp.dot(lhs, w_ref[:, j * RCOL:(j + 1) * RCOL], preferred_element_type=F32)
            a_copy(j).start()
        for j in range(n_red):
            a_copy(j).wait_recv()
            s_buf[step, j] = part[j, mine] + r1[step, j]
            b_copy(j).start()
        for j in range(n_red):
            b_copy(j).wait_recv()
            total = (s_buf[step, j] + r2[step, j]).astype(BF16)
            cols = pl.ds(j * RCOL, RCOL)
            dst[mine, cols] = (base[mine, cols].astype(F32) + total.astype(F32)).astype(BF16)
            c_copy(j).start()
        for j in range(n_red):
            c_arrival(j).wait_recv()
            a_copy(j).wait_send()
            b_copy(j).wait_send()
            c_copy(j).wait_send()

    load_o.wait()
    o_cat = jnp.concatenate([jnp.concatenate([o_all[d, h] for h in range(heads)], axis=1) for d in range(NZ)], axis=0)
    x_buf[...] = o_cat
    reduce_tp(0, x_buf[...], wo_b, hid, h_mid, None)
    for k in range(1, NZ):
        o_copy(z, lax.rem(z + k, NZ)).wait_send()

    x = h_mid[...].astype(F32)
    sq = exchange_sq(z, x, sq_buf, sq_s, sq_r)
    x_buf[...] = (x * lax.rsqrt(sq / (width * NZ) + EPS) * gain[...].astype(F32)).astype(BF16)

    low, high = pl.ds(0, half), pl.ds(half, half)
    nxt, prv = lax.rem(z + 1, NZ), lax.rem(z + NZ - 1, NZ)

    def right(c):
        return remote(pbuf.at[c, 1], rbuf.at[c], rs.at[c], rr.at[c], dm=nxt)

    def left(c):
        return remote(pbuf.at[c, 0], lbuf.at[c], ls.at[c], lr.at[c], dm=prv)

    def cols_of(c):
        return pl.ds(pl.multiple_of(c * COL, COL), COL)

    def m_left(c):
        view = mbuf.at[high, cols_of(c)]
        return remote(view, view, mr_s.at[c], mr_r.at[c], dm=prv)

    def m_right(c):
        view = mbuf.at[low, cols_of(c)]
        return remote(view, view, ml_s.at[c], ml_r.at[c], dm=nxt)

    def gated(a):
        g, u = a[:, :COL], a[:, COL:]
        return (g * (1.0 / (1.0 + jnp.exp(-g))) * u).astype(BF16)

    def slot(t, carry):
        @pl.when(t < n_col)
        def _():
            per_grp = n_col // n_grp

            @pl.when(lax.rem(t, per_grp) == 0)
            def _():
                load(0, t // per_grp).wait()
                load(1, t // per_grp).wait()

            g = jnp.dot(x_buf[...], wg_b[:, cols_of(t)], preferred_element_type=F32)
            u = jnp.dot(x_buf[...], wu_b[:, cols_of(t)], preferred_element_type=F32)
            pbuf[t, 0, :, 0:COL] = g[:half]
            pbuf[t, 1, :, 0:COL] = g[half:]
            pbuf[t, 0, :, COL:] = u[:half]
            pbuf[t, 1, :, COL:] = u[half:]

        c = t - E_LAG * z

        @pl.when((c >= 0) & (c < n_col))
        def _():
            @pl.when(z > 0)
            def _():
                right(c).wait_recv()
                pbuf[c, 1] = pbuf[c, 1] + rbuf[c]

            @pl.when(z < NZ - 1)
            def _():
                right(c).start()

            @pl.when(z == NZ - 1)
            def _():
                mbuf[high, cols_of(c)] = gated(pbuf[c, 1])
                m_left(c).start()

        b = t - E_LAG * (NZ - 1 - z)

        @pl.when((b >= 0) & (b < n_col))
        def _():
            @pl.when(z < NZ - 1)
            def _():
                left(b).wait_recv()
                pbuf[b, 0] = pbuf[b, 0] + lbuf[b]

            @pl.when(z > 0)
            def _():
                left(b).start()

            @pl.when(z == 0)
            def _():
                mbuf[low, cols_of(b)] = gated(pbuf[b, 0])
                m_right(b).start()

        e = t - E_LAG * (2 * NZ - 2 - z)

        @pl.when((e >= 0) & (e < n_col) & (z < NZ - 1))
        def _():
            m_left(e).wait_recv()

            @pl.when(z > 0)
            def _():
                m_left(e).start()

        f = t - E_LAG * (NZ - 1 + z)

        @pl.when((f >= 0) & (f < n_col) & (z > 0))
        def _():
            m_right(f).wait_recv()

            @pl.when(z < NZ - 1)
            def _():
                m_right(f).start()

        return carry

    lax.fori_loop(0, n_col + E_LAG * (2 * NZ - 2), slot, 0)
    load_d.wait()
    reduce_tp(1, mbuf[...], wd_b, h_mid, out, None)

    def drain(c, carry):
        @pl.when(z < NZ - 1)
        def _():
            right(c).wait_send()
            m_right(c).wait_send()

        @pl.when(z > 0)
        def _():
            left(c).wait_send()
            m_left(c).wait_send()

        return carry

    lax.fori_loop(0, n_col, drain, 0)


def mlp_call(o_mine, hid, gain, wo, wg, wu, wd):
    rows, width = hid.shape
    heads, per, hd = o_mine.shape
    ff = wg.shape[1]
    n_col, n_red = ff // COL, width // RCOL
    n_grp = 9 if n_col % 9 == 0 else 1
    half = rows // 2
    vm = pl.BlockSpec(memory_space=pltpu.VMEM)
    hbm = pl.BlockSpec(memory_space=pltpu.HBM)
    dma = pltpu.SemaphoreType.DMA
    return pl.pallas_call(
        mlp_kernel,
        name='mlp',
        out_shape=jax.ShapeDtypeStruct((rows, width), BF16),
        in_specs=[vm, vm, vm, hbm, hbm, hbm, hbm],
        out_specs=vm,
        scratch_shapes=[
            pltpu.VMEM(wo.shape, BF16), pltpu.VMEM(wg.shape, BF16), pltpu.VMEM(wu.shape, BF16), pltpu.VMEM(wd.shape, BF16),
            pltpu.VMEM((NZ, heads, per, hd), BF16),
            pltpu.VMEM((n_red, rows, RCOL), F32),
            pltpu.VMEM((2, n_red, half, RCOL), F32),
            pltpu.VMEM((2, n_red, half, RCOL), F32),
            pltpu.VMEM((2, n_red, half, RCOL), F32),
            pltpu.VMEM((rows, width), BF16),
            pltpu.VMEM((rows, width), BF16),
            pltpu.VMEM((n_col, 2, half, 2 * COL), F32),
            pltpu.VMEM((n_col, half, 2 * COL), F32),
            pltpu.VMEM((n_col, half, 2 * COL), F32),
            pltpu.VMEM((rows, ff), BF16),
            pltpu.VMEM((NZ, 8, 128), F32),
            dma((2,)), dma((2, n_grp)),
            dma((NZ,)), dma((NZ,)),
            dma((2, n_red)), dma((2, n_red)), dma((2, n_red)), dma((2, n_red)), dma((2, n_red)), dma((2, n_red)),
            dma((NZ,)), dma((NZ,)),
            dma((n_col,)), dma((n_col,)), dma((n_col,)), dma((n_col,)),
            dma((n_col,)), dma((n_col,)), dma((n_col,)), dma((n_col,)),
        ],
        compiler_params=pltpu.CompilerParams(collective_id=1, has_side_effects=True, vmem_limit_bytes=44 * 2**20),
        cost_estimate=pl.CostEstimate(flops=2 * rows * width * (width + 3 * ff), bytes_accessed=150_000_000, transcendentals=0),
    )(o_mine, hid, gain, wo, wg, wu, wd)


def solution(mesh):
    row_spec = P('dp', 'dm')
    cache_spec = P(('dp', 'dm'), None, 'tp', None)
    batch_spec = P(('dp', 'dm'))
    rope_spec = P(('dp', 'dm'), None)
    in_specs = (row_spec, P('dm', 'tp', None), P('dm', 'tp', None), P('dm', 'tp', None), P('tp', None, 'dm'), P('dm', 'tp'), P('dm', 'tp'), P('tp', 'dm'), P('dm'), P('dm'), cache_spec, cache_spec, batch_spec, rope_spec, rope_spec)
    out_specs = (row_spec, cache_spec, cache_spec)

    def local_layer(hidden, w_q, w_k, w_v, w_o, w_gate, w_up, w_down, norm_attn, norm_mlp, k_cache, v_cache, seq_lens, rope_cos, rope_sin):
        by_head = [w.transpose(1, 0, 2) for w in (w_q, w_k, w_v)]
        qkv = qkv_call(hidden, norm_attn.reshape(1, -1), *by_head, rope_cos, rope_sin)
        heads, k_out, v_out = attn_call(seq_lens, qkv, k_cache.transpose(0, 2, 1, 3), v_cache.transpose(0, 2, 1, 3))
        h_out = mlp_call(heads, hidden, norm_mlp.reshape(1, -1), w_o.reshape(-1, w_o.shape[-1]), w_gate, w_up, w_down)
        return h_out, k_out.transpose(0, 2, 1, 3), v_out.transpose(0, 2, 1, 3)

    return jax.shard_map(local_layer, mesh=mesh, in_specs=in_specs, out_specs=out_specs, check_vma=False)
```

```python
import jax
import jax.numpy as jnp
from jax import lax
from jax.experimental import pallas as pl
from jax.experimental.pallas import tpu as pltpu
from jax.sharding import PartitionSpec as P

EPS = 1e-6
MESH = pl.DeviceIdType.MESH
F32 = jnp.float32
BF16 = jnp.bfloat16
NZ = 4
A_LAG = 2
E_LAG = 4
COL = 128
RCOL = 256


def remote(src, dst, send_sem, recv_sem, **where):
    return pltpu.make_async_remote_copy(src_ref=src, dst_ref=dst, send_sem=send_sem, recv_sem=recv_sem, device_id=where, device_id_type=MESH)


def partner(tp, k):
    if k == 1:
        return tp + 1 - 2 * lax.rem(tp, 2)
    return lax.rem(tp + 2, 4)


def pack_rows(col):
    rows = col.shape[0]
    lane = lax.broadcasted_iota(jnp.int32, (rows, 128), 1)
    row = lax.broadcasted_iota(jnp.int32, (rows, 128), 0)
    packed = jnp.sum(jnp.where(lane == row, col, 0.0), axis=0, keepdims=True)
    return jnp.broadcast_to(packed, (8, 128))


def unpack_rows(tile, rows):
    lane = lax.broadcasted_iota(jnp.int32, (rows, 128), 1)
    row = lax.broadcasted_iota(jnp.int32, (rows, 128), 0)
    wide = jnp.broadcast_to(tile[0:1], (rows, 128))
    return jnp.sum(jnp.where(lane == row, wide, 0.0), axis=1, keepdims=True)


def layer_kernel(hid_h, g1_h, g2_h, wq, wk, wv, wo, wg, wu, wd, kc, vc, lens_h, cos_h, sin_h,
                 out, k_out, v_out,
                 hid, g1, g2, lens, cos, sin, wbuf, wo_b, wg_b, wu_b, wd_b,
                 part, rbuf, lbuf, x_buf, o_x, new_kv, red, r1, s_buf, r2, h_mid, pbuf, rbuf2, lbuf2, mbuf,
                 cum_in, cum_out, own_sq, fac,
                 s_sem, w_sem, c_sem, b_sem, g_sem, rs, rr, ls, lr, o_s, o_r, a_s, a_r, b_s, b_r, c_s, c_r,
                 q_s, q_r, rs2, rr2, ls2, lr2, mr_s, mr_r, ml_s, ml_r):
    z = lax.axis_index('dm')
    tp = lax.axis_index('tp')
    rows, width = hid.shape
    full = width * NZ
    heads = wq.shape[0]
    hd = wq.shape[2]
    per = rows // NZ
    half = rows // 2
    slots = kc.shape[2]
    ff = wg.shape[1]
    n_col = ff // COL
    n_grp = g_sem.shape[1]
    grp = ff // n_grp
    n_red = width // RCOL
    early = (n_col * 2 // 3) // 2 * 2
    core = lax.rem(tp, 2)
    sib, across = partner(tp, 1), partner(tp, 2)
    nxt, prv = lax.rem(z + 1, NZ), lax.rem(z + NZ - 1, NZ)

    small = [pltpu.make_async_copy(a, b, s_sem.at[i]) for i, (a, b) in enumerate(((hid_h, hid), (g1_h, g1), (g2_h, g2), (cos_h, cos), (sin_h, sin), (lens_h, lens)))]
    load_o = pltpu.make_async_copy(wo, wo_b, b_sem.at[0])
    load_d = pltpu.make_async_copy(wd, wd_b, b_sem.at[1])

    def load_w(i, h):
        return pltpu.make_async_copy((wq, wk, wv)[i].at[h], wbuf.at[i, h], w_sem.at[i, h])

    def load_c(i, h):
        return pltpu.make_async_copy((kc, vc)[i].at[:, h], (k_out, v_out)[i].at[:, h], c_sem.at[i, h])

    def load(i, g):
        src, dst = ((wg, wg_b), (wu, wu_b))[i]
        cols = pl.ds(pl.multiple_of(g * grp, COL), grp)
        return pltpu.make_async_copy(src.at[:, cols], dst.at[:, cols], g_sem.at[i, g])

    for cp in small:
        cp.start()
    for h in range(heads):
        for i in range(3):
            load_w(i, h).start()
        if h >= 2:
            load_c(0, h - 2).start()
            load_c(1, h - 2).start()
    for h in range(max(heads - 2, 0), heads):
        load_c(0, h).start()
        load_c(1, h).start()
    load_o.start()
    for g in range(n_grp):
        load(0, g).start()
        load(1, g).start()
    load_d.start()

    sem = pltpu.get_barrier_semaphore()
    for k in range(1, NZ):
        pl.semaphore_signal(sem, inc=1, device_id={'dm': lax.rem(z + k, NZ)}, device_id_type=MESH)
    for k in (1, 2):
        pl.semaphore_signal(sem, inc=1, device_id={'tp': partner(tp, k)}, device_id_type=MESH)

    for cp in small:
        cp.wait()

    def local_norm(x, gain, step):
        col = jnp.sum(x * x, axis=-1, keepdims=True)
        own_sq[step] = pack_rows(col)
        x_buf[...] = (x * lax.rsqrt(col / full + EPS) * gain).astype(BF16)

    def inv(tile):
        return lax.rsqrt(tile / full + EPS)

    def stat(step, side):
        return remote(cum_out.at[step, side], cum_in.at[step, side], q_s.at[step, side], q_r.at[step, side], dm=(nxt, prv)[side])

    def relay_stat(step, side):
        has_in = (z > 0) if side == 0 else (z < NZ - 1)
        has_out = (z < NZ - 1) if side == 0 else (z > 0)

        @pl.when(has_in)
        def _():
            stat(step, side).wait_recv()

        @pl.when(jnp.logical_not(has_in))
        def _():
            cum_in[step, side] = jnp.zeros((8, 128), F32)

        before, own = cum_in[step, side], own_sq[step]
        cum = before + own
        cum_out[step, side] = cum

        @pl.when(has_out)
        def _():
            stat(step, side).start()

        scale = inv(cum)
        put_fac(2 * side, scale / inv(own))
        put_fac(2 * side + 1, scale / inv(before))

    def put_fac(i, tile):
        wide = jnp.broadcast_to(unpack_rows(tile, rows), (rows, 128))
        for d in range(NZ):
            fac[i, d] = wide[d * per:(d + 1) * per]

    local_norm(hid[...].astype(F32), g1[...].astype(F32).reshape(1, width), 0)
    cos2 = jnp.concatenate([cos[...], cos[...]], axis=-1)
    sin2 = jnp.concatenate([-sin[...], sin[...]], axis=-1)

    @pl.when(z == 0)
    def _():
        rbuf[0] = jnp.zeros(rbuf.shape[1:], F32)

    @pl.when(z == NZ - 1)
    def _():
        lbuf[NZ - 1] = jnp.zeros(lbuf.shape[1:], F32)

    row = lax.broadcasted_iota(jnp.int32, (per, slots), 0)
    pos = lax.broadcasted_iota(jnp.int32, (per, slots), 1)
    length = jnp.zeros((per, slots), jnp.int32)
    for r in range(per):
        length = jnp.where(row == r, lens[r], length)
    at_len = pos == length
    seen = pos <= length

    pl.semaphore_wait(sem, NZ + 1)

    def right(d, p):
        return remote(part.at[d, p], rbuf.at[d, p], rs.at[d, p], rr.at[d, p], dm=nxt)

    def left(d, p):
        return remote(part.at[d, p], lbuf.at[d, p], ls.at[d, p], lr.at[d, p], dm=prv)

    def o_view(src, p):
        return o_x.at[pl.ds(pl.multiple_of(src * per, per), per), pl.ds(pl.multiple_of(p * hd, hd), hd)]

    def o_copy(src, to, p):
        return remote(o_view(src, p), o_view(src, p), o_s.at[p, to], o_r.at[p, src], dm=to)

    def thrice(i, d):
        f = fac[i, d]
        return jnp.concatenate([f, f, f], axis=1)

    def attend(h):
        y = part[z, h] * thrice(4, z) + (rbuf[z, h] * thrice(5, z) + lbuf[z, h] * thrice(6, z))
        q, k = y[:, 0:hd], y[:, hd:2 * hd]
        q = (q * cos2 + pltpu.roll(q, hd // 2, 1) * sin2).astype(BF16)
        k_new = (k * cos2 + pltpu.roll(k, hd // 2, 1) * sin2).astype(BF16).astype(F32)
        v_new = y[:, 2 * hd:].astype(BF16).astype(F32)
        new_kv[0, h] = k_new
        new_kv[1, h] = v_new
        load_c(0, h).wait()
        load_c(1, h).wait()
        s = jnp.zeros((per, slots), F32)
        for r in range(per):
            t = lax.dot_general(q, k_out[r, h], (((1,), (1,)), ((), ())), preferred_element_type=F32)
            s = jnp.where(row == r, t, s)
        s_new = jnp.sum(q.astype(F32) * k_new, axis=-1, keepdims=True)
        s = jnp.where(at_len, s_new, s) * (hd ** -0.5)
        s = jnp.where(seen, s, -1e30)
        e = jnp.exp(s - jnp.max(s, axis=-1, keepdims=True))
        prob = (e / jnp.sum(e, axis=-1, keepdims=True)).astype(BF16).astype(F32)
        p_new = jnp.sum(jnp.where(at_len, prob, 0.0), axis=-1, keepdims=True)
        p_old = jnp.where(at_len, 0.0, prob).astype(BF16)
        acc = jnp.zeros((per, hd), F32)
        for r in range(per):
            t = jnp.dot(p_old, v_out[r, h], preferred_element_type=F32)
            acc = jnp.where(row == r, t, acc)
        o_x[pl.ds(pl.multiple_of(z * per, per), per), pl.ds(pl.multiple_of(h * hd, hd), hd)] = (acc + p_new * v_new).astype(BF16)
        for k in (2, 1, 3):
            o_copy(z, lax.rem(z + k, NZ), h).start()

    def patch(lo, hi):
        where = lax.broadcasted_iota(jnp.int32, (slots, hd), 0)

        def body(h, carry):
            for r in range(per):
                hit = where == lens[r]
                for i, ref in enumerate((k_out, v_out)):
                    fresh = jnp.broadcast_to(new_kv[i, h, r:r + 1, :], (slots, hd))
                    ref[r, h] = jnp.where(hit, fresh, ref[r, h].astype(F32)).astype(BF16)
            return carry

        lax.fori_loop(lo, hi, body, 0)

    def a_slot(t, carry):
        @pl.when(t < heads)
        def _():
            for i in range(3):
                load_w(i, t).wait()
                y = jnp.dot(x_buf[...], wbuf[i, t], preferred_element_type=F32)
                for d in range(NZ):
                    part[d, t, :, i * hd:(i + 1) * hd] = y[d * per:(d + 1) * per]

        p = t - A_LAG * z

        @pl.when(p == 0)
        def _():
            relay_stat(0, 0)

        @pl.when((p >= 0) & (p < heads))
        def _():
            for d in (3, 2, 1):
                @pl.when((z > 0) & (z <= d))
                def _(d=d):
                    right(d, p).wait_recv()

                @pl.when((z > 0) & (z < d))
                def _(d=d):
                    part[d, p] = part[d, p] * thrice(0, d) + rbuf[d, p] * thrice(1, d)

                @pl.when(z < d)
                def _(d=d):
                    right(d, p).start()

        b = t - A_LAG * (NZ - 1 - z)

        @pl.when(b == 0)
        def _():
            relay_stat(0, 1)

        @pl.when((b >= 0) & (b < heads))
        def _():
            for d in (0, 1, 2):
                @pl.when((z < NZ - 1) & (z >= d))
                def _(d=d):
                    left(d, b).wait_recv()

                @pl.when((z < NZ - 1) & (z > d))
                def _(d=d):
                    part[d, b] = part[d, b] * thrice(2, d) + lbuf[d, b] * thrice(3, d)

                @pl.when(z > d)
                def _(d=d):
                    left(d, b).start()

        f = t - A_LAG * jnp.maximum(z, NZ - 1 - z)

        @pl.when(f == 0)
        def _():
            own = own_sq[0]
            scale = inv((cum_in[0, 0] + own) + cum_in[0, 1])
            put_fac(4, scale / inv(own))
            put_fac(5, scale / inv(cum_in[0, 0]))
            put_fac(6, scale / inv(cum_in[0, 1]))

        @pl.when((f >= 0) & (f < heads))
        def _():
            attend(f)

        return carry

    lax.fori_loop(0, heads + A_LAG * (NZ - 1), a_slot, 0)
    patch(0, heads // 2)

    def o_wait(p, carry):
        for k in (1, 3, 2):
            o_copy(lax.rem(z + k, NZ), lax.rem(z + k, NZ), p).wait_recv()
        return carry

    lax.fori_loop(0, heads, o_wait, 0)
    load_o.wait()

    mine = pl.ds(pl.multiple_of(core * half, half), half)
    other = pl.ds(pl.multiple_of((1 - core) * half, half), half)

    def reduce_tp(step, product, base, dst, meanwhile):
        def a_copy(j):
            return remote(red.at[j, other], r1.at[step, j], a_s.at[step, j], a_r.at[step, j], tp=sib)

        def b_copy(j):
            return remote(s_buf.at[step, j], r2.at[step, j], b_s.at[step, j], b_r.at[step, j], tp=across)

        def c_copy(j, part_rows):
            view = dst.at[part_rows, pl.ds(j * RCOL, RCOL)]
            return remote(view, view, c_s.at[step, j], c_r.at[step, j], tp=sib)

        for j in range(n_red):
            red[j] = product(j)
            a_copy(j).start()
        for j in range(n_red):
            a_copy(j).wait_recv()
            s_buf[step, j] = red[j, mine] + r1[step, j]
            b_copy(j).start()
        meanwhile()
        for j in range(n_red):
            b_copy(j).wait_recv()
            total = (s_buf[step, j] + r2[step, j]).astype(BF16)
            cols = pl.ds(j * RCOL, RCOL)
            dst[mine, cols] = (base[mine, cols].astype(F32) + total.astype(F32)).astype(BF16)
            c_copy(j, mine).start()
        for j in range(n_red):
            c_copy(j, other).wait_recv()
        for j in range(n_red):
            a_copy(j).wait_send()
            b_copy(j).wait_send()
            c_copy(j, mine).wait_send()

    reduce_tp(0, lambda j: jnp.dot(o_x[...], wo_b[:, j * RCOL:(j + 1) * RCOL], preferred_element_type=F32), hid, h_mid, lambda: patch(heads // 2, heads))
    local_norm(h_mid[...].astype(F32), g2[...].astype(F32).reshape(1, width), 1)

    def right2(c):
        return remote(pbuf.at[c, 1], rbuf2.at[c], rs2.at[c], rr2.at[c], dm=nxt)

    def left2(c):
        return remote(pbuf.at[c, 0], lbuf2.at[c], ls2.at[c], lr2.at[c], dm=prv)

    low, high = pl.ds(0, half), pl.ds(half, half)

    def cols_of(c):
        return pl.ds(pl.multiple_of(c * COL, COL), COL)

    def m_left(c):
        view = mbuf.at[high, cols_of(c)]
        return remote(view, view, mr_s.at[c], mr_r.at[c], dm=prv)

    def m_right(c):
        view = mbuf.at[low, cols_of(c)]
        return remote(view, view, ml_s.at[c], ml_r.at[c], dm=nxt)

    def gated(a):
        g, u = a[:, :COL], a[:, COL:]
        return (g * (1.0 / (1.0 + jnp.exp(-g))) * u).astype(BF16)

    def wide(i, first):
        f = jnp.concatenate([fac[i, first], fac[i, first + 1]], axis=0)
        return jnp.concatenate([f, f], axis=1)

    def e_slot(t, carry):
        @pl.when(t < n_col)
        def _():
            per_grp = n_col // n_grp

            @pl.when(lax.rem(t, per_grp) == 0)
            def _():
                load(0, t // per_grp).wait()
                load(1, t // per_grp).wait()

            g = jnp.dot(x_buf[...], wg_b[:, cols_of(t)], preferred_element_type=F32)
            u = jnp.dot(x_buf[...], wu_b[:, cols_of(t)], preferred_element_type=F32)
            pbuf[t, 0, :, 0:COL] = g[:half]
            pbuf[t, 1, :, 0:COL] = g[half:]
            pbuf[t, 0, :, COL:] = u[:half]
            pbuf[t, 1, :, COL:] = u[half:]

        c = t - E_LAG * z

        @pl.when(c == 0)
        def _():
            relay_stat(1, 0)

        @pl.when((c >= 0) & (c < n_col))
        def _():
            @pl.when(z > 0)
            def _():
                right2(c).wait_recv()
                pbuf[c, 1] = pbuf[c, 1] * wide(0, 2) + rbuf2[c] * wide(1, 2)

            @pl.when(z < NZ - 1)
            def _():
                right2(c).start()

            @pl.when(z == NZ - 1)
            def _():
                mbuf[high, cols_of(c)] = gated(pbuf[c, 1])
                m_left(c).start()

        b = t - E_LAG * (NZ - 1 - z)

        @pl.when(b == 0)
        def _():
            relay_stat(1, 1)

        @pl.when((b >= 0) & (b < n_col))
        def _():
            @pl.when(z < NZ - 1)
            def _():
                left2(b).wait_recv()
                pbuf[b, 0] = pbuf[b, 0] * wide(2, 0) + lbuf2[b] * wide(3, 0)

            @pl.when(z > 0)
            def _():
                left2(b).start()

            @pl.when(z == 0)
            def _():
                mbuf[low, cols_of(b)] = gated(pbuf[b, 0])
                m_right(b).start()

        e = t - E_LAG * (2 * NZ - 2 - z)

        @pl.when((e >= 0) & (e < n_col) & (z < NZ - 1))
        def _():
            m_left(e).wait_recv()

            @pl.when(z > 0)
            def _():
                m_left(e).start()

        f = t - E_LAG * (NZ - 1 + z)

        @pl.when((f >= 0) & (f < n_col) & (z > 0))
        def _():
            m_right(f).wait_recv()

            @pl.when(z < NZ - 1)
            def _():
                m_right(f).start()

        w = t - (early + E_LAG * (2 * NZ - 2))

        @pl.when(w == 0)
        def _():
            load_d.wait()

        @pl.when((w >= 0) & (w < n_red))
        def _():
            red[w] = jnp.dot(mbuf[:, 0:early * COL], wd_b[0:early * COL, pl.ds(pl.multiple_of(w * RCOL, RCOL), RCOL)], preferred_element_type=F32)

        return carry

    lax.fori_loop(0, max(n_col, early + n_red) + E_LAG * (2 * NZ - 2), e_slot, 0)
    reduce_tp(1, lambda j: red[j] + jnp.dot(mbuf[:, early * COL:], wd_b[early * COL:, j * RCOL:(j + 1) * RCOL], preferred_element_type=F32), h_mid, out, lambda: None)

    def drain_a(p, carry):
        for d in range(NZ):
            @pl.when(z < d)
            def _(d=d):
                right(d, p).wait_send()

            @pl.when(z > d)
            def _(d=d):
                left(d, p).wait_send()

        for k in range(1, NZ):
            o_copy(z, lax.rem(z + k, NZ), p).wait_send()
        return carry

    lax.fori_loop(0, heads, drain_a, 0)

    def drain_e(c, carry):
        @pl.when(z < NZ - 1)
        def _():
            right2(c).wait_send()
            m_right(c).wait_send()

        @pl.when(z > 0)
        def _():
            left2(c).wait_send()
            m_left(c).wait_send()

        return carry

    lax.fori_loop(0, n_col, drain_e, 0)
    for step in range(2):
        @pl.when(z < NZ - 1)
        def _(step=step):
            stat(step, 0).wait_send()

        @pl.when(z > 0)
        def _(step=step):
            stat(step, 1).wait_send()


def layer_call(hid, g1, g2, wq, wk, wv, wo, wg, wu, wd, kc, vc, lens, cos, sin):
    rows, width = hid.shape
    heads, hd = wq.shape[0], wq.shape[2]
    ff = wg.shape[1]
    per, half = rows // NZ, rows // 2
    n_col, n_red = ff // COL, width // RCOL
    n_grp = 9 if n_col % 9 == 0 else 1
    vm = pl.BlockSpec(memory_space=pltpu.VMEM)
    hbm = pl.BlockSpec(memory_space=pl.ANY)
    dma = pltpu.SemaphoreType.DMA
    lane_sum = pltpu.VMEM((NZ, heads, per, 3 * hd), F32)
    red = pltpu.VMEM((2, n_red, half, RCOL), F32)
    act = pltpu.VMEM((rows, width), BF16)
    return pl.pallas_call(
        layer_kernel,
        name='layer',
        out_shape=[pltpu.VMEM((rows, width), BF16), pltpu.VMEM(kc.shape, BF16), pltpu.VMEM(vc.shape, BF16)],
        in_specs=[hbm] * 15,
        out_specs=[vm, vm, vm],
        scratch_shapes=[
            act, pltpu.VMEM(g1.shape, g1.dtype), pltpu.VMEM(g2.shape, g2.dtype), pltpu.SMEM(lens.shape, jnp.int32), pltpu.VMEM(cos.shape, F32), pltpu.VMEM(sin.shape, F32),
            pltpu.VMEM((3, heads, width, hd), BF16),
            pltpu.VMEM(wo.shape, BF16), pltpu.VMEM(wg.shape, BF16), pltpu.VMEM(wu.shape, BF16), pltpu.VMEM(wd.shape, BF16),
            lane_sum, lane_sum, lane_sum,
            act, act,
            pltpu.VMEM((2, heads, per, hd), F32),
            pltpu.VMEM((n_red, rows, RCOL), F32),
            red, red, red,
            act,
            pltpu.VMEM((n_col, 2, half, 2 * COL), F32),
            pltpu.VMEM((n_col, half, 2 * COL), F32),
            pltpu.VMEM((n_col, half, 2 * COL), F32),
            pltpu.VMEM((rows, ff), BF16),
            pltpu.VMEM((2, 2, 8, 128), F32), pltpu.VMEM((2, 2, 8, 128), F32), pltpu.VMEM((2, 8, 128), F32),
            pltpu.VMEM((7, NZ, per, 128), F32),
            dma((6,)), dma((3, heads)), dma((2, heads)), dma((2,)), dma((2, n_grp)),
            dma((NZ, heads)), dma((NZ, heads)), dma((NZ, heads)), dma((NZ, heads)),
            dma((heads, NZ)), dma((heads, NZ)),
            dma((2, n_red)), dma((2, n_red)), dma((2, n_red)), dma((2, n_red)), dma((2, n_red)), dma((2, n_red)),
            dma((2, 2)), dma((2, 2)),
            dma((n_col,)), dma((n_col,)), dma((n_col,)), dma((n_col,)),
            dma((n_col,)), dma((n_col,)), dma((n_col,)), dma((n_col,)),
        ],
        compiler_params=pltpu.CompilerParams(collective_id=0, has_side_effects=True, vmem_limit_bytes=VMEM_KIB * 1024),
    )(hid, g1, g2, wq, wk, wv, wo, wg, wu, wd, kc, vc, lens, cos, sin)


VMEM_KIB = 49 * 1024


def solution(mesh):
    row_spec = P('dp', 'dm')
    cache_spec = P(('dp', 'dm'), None, 'tp', None)
    batch_spec = P(('dp', 'dm'))
    rope_spec = P(('dp', 'dm'), None)
    in_specs = (row_spec, P('dm', 'tp', None), P('dm', 'tp', None), P('dm', 'tp', None), P('tp', None, 'dm'), P('dm', 'tp'), P('dm', 'tp'), P('tp', 'dm'), P('dm'), P('dm'), cache_spec, cache_spec, batch_spec, rope_spec, rope_spec)
    out_specs = (row_spec, cache_spec, cache_spec)

    def local_layer(hidden, w_q, w_k, w_v, w_o, w_gate, w_up, w_down, norm_attn, norm_mlp, k_cache, v_cache, seq_lens, rope_cos, rope_sin):
        by_head = [w.transpose(1, 0, 2) for w in (w_q, w_k, w_v)]
        caches = [c.transpose(0, 2, 1, 3) for c in (k_cache, v_cache)]
        h_out, k_out, v_out = layer_call(hidden, norm_attn, norm_mlp, *by_head, w_o.reshape(-1, w_o.shape[-1]), w_gate, w_up, w_down, *caches, seq_lens, rope_cos, rope_sin)
        return h_out, k_out.transpose(0, 2, 1, 3), v_out.transpose(0, 2, 1, 3)

    return jax.shard_map(local_layer, mesh=mesh, in_specs=in_specs, out_specs=out_specs, check_vma=False)
```

```python
import jax
import jax.numpy as jnp
from jax import lax
from jax.experimental import pallas as pl
from jax.experimental.pallas import tpu as pltpu
from jax.sharding import PartitionSpec as P

EPS = 1e-6
MESH = pl.DeviceIdType.MESH
F32 = jnp.float32
BF16 = jnp.bfloat16
NZ = 4
A_LAG = 2
E_LAG = 2
COL = 384
RCOL = 256


def remote(src, dst, send_sem, recv_sem, **where):
    return pltpu.make_async_remote_copy(src_ref=src, dst_ref=dst, send_sem=send_sem, recv_sem=recv_sem, device_id=where, device_id_type=MESH)


def partner(tp, k):
    if k == 1:
        return tp + 1 - 2 * lax.rem(tp, 2)
    return lax.rem(tp + 2, 4)


def pack_rows(col):
    rows = col.shape[0]
    lane = lax.broadcasted_iota(jnp.int32, (rows, 128), 1)
    row = lax.broadcasted_iota(jnp.int32, (rows, 128), 0)
    packed = jnp.sum(jnp.where(lane == row, col, 0.0), axis=0, keepdims=True)
    return jnp.broadcast_to(packed, (8, 128))


def unpack_rows(tile, rows):
    lane = lax.broadcasted_iota(jnp.int32, (rows, 128), 1)
    row = lax.broadcasted_iota(jnp.int32, (rows, 128), 0)
    wide = jnp.broadcast_to(tile[0:1], (rows, 128))
    return jnp.sum(jnp.where(lane == row, wide, 0.0), axis=1, keepdims=True)


def layer_kernel(hid_h, g1_h, g2_h, wq, wk, wv, wo, wg, wu, wd, kc, vc, lens_h, cos_h, sin_h,
                 out, k_out, v_out,
                 hid, g1, g2, lens, cos, sin, wbuf, wo_b, wg_b, wu_b, wd_b,
                 part, rbuf, lbuf, x_buf, o_x, new_kv, red, r1, s_buf, r2, h_mid, pbuf, rbuf2, lbuf2, mbuf,
                 cum_in, cum_out, own_sq, fac,
                 s_sem, w_sem, c_sem, b_sem, g_sem, rs, rr, ls, lr, o_s, o_r, a_s, a_r, b_s, b_r, c_s, c_r,
                 q_s, q_r, rs2, rr2, ls2, lr2, mr_s, mr_r, ml_s, ml_r):
    z = lax.axis_index('dm')
    tp = lax.axis_index('tp')
    rows, width = hid.shape
    full = width * NZ
    heads = wq.shape[0]
    hd = wq.shape[2]
    per = rows // NZ
    half = rows // 2
    slots = kc.shape[2]
    ff = wg.shape[1]
    n_col = ff // COL
    n_grp = g_sem.shape[1]
    grp = ff // n_grp
    n_red = width // RCOL
    early = (n_col * 2 // 3) // 2 * 2
    core = lax.rem(tp, 2)
    sib, across = partner(tp, 1), partner(tp, 2)
    nxt, prv = lax.rem(z + 1, NZ), lax.rem(z + NZ - 1, NZ)

    small = [pltpu.make_async_copy(a, b, s_sem.at[i]) for i, (a, b) in enumerate(((hid_h, hid), (g1_h, g1), (g2_h, g2), (cos_h, cos), (sin_h, sin), (lens_h, lens)))]
    load_o = pltpu.make_async_copy(wo, wo_b, b_sem.at[0])
    load_d = pltpu.make_async_copy(wd, wd_b, b_sem.at[1])

    def load_w(i, h):
        return pltpu.make_async_copy((wq, wk, wv)[i].at[h], wbuf.at[i, h], w_sem.at[i, h])

    def load_c(i, h):
        return pltpu.make_async_copy((kc, vc)[i].at[:, h], (k_out, v_out)[i].at[:, h], c_sem.at[i, h])

    def load(i, g):
        src, dst = ((wg, wg_b), (wu, wu_b))[i]
        cols = pl.ds(pl.multiple_of(g * grp, COL), grp)
        return pltpu.make_async_copy(src.at[:, cols], dst.at[:, cols], g_sem.at[i, g])

    for cp in small:
        cp.start()
    for h in range(heads):
        for i in range(3):
            load_w(i, h).start()
        if h >= 2:
            load_c(0, h - 2).start()
            load_c(1, h - 2).start()
    for h in range(max(heads - 2, 0), heads):
        load_c(0, h).start()
        load_c(1, h).start()
    load_o.start()
    for g in range(n_grp):
        load(0, g).start()
        load(1, g).start()
    load_d.start()

    sem = pltpu.get_barrier_semaphore()
    for k in range(1, NZ):
        pl.semaphore_signal(sem, inc=1, device_id={'dm': lax.rem(z + k, NZ)}, device_id_type=MESH)
    for k in (1, 2):
        pl.semaphore_signal(sem, inc=1, device_id={'tp': partner(tp, k)}, device_id_type=MESH)

    for cp in small:
        cp.wait()

    def local_norm(x, gain, step):
        col = jnp.sum(x * x, axis=-1, keepdims=True)
        own_sq[step] = pack_rows(col)
        x_buf[...] = (x * lax.rsqrt(col / full + EPS) * gain).astype(BF16)

    def inv(tile):
        return lax.rsqrt(tile / full + EPS)

    def stat(step, side):
        return remote(cum_out.at[step, side], cum_in.at[step, side], q_s.at[step, side], q_r.at[step, side], dm=(nxt, prv)[side])

    def relay_stat(step, side):
        has_in = (z > 0) if side == 0 else (z < NZ - 1)
        has_out = (z < NZ - 1) if side == 0 else (z > 0)

        @pl.when(has_in)
        def _():
            stat(step, side).wait_recv()

        @pl.when(jnp.logical_not(has_in))
        def _():
            cum_in[step, side] = jnp.zeros((8, 128), F32)

        before, own = cum_in[step, side], own_sq[step]
        cum = before + own
        cum_out[step, side] = cum

        @pl.when(has_out)
        def _():
            stat(step, side).start()

        scale = inv(cum)
        put_fac(2 * side, scale / inv(own))
        put_fac(2 * side + 1, scale / inv(before))

    def put_fac(i, tile):
        wide = jnp.broadcast_to(unpack_rows(tile, rows), (rows, 128))
        for d in range(NZ):
            fac[i, d] = wide[d * per:(d + 1) * per]

    local_norm(hid[...].astype(F32), g1[...].astype(F32).reshape(1, width), 0)
    cos2 = jnp.concatenate([cos[...], cos[...]], axis=-1)
    sin2 = jnp.concatenate([-sin[...], sin[...]], axis=-1)

    @pl.when(z == 0)
    def _():
        rbuf[0] = jnp.zeros(rbuf.shape[1:], F32)

    @pl.when(z == NZ - 1)
    def _():
        lbuf[NZ - 1] = jnp.zeros(lbuf.shape[1:], F32)

    row = lax.broadcasted_iota(jnp.int32, (per, slots), 0)
    pos = lax.broadcasted_iota(jnp.int32, (per, slots), 1)
    length = jnp.zeros((per, slots), jnp.int32)
    for r in range(per):
        length = jnp.where(row == r, lens[r], length)
    at_len = pos == length
    seen = pos <= length

    pl.semaphore_wait(sem, NZ + 1)

    def right(d, p):
        return remote(part.at[d, p], rbuf.at[d, p], rs.at[d, p], rr.at[d, p], dm=nxt)

    def left(d, p):
        return remote(part.at[d, p], lbuf.at[d, p], ls.at[d, p], lr.at[d, p], dm=prv)

    def o_view(src, p):
        return o_x.at[pl.ds(pl.multiple_of(src * per, per), per), pl.ds(pl.multiple_of(p * hd, hd), hd)]

    def o_copy(src, to, p):
        return remote(o_view(src, p), o_view(src, p), o_s.at[p, to], o_r.at[p, src], dm=to)

    def thrice(i, d):
        f = fac[i, d]
        return jnp.concatenate([f, f, f], axis=1)

    def attend(h):
        y = part[z, h] * thrice(4, z) + (rbuf[z, h] * thrice(5, z) + lbuf[z, h] * thrice(6, z))
        q, k = y[:, 0:hd], y[:, hd:2 * hd]
        q = (q * cos2 + pltpu.roll(q, hd // 2, 1) * sin2).astype(BF16)
        k_new = (k * cos2 + pltpu.roll(k, hd // 2, 1) * sin2).astype(BF16).astype(F32)
        v_new = y[:, 2 * hd:].astype(BF16).astype(F32)
        new_kv[0, h] = k_new
        new_kv[1, h] = v_new
        load_c(0, h).wait()
        load_c(1, h).wait()
        s = jnp.zeros((per, slots), F32)
        for r in range(per):
            t = lax.dot_general(q, k_out[r, h], (((1,), (1,)), ((), ())), preferred_element_type=F32)
            s = jnp.where(row == r, t, s)
        s_new = jnp.sum(q.astype(F32) * k_new, axis=-1, keepdims=True)
        s = jnp.where(at_len, s_new, s) * (hd ** -0.5)
        s = jnp.where(seen, s, -1e30)
        e = jnp.exp(s - jnp.max(s, axis=-1, keepdims=True))
        prob = (e / jnp.sum(e, axis=-1, keepdims=True)).astype(BF16).astype(F32)
        p_new = jnp.sum(jnp.where(at_len, prob, 0.0), axis=-1, keepdims=True)
        p_old = jnp.where(at_len, 0.0, prob).astype(BF16)
        acc = jnp.zeros((per, hd), F32)
        for r in range(per):
            t = jnp.dot(p_old, v_out[r, h], preferred_element_type=F32)
            acc = jnp.where(row == r, t, acc)
        o_x[pl.ds(pl.multiple_of(z * per, per), per), pl.ds(pl.multiple_of(h * hd, hd), hd)] = (acc + p_new * v_new).astype(BF16)
        for k in (2, 1, 3):
            o_copy(z, lax.rem(z + k, NZ), h).start()

    def patch(lo, hi):
        where = lax.broadcasted_iota(jnp.int32, (slots, hd), 0)

        def body(h, carry):
            for r in range(per):
                hit = where == lens[r]
                for i, ref in enumerate((k_out, v_out)):
                    fresh = jnp.broadcast_to(new_kv[i, h, r:r + 1, :], (slots, hd))
                    ref[r, h] = jnp.where(hit, fresh, ref[r, h].astype(F32)).astype(BF16)
            return carry

        lax.fori_loop(lo, hi, body, 0)

    def a_slot(t, carry):
        @pl.when(t < heads)
        def _():
            for i in range(3):
                load_w(i, t).wait()
                y = jnp.dot(x_buf[...], wbuf[i, t], preferred_element_type=F32)
                for d in range(NZ):
                    part[d, t, :, i * hd:(i + 1) * hd] = y[d * per:(d + 1) * per]

        p = t - A_LAG * z

        @pl.when(p == 0)
        def _():
            relay_stat(0, 0)

        @pl.when((p >= 0) & (p < heads))
        def _():
            for d in (3, 2, 1):
                @pl.when((z > 0) & (z <= d))
                def _(d=d):
                    right(d, p).wait_recv()

                @pl.when((z > 0) & (z < d))
                def _(d=d):
                    part[d, p] = part[d, p] * thrice(0, d) + rbuf[d, p] * thrice(1, d)

                @pl.when(z < d)
                def _(d=d):
                    right(d, p).start()

        b = t - A_LAG * (NZ - 1 - z)

        @pl.when(b == 0)
        def _():
            relay_stat(0, 1)

        @pl.when((b >= 0) & (b < heads))
        def _():
            for d in (0, 1, 2):
                @pl.when((z < NZ - 1) & (z >= d))
                def _(d=d):
                    left(d, b).wait_recv()

                @pl.when((z < NZ - 1) & (z > d))
                def _(d=d):
                    part[d, b] = part[d, b] * thrice(2, d) + lbuf[d, b] * thrice(3, d)

                @pl.when(z > d)
                def _(d=d):
                    left(d, b).start()

        f = t - A_LAG * jnp.maximum(z, NZ - 1 - z)

        @pl.when(f == 0)
        def _():
            own = own_sq[0]
            scale = inv((cum_in[0, 0] + own) + cum_in[0, 1])
            put_fac(4, scale / inv(own))
            put_fac(5, scale / inv(cum_in[0, 0]))
            put_fac(6, scale / inv(cum_in[0, 1]))

        @pl.when((f >= 0) & (f < heads))
        def _():
            attend(f)

        return carry

    lax.fori_loop(0, heads + A_LAG * (NZ - 1), a_slot, 0)
    patch(0, heads // 2)

    def o_wait(p, carry):
        for k in (1, 3, 2):
            o_copy(lax.rem(z + k, NZ), lax.rem(z + k, NZ), p).wait_recv()
        return carry

    lax.fori_loop(0, heads, o_wait, 0)
    load_o.wait()

    mine = pl.ds(pl.multiple_of(core * half, half), half)
    other = pl.ds(pl.multiple_of((1 - core) * half, half), half)

    def reduce_tp(step, product, base, dst, meanwhile):
        def a_copy(j):
            return remote(red.at[j, other], r1.at[step, j], a_s.at[step, j], a_r.at[step, j], tp=sib)

        def b_copy(j):
            return remote(s_buf.at[step, j], r2.at[step, j], b_s.at[step, j], b_r.at[step, j], tp=across)

        def c_copy(j, part_rows):
            view = dst.at[part_rows, pl.ds(j * RCOL, RCOL)]
            return remote(view, view, c_s.at[step, j], c_r.at[step, j], tp=sib)

        for j in range(n_red):
            red[j] = product(j)
            a_copy(j).start()
        for j in range(n_red):
            a_copy(j).wait_recv()
            s_buf[step, j] = red[j, mine] + r1[step, j]
            b_copy(j).start()
        meanwhile()
        for j in range(n_red):
            b_copy(j).wait_recv()
            total = (s_buf[step, j] + r2[step, j]).astype(BF16)
            cols = pl.ds(j * RCOL, RCOL)
            dst[mine, cols] = (base[mine, cols].astype(F32) + total.astype(F32)).astype(BF16)
            c_copy(j, mine).start()
        for j in range(n_red):
            c_copy(j, other).wait_recv()
        for j in range(n_red):
            a_copy(j).wait_send()
            b_copy(j).wait_send()
            c_copy(j, mine).wait_send()

    reduce_tp(0, lambda j: jnp.dot(o_x[...], wo_b[:, j * RCOL:(j + 1) * RCOL], preferred_element_type=F32), hid, h_mid, lambda: patch(heads // 2, heads))
    local_norm(h_mid[...].astype(F32), g2[...].astype(F32).reshape(1, width), 1)

    def right2(c):
        return remote(pbuf.at[c, 1], rbuf2.at[c], rs2.at[c], rr2.at[c], dm=nxt)

    def left2(c):
        return remote(pbuf.at[c, 0], lbuf2.at[c], ls2.at[c], lr2.at[c], dm=prv)

    low, high = pl.ds(0, half), pl.ds(half, half)

    def cols_of(c):
        return pl.ds(pl.multiple_of(c * COL, COL), COL)

    def m_left(c):
        view = mbuf.at[high, cols_of(c)]
        return remote(view, view, mr_s.at[c], mr_r.at[c], dm=prv)

    def m_right(c):
        view = mbuf.at[low, cols_of(c)]
        return remote(view, view, ml_s.at[c], ml_r.at[c], dm=nxt)

    def gated(a):
        g, u = a[:, :COL], a[:, COL:]
        return (g * (1.0 / (1.0 + jnp.exp(-g))) * u).astype(BF16)

    def wide(i, first):
        f = jnp.concatenate([fac[i, first], fac[i, first + 1]], axis=0)
        return jnp.concatenate([f] * (2 * COL // 128), axis=1)

    def e_slot(t, carry):
        @pl.when(t < n_col)
        def _():
            per_grp = n_col // n_grp

            @pl.when(lax.rem(t, per_grp) == 0)
            def _():
                load(0, t // per_grp).wait()
                load(1, t // per_grp).wait()

            g = jnp.dot(x_buf[...], wg_b[:, cols_of(t)], preferred_element_type=F32)
            u = jnp.dot(x_buf[...], wu_b[:, cols_of(t)], preferred_element_type=F32)
            pbuf[t, 0, :, 0:COL] = g[:half]
            pbuf[t, 1, :, 0:COL] = g[half:]
            pbuf[t, 0, :, COL:] = u[:half]
            pbuf[t, 1, :, COL:] = u[half:]

        c = t - E_LAG * z

        @pl.when(c == 0)
        def _():
            relay_stat(1, 0)

        @pl.when((c >= 0) & (c < n_col))
        def _():
            @pl.when(z > 0)
            def _():
                right2(c).wait_recv()
                pbuf[c, 1] = pbuf[c, 1] * wide(0, 2) + rbuf2[c] * wide(1, 2)

            @pl.when(z < NZ - 1)
            def _():
                right2(c).start()

            @pl.when(z == NZ - 1)
            def _():
                mbuf[high, cols_of(c)] = gated(pbuf[c, 1])
                m_left(c).start()

        b = t - E_LAG * (NZ - 1 - z)

        @pl.when(b == 0)
        def _():
            relay_stat(1, 1)

        @pl.when((b >= 0) & (b < n_col))
        def _():
            @pl.when(z < NZ - 1)
            def _():
                left2(b).wait_recv()
                pbuf[b, 0] = pbuf[b, 0] * wide(2, 0) + lbuf2[b] * wide(3, 0)

            @pl.when(z > 0)
            def _():
                left2(b).start()

            @pl.when(z == 0)
            def _():
                mbuf[low, cols_of(b)] = gated(pbuf[b, 0])
                m_right(b).start()

        e = t - E_LAG * (2 * NZ - 2 - z)

        @pl.when((e >= 0) & (e < n_col) & (z < NZ - 1))
        def _():
            m_left(e).wait_recv()

            @pl.when(z > 0)
            def _():
                m_left(e).start()

        f = t - E_LAG * (NZ - 1 + z)

        @pl.when((f >= 0) & (f < n_col) & (z > 0))
        def _():
            m_right(f).wait_recv()

            @pl.when(z < NZ - 1)
            def _():
                m_right(f).start()

        w = t - (early + E_LAG * (2 * NZ - 2))

        @pl.when(w == 0)
        def _():
            load_d.wait()

        @pl.when((w >= 0) & (w < n_red))
        def _():
            red[w] = jnp.dot(mbuf[:, 0:early * COL], wd_b[0:early * COL, pl.ds(pl.multiple_of(w * RCOL, RCOL), RCOL)], preferred_element_type=F32)

        return carry

    lax.fori_loop(0, max(n_col, early + n_red) + E_LAG * (2 * NZ - 2), e_slot, 0)
    reduce_tp(1, lambda j: red[j] + jnp.dot(mbuf[:, early * COL:], wd_b[early * COL:, j * RCOL:(j + 1) * RCOL], preferred_element_type=F32), h_mid, out, lambda: None)

    def drain_a(p, carry):
        for d in range(NZ):
            @pl.when(z < d)
            def _(d=d):
                right(d, p).wait_send()

            @pl.when(z > d)
            def _(d=d):
                left(d, p).wait_send()

        for k in range(1, NZ):
            o_copy(z, lax.rem(z + k, NZ), p).wait_send()
        return carry

    lax.fori_loop(0, heads, drain_a, 0)

    def drain_e(c, carry):
        @pl.when(z < NZ - 1)
        def _():
            right2(c).wait_send()
            m_right(c).wait_send()

        @pl.when(z > 0)
        def _():
            left2(c).wait_send()
            m_left(c).wait_send()

        return carry

    lax.fori_loop(0, n_col, drain_e, 0)
    for step in range(2):
        @pl.when(z < NZ - 1)
        def _(step=step):
            stat(step, 0).wait_send()

        @pl.when(z > 0)
        def _(step=step):
            stat(step, 1).wait_send()


def layer_call(hid, g1, g2, wq, wk, wv, wo, wg, wu, wd, kc, vc, lens, cos, sin):
    rows, width = hid.shape
    heads, hd = wq.shape[0], wq.shape[2]
    ff = wg.shape[1]
    per, half = rows // NZ, rows // 2
    n_col, n_red = ff // COL, width // RCOL
    n_grp = 9 if n_col % 9 == 0 else 1
    vm = pl.BlockSpec(memory_space=pltpu.VMEM)
    hbm = pl.BlockSpec(memory_space=pl.ANY)
    dma = pltpu.SemaphoreType.DMA
    lane_sum = pltpu.VMEM((NZ, heads, per, 3 * hd), F32)
    red = pltpu.VMEM((2, n_red, half, RCOL), F32)
    act = pltpu.VMEM((rows, width), BF16)
    return pl.pallas_call(
        layer_kernel,
        name='layer',
        out_shape=[pltpu.VMEM((rows, width), BF16), pltpu.VMEM(kc.shape, BF16), pltpu.VMEM(vc.shape, BF16)],
        in_specs=[hbm] * 15,
        out_specs=[vm, vm, vm],
        scratch_shapes=[
            act, pltpu.VMEM(g1.shape, g1.dtype), pltpu.VMEM(g2.shape, g2.dtype), pltpu.SMEM(lens.shape, jnp.int32), pltpu.VMEM(cos.shape, F32), pltpu.VMEM(sin.shape, F32),
            pltpu.VMEM((3, heads, width, hd), BF16),
            pltpu.VMEM(wo.shape, BF16), pltpu.VMEM(wg.shape, BF16), pltpu.VMEM(wu.shape, BF16), pltpu.VMEM(wd.shape, BF16),
            lane_sum, lane_sum, lane_sum,
            act, act,
            pltpu.VMEM((2, heads, per, hd), F32),
            pltpu.VMEM((n_red, rows, RCOL), F32),
            red, red, red,
            act,
            pltpu.VMEM((n_col, 2, half, 2 * COL), F32),
            pltpu.VMEM((n_col, half, 2 * COL), F32),
            pltpu.VMEM((n_col, half, 2 * COL), F32),
            pltpu.VMEM((rows, ff), BF16),
            pltpu.VMEM((2, 2, 8, 128), F32), pltpu.VMEM((2, 2, 8, 128), F32), pltpu.VMEM((2, 8, 128), F32),
            pltpu.VMEM((7, NZ, per, 128), F32),
            dma((6,)), dma((3, heads)), dma((2, heads)), dma((2,)), dma((2, n_grp)),
            dma((NZ, heads)), dma((NZ, heads)), dma((NZ, heads)), dma((NZ, heads)),
            dma((heads, NZ)), dma((heads, NZ)),
            dma((2, n_red)), dma((2, n_red)), dma((2, n_red)), dma((2, n_red)), dma((2, n_red)), dma((2, n_red)),
            dma((2, 2)), dma((2, 2)),
            dma((n_col,)), dma((n_col,)), dma((n_col,)), dma((n_col,)),
            dma((n_col,)), dma((n_col,)), dma((n_col,)), dma((n_col,)),
        ],
        compiler_params=pltpu.CompilerParams(collective_id=0, has_side_effects=True, vmem_limit_bytes=VMEM_KIB * 1024),
    )(hid, g1, g2, wq, wk, wv, wo, wg, wu, wd, kc, vc, lens, cos, sin)


VMEM_KIB = 49 * 1024


def solution(mesh):
    row_spec = P('dp', 'dm')
    cache_spec = P(('dp', 'dm'), None, 'tp', None)
    batch_spec = P(('dp', 'dm'))
    rope_spec = P(('dp', 'dm'), None)
    in_specs = (row_spec, P('dm', 'tp', None), P('dm', 'tp', None), P('dm', 'tp', None), P('tp', None, 'dm'), P('dm', 'tp'), P('dm', 'tp'), P('tp', 'dm'), P('dm'), P('dm'), cache_spec, cache_spec, batch_spec, rope_spec, rope_spec)
    out_specs = (row_spec, cache_spec, cache_spec)

    def local_layer(hidden, w_q, w_k, w_v, w_o, w_gate, w_up, w_down, norm_attn, norm_mlp, k_cache, v_cache, seq_lens, rope_cos, rope_sin):
        by_head = [w.transpose(1, 0, 2) for w in (w_q, w_k, w_v)]
        caches = [c.transpose(0, 2, 1, 3) for c in (k_cache, v_cache)]
        h_out, k_out, v_out = layer_call(hidden, norm_attn, norm_mlp, *by_head, w_o.reshape(-1, w_o.shape[-1]), w_gate, w_up, w_down, *caches, seq_lens, rope_cos, rope_sin)
        return h_out, k_out.transpose(0, 2, 1, 3), v_out.transpose(0, 2, 1, 3)

    return jax.shard_map(local_layer, mesh=mesh, in_specs=in_specs, out_specs=out_specs, check_vma=False)
```

```python
import jax
import jax.numpy as jnp
from jax import lax
from jax.experimental import pallas as pl
from jax.experimental.pallas import tpu as pltpu
from jax.sharding import PartitionSpec as P

EPS = 1e-6
MESH = pl.DeviceIdType.MESH
F32 = jnp.float32
BF16 = jnp.bfloat16
NZ = 4
NP = 8
A_LAG = 2
E_LAG = 3
COL = 384
DIRECT = 4


def remote(src, dst, send_sem, recv_sem, **where):
    return pltpu.make_async_remote_copy(src_ref=src, dst_ref=dst, send_sem=send_sem, recv_sem=recv_sem, device_id=where, device_id_type=MESH)


def partner(tp, k):
    if k == 1:
        return tp + 1 - 2 * lax.rem(tp, 2)
    return lax.rem(tp + 2, 4)


def pack_rows(col):
    rows = col.shape[0]
    lane = lax.broadcasted_iota(jnp.int32, (rows, 128), 1)
    row = lax.broadcasted_iota(jnp.int32, (rows, 128), 0)
    packed = jnp.sum(jnp.where(lane == row, col, 0.0), axis=0, keepdims=True)
    return jnp.broadcast_to(packed, (8, 128))


def unpack_rows(tile, rows):
    lane = lax.broadcasted_iota(jnp.int32, (rows, 128), 1)
    row = lax.broadcasted_iota(jnp.int32, (rows, 128), 0)
    wide = jnp.broadcast_to(tile[0:1], (rows, 128))
    return jnp.sum(jnp.where(lane == row, wide, 0.0), axis=1, keepdims=True)


def layer_kernel(hid_h, g1_h, g2_h, wq, wk, wv, wo, wg, wu, wd, kc, vc, lens_h, cos_h, sin_h,
                 out, k_out, v_out,
                 hid, g1, g2, lens, cos, sin, hid_p, len_v, rope, wbuf, wo_b, wg_b, wu_b, wd_b,
                 part, rbuf, lbuf, x_buf, o_x, o_cat, new_kv, red, r1, s_buf, r2, h_mid, h_fin, pbuf, rbuf2, lbuf2, mbuf,
                 cum_in, cum_out, own_sq, fac,
                 s_sem, w_sem, c_sem, b_sem, g_sem, rs, rr, ls, lr, o_s, o_r, a_s, a_r, b_s, b_r, c_s, c_r,
                 q_s, q_r, rs2, rr2, ls2, lr2, mr_s, mr_r, ml_s, ml_r, far_s):
    z = lax.axis_index('dm')
    tp = lax.axis_index('tp')
    rows, width = hid.shape
    full = width * NZ
    heads = wq.shape[0]
    hd = wq.shape[2]
    per = rows // NZ
    half = rows // 2
    side = half // 2
    slots = kc.shape[2]
    ff = wg.shape[1]
    n_pair = heads // 2
    n_a = 2 * n_pair
    n_col = ff // COL
    second = max(n_col, 8)
    n_e = second + n_col
    trip = E_LAG * (NZ - 1)
    n_grp = g_sem.shape[1]
    n_red = red.shape[1]
    rcol = width // n_red
    early = n_col * 2 // 3
    direct_from = n_e - DIRECT
    core = lax.rem(tp, 2)
    sib, across = partner(tp, 1), partner(tp, 2)
    nxt, prv = lax.rem(z + 1, NZ), lax.rem(z + NZ - 1, NZ)

    small = [pltpu.make_async_copy(a, b, s_sem.at[i]) for i, (a, b) in enumerate(((hid_h, hid), (g1_h, g1), (g2_h, g2), (cos_h, cos), (sin_h, sin), (lens_h, lens)))]
    load_o = pltpu.make_async_copy(wo, wo_b, b_sem.at[0])
    load_d = pltpu.make_async_copy(wd, wd_b, b_sem.at[1])

    def load_w(i, h):
        return pltpu.make_async_copy((wq, wk, wv)[i].at[h], wbuf.at[i, h], w_sem.at[i, h])

    def load_c(i, h):
        return pltpu.make_async_copy((kc, vc)[i].at[:, h], (k_out, v_out)[i].at[:, h], c_sem.at[i, h])

    def load(i, g):
        src, dst = ((wg, wg_b), (wu, wu_b))[i]
        cols = pl.ds(pl.multiple_of(g * COL, COL), COL)
        return pltpu.make_async_copy(src.at[:, cols], dst.at[:, cols], g_sem.at[i, g])

    for cp in small:
        cp.start()
    for h in range(heads):
        for i in range(3):
            load_w(i, h).start()
        if h >= 2:
            load_c(0, h - 2).start()
            load_c(1, h - 2).start()
    for h in range(max(heads - 2, 0), heads):
        load_c(0, h).start()
        load_c(1, h).start()
    load_o.start()
    for g in range(n_grp):
        load(0, g).start()
        load(1, g).start()
    load_d.start()

    sem = pltpu.get_barrier_semaphore()
    for k in range(1, NZ):
        pl.semaphore_signal(sem, inc=1, device_id={'dm': lax.rem(z + k, NZ)}, device_id_type=MESH)
    for k in (1, 2):
        pl.semaphore_signal(sem, inc=1, device_id={'tp': partner(tp, k)}, device_id_type=MESH)

    for cp in small:
        cp.wait()

    def inv(tile):
        return lax.rsqrt(tile / full + EPS)

    def local_norm(x, gain, step, lo):
        col = jnp.sum(x * x, axis=-1, keepdims=True)
        own_sq[step] = pack_rows(col)
        x_buf[lo:lo + x.shape[0]] = (x * lax.rsqrt(col / full + EPS) * gain).astype(BF16)

    def place(b, d):
        return d * per + b * NP

    x0 = hid[...].astype(F32)
    x0 = jnp.concatenate([x0[place(b, d):place(b, d) + NP] for b in range(2) for d in range(NZ)], axis=0)
    hid_p[...] = x0.astype(BF16)
    local_norm(x0, g1[...].astype(F32).reshape(1, width), 0, 0)
    cs, sn = cos[...], sin[...]
    row = lax.broadcasted_iota(jnp.int32, (NP, slots), 0)
    pos = lax.broadcasted_iota(jnp.int32, (NP, slots), 1)
    for b in range(2):
        part_cs, part_sn = cs[b * NP:(b + 1) * NP], sn[b * NP:(b + 1) * NP]
        rope[0, b] = jnp.concatenate([part_cs, part_cs], axis=-1)
        rope[1, b] = jnp.concatenate([-part_sn, part_sn], axis=-1)
        length = jnp.zeros((NP, slots), jnp.int32)
        for r in range(NP):
            length = jnp.where(row == r, lens[b * NP + r], length)
        len_v[b] = length

    def stat(step, way):
        return remote(cum_out.at[step, way], cum_in.at[step, way], q_s.at[step, way], q_r.at[step, way], dm=(nxt, prv)[way])

    def put_fac(i, tile, halves):
        n = len(halves) * half
        wide = jnp.broadcast_to(unpack_rows(tile, n), (n, 128))
        for k, b in enumerate(halves):
            for d in range(NZ):
                lo = (k * NZ + d) * NP
                fac[i, b, d] = wide[lo:lo + NP]

    def relay_stat(step, way, halves):
        has_in = (z > 0) if way == 0 else (z < NZ - 1)
        has_out = (z < NZ - 1) if way == 0 else (z > 0)

        @pl.when(has_in)
        def _():
            stat(step, way).wait_recv()

        @pl.when(jnp.logical_not(has_in))
        def _():
            cum_in[step, way] = jnp.zeros((8, 128), F32)

        before, own = cum_in[step, way], own_sq[step]
        cum = before + own
        cum_out[step, way] = cum

        @pl.when(has_out)
        def _():
            stat(step, way).start()

        scale = inv(cum)
        put_fac(2 * way, scale / inv(own), halves)
        put_fac(2 * way + 1, scale / inv(before), halves)

    @pl.when(z == 0)
    def _():
        rbuf[0] = jnp.zeros(rbuf.shape[1:], F32)

    @pl.when(z == NZ - 1)
    def _():
        lbuf[NZ - 1] = jnp.zeros(lbuf.shape[1:], F32)

    pl.semaphore_wait(sem, NZ + 1)

    def right(d, p):
        return remote(part.at[d, p], rbuf.at[d, p], rs.at[d, p], rr.at[d, p], dm=nxt)

    def left(d, p):
        return remote(part.at[d, p], lbuf.at[d, p], ls.at[d, p], lr.at[d, p], dm=prv)

    def split(it):
        b = it // n_pair
        return b, it - b * n_pair

    def o_copy(src, to, it):
        b, p = split(it)
        view = o_x.at[b, src, pl.ds(2 * p, 2)]
        return remote(view, view, o_s.at[it, to], o_r.at[it, src], dm=to)

    def repeat(f, n):
        return jnp.concatenate([f] * n, axis=1)

    def attend(it):
        b, p = split(it)
        y6 = part[z, it] * repeat(fac[4, b, z], 6) + (rbuf[z, it] * repeat(fac[5, b, z], 6) + lbuf[z, it] * repeat(fac[6, b, z], 6))
        cos2, sin2 = rope[0, b], rope[1, b]
        at_len = pos == len_v[b]
        seen = pos <= len_v[b]
        for e in range(2):
            h = 2 * p + e
            y = y6[:, e * 3 * hd:(e + 1) * 3 * hd]
            q, k = y[:, 0:hd], y[:, hd:2 * hd]
            q = (q * cos2 + pltpu.roll(q, hd // 2, 1) * sin2).astype(BF16)
            k_new = (k * cos2 + pltpu.roll(k, hd // 2, 1) * sin2).astype(BF16).astype(F32)
            v_new = y[:, 2 * hd:].astype(BF16).astype(F32)
            new_kv[0, h, b] = k_new
            new_kv[1, h, b] = v_new

            @pl.when(b == 0)
            def _(h=h):
                load_c(0, h).wait()
                load_c(1, h).wait()

            s = jnp.zeros((NP, slots), F32)
            for r in range(NP):
                t = lax.dot_general(q, k_out[b * NP + r, h], (((1,), (1,)), ((), ())), preferred_element_type=F32)
                s = jnp.where(row == r, t, s)
            s_new = jnp.sum(q.astype(F32) * k_new, axis=-1, keepdims=True)
            s = jnp.where(at_len, s_new, s) * (hd ** -0.5)
            s = jnp.where(seen, s, -1e30)
            ex = jnp.exp(s - jnp.max(s, axis=-1, keepdims=True))
            prob = (ex / jnp.sum(ex, axis=-1, keepdims=True)).astype(BF16).astype(F32)
            p_new = jnp.sum(jnp.where(at_len, prob, 0.0), axis=-1, keepdims=True)
            p_old = jnp.where(at_len, 0.0, prob).astype(BF16)
            acc = jnp.zeros((NP, hd), F32)
            for r in range(NP):
                t = jnp.dot(p_old, v_out[b * NP + r, h], preferred_element_type=F32)
                acc = jnp.where(row == r, t, acc)
            o_x[b, z, h] = (acc + p_new * v_new).astype(BF16)
        for k in (2, 1, 3):
            o_copy(z, lax.rem(z + k, NZ), it).start()

    where = lax.broadcasted_iota(jnp.int32, (slots, hd), 0)

    def patch(h, b):
        for r in range(NP):
            hit = where == lens[b * NP + r]
            for i, ref in enumerate((k_out, v_out)):
                fresh = jnp.broadcast_to(new_kv[i, h, b, r:r + 1, :], (slots, hd))
                ref[b * NP + r, h] = jnp.where(hit, fresh, ref[b * NP + r, h].astype(F32)).astype(BF16)

    mine = pl.ds(pl.multiple_of(core * side, side), side)
    other = pl.ds(pl.multiple_of((1 - core) * side, side), side)

    def a_copy(key, j):
        return remote(red.at[key, j, other], r1.at[key, j], a_s.at[key, j], a_r.at[key, j], tp=sib)

    def b_copy(key, j):
        return remote(s_buf.at[key, j], r2.at[key, j], b_s.at[key, j], b_r.at[key, j], tp=across)

    def c_copy(key, j, who):
        view = (h_mid, h_fin)[key // 2].at[key % 2, j, pl.ds(pl.multiple_of(who * side, side), side)]
        return remote(view, view, c_s.at[key, j], c_r.at[key, j], tp=sib)

    def o_gather(b):
        def wait(p, carry):
            it = b * n_pair + p
            for k in (1, 3, 2):
                o_copy(lax.rem(z + k, NZ), lax.rem(z + k, NZ), it).wait_recv()
            return carry

        lax.fori_loop(0, n_pair, wait, 0)
        o_cat[...] = jnp.concatenate([jnp.concatenate([o_x[b, d, h].astype(F32) for h in range(heads)], axis=1) for d in range(NZ)], axis=0).astype(BF16)

    def o_product(b, j):
        red[b, j] = jnp.dot(o_cat[...], wo_b[:, j * rcol:(j + 1) * rcol], preferred_element_type=F32)
        a_copy(b, j).start()

    def m_rows(b):
        return pl.ds(b * half, half)

    def stage_b(key):
        for j in range(n_red):
            a_copy(key, j).wait_recv()
            s_buf[key, j] = red[key, j, mine] + r1[key, j]
            b_copy(key, j).start()

    def stage_c(key):
        b = key % 2
        for j in range(n_red):
            b_copy(key, j).wait_recv()
            total = (s_buf[key, j] + r2[key, j]).astype(BF16).astype(F32)
            if key < 2:
                base = hid_p[pl.ds(pl.multiple_of(b * half + core * side, side), side), pl.ds(j * rcol, rcol)]
                h_mid[b, j, mine] = (base.astype(F32) + total).astype(BF16)
            else:
                h_fin[b, j, mine] = (h_mid[b, j, mine].astype(F32) + total).astype(BF16)
            c_copy(key, j, core).start()

    def stage_d(key):
        for j in range(n_red):
            c_copy(key, j, 1 - core).wait_recv()
        if key < 2:
            x = jnp.concatenate([h_mid[key, j].astype(F32) for j in range(n_red)], axis=1)
            local_norm(x, g2[...].astype(F32).reshape(1, width), 1 + key, key * half)

    def a_slot(t, carry):
        @pl.when(t < n_pair)
        def _():
            for e in range(2):
                h = 2 * t + e
                for i in range(3):
                    load_w(i, h).wait()
                    y = jnp.dot(x_buf[...], wbuf[i, h], preferred_element_type=F32)
                    for b in range(2):
                        for d in range(NZ):
                            lo = (b * NZ + d) * NP
                            part[d, b * n_pair + t, :, (3 * e + i) * hd:(3 * e + i + 1) * hd] = y[lo:lo + NP]

        p = t - A_LAG * z

        @pl.when(p == 0)
        def _():
            relay_stat(0, 0, (0, 1))

        @pl.when((p >= 0) & (p < n_a))
        def _():
            b = p // n_pair
            for d in (3, 2, 1):
                @pl.when((z > 0) & (z <= d))
                def _(d=d):
                    right(d, p).wait_recv()

                @pl.when((z > 0) & (z < d))
                def _(d=d):
                    part[d, p] = part[d, p] * repeat(fac[0, b, d], 6) + rbuf[d, p] * repeat(fac[1, b, d], 6)

                @pl.when(z < d)
                def _(d=d):
                    right(d, p).start()

        q = t - A_LAG * (NZ - 1 - z)

        @pl.when(q == 0)
        def _():
            relay_stat(0, 1, (0, 1))

        @pl.when((q >= 0) & (q < n_a))
        def _():
            b = q // n_pair
            for d in (0, 1, 2):
                @pl.when((z < NZ - 1) & (z >= d))
                def _(d=d):
                    left(d, q).wait_recv()

                @pl.when((z < NZ - 1) & (z > d))
                def _(d=d):
                    part[d, q] = part[d, q] * repeat(fac[2, b, d], 6) + lbuf[d, q] * repeat(fac[3, b, d], 6)

                @pl.when(z > d)
                def _(d=d):
                    left(d, q).start()

        f = t - A_LAG * jnp.maximum(z, NZ - 1 - z)

        @pl.when(f == 0)
        def _():
            own = own_sq[0]
            scale = inv((cum_in[0, 0] + own) + cum_in[0, 1])
            put_fac(4, scale / inv(own), (0, 1))
            put_fac(5, scale / inv(cum_in[0, 0]), (0, 1))
            put_fac(6, scale / inv(cum_in[0, 1]), (0, 1))

        @pl.when((f >= 0) & (f < n_a))
        def _():
            attend(f)

        o_at = n_pair - 1 + A_LAG * (NZ - 1) + 2

        @pl.when(t == o_at)
        def _():
            load_o.wait()
            o_gather(0)
            for j in range(n_red):
                o_product(0, j)

        @pl.when(t == o_at + 1)
        def _():
            stage_b(0)

        return carry

    a_end = max(n_a + A_LAG * (NZ - 1), n_pair + A_LAG * (NZ - 1) + 3)
    lax.fori_loop(0, a_end, a_slot, 0)

    def patch_x(h, carry):
        patch(h, 0)
        return carry

    lax.fori_loop(0, heads, patch_x, 0)
    stage_c(0)
    stage_d(0)

    def right2(c):
        return remote(pbuf.at[c, 1], rbuf2.at[c], rs2.at[c], rr2.at[c], dm=nxt)

    def left2(c):
        return remote(pbuf.at[c, 0], lbuf2.at[c], ls2.at[c], lr2.at[c], dm=prv)

    def valid(c):
        return ((c >= 0) & (c < n_col)) | ((c >= second) & (c < n_e))

    def half_of(c):
        b = c // second
        return b, c - b * second

    def m_view(c, high):
        b, k = half_of(c)
        return mbuf.at[pl.ds(pl.multiple_of(b * half + high * side, side), side), pl.ds(pl.multiple_of(k * COL, COL), COL)]

    def m_left(c):
        return remote(m_view(c, 1), m_view(c, 1), mr_s.at[c], mr_r.at[c], dm=prv)

    def m_right(c):
        return remote(m_view(c, 0), m_view(c, 0), ml_s.at[c], ml_r.at[c], dm=nxt)

    def m_far(c, high, k):
        to = (NZ - 1 - k) if high else k
        recv = mr_r if high else ml_r
        return remote(m_view(c, high), m_view(c, high), far_s.at[high, c - direct_from, k - 2], recv.at[c], dm=to)

    def gated(a):
        g, u = a[:, :COL], a[:, COL:]
        return (g * (1.0 / (1.0 + jnp.exp(-g))) * u).astype(BF16)

    def wide(i, b, first):
        f = jnp.concatenate([fac[i, b, first], fac[i, b, first + 1]], axis=0)
        return repeat(f, 2 * COL // 128)

    def finish(c, high):
        b, k = half_of(c)
        mbuf[pl.ds(pl.multiple_of(b * half + high * side, side), side), pl.ds(pl.multiple_of(k * COL, COL), COL)] = gated(pbuf[c, high])

        @pl.when(c >= direct_from)
        def _():
            m_far(c, high, 3).start()
            m_far(c, high, 2).start()

        (m_left if high else m_right)(c).start()

    def e_slot(t, carry):
        @pl.when(valid(t))
        def _():
            b, k = half_of(t)

            @pl.when(b == 0)
            def _():
                load(0, k).wait()
                load(1, k).wait()

            cols = pl.ds(pl.multiple_of(k * COL, COL), COL)
            x = x_buf[pl.ds(pl.multiple_of(b * half, half), half), :]
            g = jnp.dot(x, wg_b[:, cols], preferred_element_type=F32)
            u = jnp.dot(x, wu_b[:, cols], preferred_element_type=F32)
            for s in range(2):
                pbuf[t, s, :, 0:COL] = g[s * side:(s + 1) * side]
                pbuf[t, s, :, COL:] = u[s * side:(s + 1) * side]

        c = t - E_LAG * z
        for step, first in ((1, 0), (2, second)):
            @pl.when(c == first)
            def _(step=step):
                relay_stat(step, 0, (step - 1,))

        @pl.when(valid(c))
        def _():
            b = c // second

            @pl.when(z > 0)
            def _():
                right2(c).wait_recv()
                pbuf[c, 1] = pbuf[c, 1] * wide(0, b, 2) + rbuf2[c] * wide(1, b, 2)

            @pl.when(z < NZ - 1)
            def _():
                right2(c).start()

            @pl.when(z == NZ - 1)
            def _():
                finish(c, 1)

        d = t - E_LAG * (NZ - 1 - z)
        for step, first in ((1, 0), (2, second)):
            @pl.when(d == first)
            def _(step=step):
                relay_stat(step, 1, (step - 1,))

        @pl.when(valid(d))
        def _():
            b = d // second

            @pl.when(z < NZ - 1)
            def _():
                left2(d).wait_recv()
                pbuf[d, 0] = pbuf[d, 0] * wide(2, b, 0) + lbuf2[d] * wide(3, b, 0)

            @pl.when(z > 0)
            def _():
                left2(d).start()

            @pl.when(z == 0)
            def _():
                finish(d, 0)

        e = t - E_LAG * (2 * NZ - 2 - z)

        @pl.when(valid(e) & (z < NZ - 1))
        def _():
            m_left(e).wait_recv()

            @pl.when((z > 0) & (e < direct_from))
            def _():
                m_left(e).start()

        f = t - E_LAG * (NZ - 1 + z)

        @pl.when(valid(f) & (z > 0))
        def _():
            m_right(f).wait_recv()

            @pl.when((z < NZ - 1) & (f < direct_from))
            def _():
                m_right(f).start()

        @pl.when(t == 1)
        def _():
            o_gather(1)
            for j in range(n_red):
                o_product(1, j)

        @pl.when(t == 2)
        def _():
            stage_b(1)

        @pl.when(t == 5)
        def _():
            stage_c(1)

        @pl.when(t == 7)
        def _():
            stage_d(1)

        @pl.when((t >= n_e) & (t < n_e + heads))
        def _():
            patch(t - n_e, 1)

        down = n_col + 2 * trip
        for j in range(n_red):
            @pl.when(t == down + j)
            def _(j=j):
                if j == 0:
                    load_d.wait()
                red[2, j] = jnp.dot(mbuf[m_rows(0), :], wd_b[:, j * rcol:(j + 1) * rcol], preferred_element_type=F32)
                a_copy(2, j).start()

        @pl.when(t == down + 2)
        def _():
            stage_b(2)

        @pl.when(t == down + 5)
        def _():
            stage_c(2)

        @pl.when(t == down + 7)
        def _():
            stage_d(2)

        late = second + early + 2 * trip
        for j in range(n_red):
            @pl.when(t == late + j)
            def _(j=j):
                red[3, j] = jnp.dot(mbuf[m_rows(1), 0:early * COL], wd_b[0:early * COL, j * rcol:(j + 1) * rcol], preferred_element_type=F32)

        return carry

    lax.fori_loop(0, max(n_e + 2 * trip, second + early + n_red + 2 * trip, n_e + heads, n_col + 2 * trip + 8), e_slot, 0)
    for j in range(n_red):
        red[3, j] = red[3, j] + jnp.dot(mbuf[m_rows(1), early * COL:], wd_b[early * COL:, j * rcol:(j + 1) * rcol], preferred_element_type=F32)
        a_copy(3, j).start()
    stage_b(3)

    def drain_a(p, carry):
        for d in range(NZ):
            @pl.when(z < d)
            def _(d=d):
                right(d, p).wait_send()

            @pl.when(z > d)
            def _(d=d):
                left(d, p).wait_send()

        for k in range(1, NZ):
            o_copy(z, lax.rem(z + k, NZ), p).wait_send()
        return carry

    lax.fori_loop(0, n_a, drain_a, 0)

    def drain_e(c, carry):
        @pl.when(valid(c))
        def _():
            @pl.when(z < NZ - 1)
            def _():
                right2(c).wait_send()

            @pl.when((z == 0) | ((z < NZ - 1) & (c < direct_from)))
            def _():
                m_right(c).wait_send()

            @pl.when(z > 0)
            def _():
                left2(c).wait_send()

            @pl.when((z == NZ - 1) | ((z > 0) & (c < direct_from)))
            def _():
                m_left(c).wait_send()

            for high in range(2):
                @pl.when((c >= direct_from) & (z == (NZ - 1) * high))
                def _(high=high):
                    m_far(c, high, 2).wait_send()
                    m_far(c, high, 3).wait_send()

        return carry

    lax.fori_loop(0, n_e, drain_e, 0)
    for step in range(3):
        @pl.when(z < NZ - 1)
        def _(step=step):
            stat(step, 0).wait_send()

        @pl.when(z > 0)
        def _(step=step):
            stat(step, 1).wait_send()

    stage_c(3)
    stage_d(3)
    for b in range(2):
        y = jnp.concatenate([h_fin[b, j].astype(F32) for j in range(n_red)], axis=1)
        if b == 0:
            ys = [y]
        else:
            ys.append(y)
    out[...] = jnp.concatenate([ys[b][d * NP:(d + 1) * NP] for d in range(NZ) for b in range(2)], axis=0).astype(BF16)
    for key in range(4):
        for j in range(n_red):
            a_copy(key, j).wait_send()
            b_copy(key, j).wait_send()
            c_copy(key, j, core).wait_send()


def layer_call(hid, g1, g2, wq, wk, wv, wo, wg, wu, wd, kc, vc, lens, cos, sin):
    rows, width = hid.shape
    heads, hd = wq.shape[0], wq.shape[2]
    slots = kc.shape[2]
    ff = wg.shape[1]
    half = rows // 2
    side = half // 2
    n_a = heads
    n_col = ff // COL
    n_e = max(n_col, 8) + n_col
    n_red = 2
    rcol = width // n_red
    hbm = pl.BlockSpec(memory_space=pl.ANY)
    vm = pl.BlockSpec(memory_space=pltpu.VMEM)
    dma = pltpu.SemaphoreType.DMA
    sums = pltpu.VMEM((NZ, n_a, NP, 6 * hd), F32)
    act = pltpu.VMEM((rows, width), BF16)
    half_red = pltpu.VMEM((4, n_red, side, rcol), F32)
    h_halves = pltpu.VMEM((2, n_red, half, rcol), BF16)
    return pl.pallas_call(
        layer_kernel,
        name='layer',
        out_shape=[pltpu.VMEM((rows, width), BF16), pltpu.VMEM(kc.shape, BF16), pltpu.VMEM(vc.shape, BF16)],
        in_specs=[hbm] * 15,
        out_specs=[vm, vm, vm],
        scratch_shapes=[
            act, pltpu.VMEM(g1.shape, g1.dtype), pltpu.VMEM(g2.shape, g2.dtype), pltpu.SMEM(lens.shape, jnp.int32), pltpu.VMEM(cos.shape, F32), pltpu.VMEM(sin.shape, F32),
            act, pltpu.VMEM((2, NP, slots), jnp.int32), pltpu.VMEM((2, 2, NP, hd), F32),
            pltpu.VMEM((3, heads, width, hd), BF16),
            pltpu.VMEM(wo.shape, BF16), pltpu.VMEM(wg.shape, BF16), pltpu.VMEM(wu.shape, BF16), pltpu.VMEM(wd.shape, BF16),
            sums, sums, sums,
            act, pltpu.VMEM((2, NZ, heads, NP, hd), BF16), pltpu.VMEM((half, width), BF16),
            pltpu.VMEM((2, heads, 2, NP, hd), F32),
            pltpu.VMEM((4, n_red, half, rcol), F32),
            half_red, half_red, half_red,
            h_halves, h_halves,
            pltpu.VMEM((n_e, 2, side, 2 * COL), F32),
            pltpu.VMEM((n_e, side, 2 * COL), F32),
            pltpu.VMEM((n_e, side, 2 * COL), F32),
            pltpu.VMEM((rows, ff), BF16),
            pltpu.VMEM((3, 2, 8, 128), F32), pltpu.VMEM((3, 2, 8, 128), F32), pltpu.VMEM((3, 8, 128), F32),
            pltpu.VMEM((7, 2, NZ, NP, 128), F32),
            dma((6,)), dma((3, heads)), dma((2, heads)), dma((2,)), dma((2, n_col)),
            dma((NZ, n_a)), dma((NZ, n_a)), dma((NZ, n_a)), dma((NZ, n_a)),
            dma((n_a, NZ)), dma((n_a, NZ)),
            dma((4, n_red)), dma((4, n_red)), dma((4, n_red)), dma((4, n_red)), dma((4, n_red)), dma((4, n_red)),
            dma((3, 2)), dma((3, 2)),
            dma((n_e,)), dma((n_e,)), dma((n_e,)), dma((n_e,)),
            dma((n_e,)), dma((n_e,)), dma((n_e,)), dma((n_e,)),
            dma((2, DIRECT, 2)),
        ],
        compiler_params=pltpu.CompilerParams(collective_id=0, has_side_effects=True, vmem_limit_bytes=VMEM_KIB * 1024),
    )(hid, g1, g2, wq, wk, wv, wo, wg, wu, wd, kc, vc, lens, cos, sin)


VMEM_KIB = 49 * 1024


def solution(mesh):
    row_spec = P('dp', 'dm')
    cache_spec = P(('dp', 'dm'), None, 'tp', None)
    batch_spec = P(('dp', 'dm'))
    rope_spec = P(('dp', 'dm'), None)
    in_specs = (row_spec, P('dm', 'tp', None), P('dm', 'tp', None), P('dm', 'tp', None), P('tp', None, 'dm'), P('dm', 'tp'), P('dm', 'tp'), P('tp', 'dm'), P('dm'), P('dm'), cache_spec, cache_spec, batch_spec, rope_spec, rope_spec)
    out_specs = (row_spec, cache_spec, cache_spec)

    def local_layer(hidden, w_q, w_k, w_v, w_o, w_gate, w_up, w_down, norm_attn, norm_mlp, k_cache, v_cache, seq_lens, rope_cos, rope_sin):
        by_head = [w.transpose(1, 0, 2) for w in (w_q, w_k, w_v)]
        caches = [c.transpose(0, 2, 1, 3) for c in (k_cache, v_cache)]
        h_out, k_out, v_out = layer_call(hidden, norm_attn, norm_mlp, *by_head, w_o.reshape(-1, w_o.shape[-1]), w_gate, w_up, w_down, *caches, seq_lens, rope_cos, rope_sin)
        return h_out, k_out.transpose(0, 2, 1, 3), v_out.transpose(0, 2, 1, 3)

    return jax.shard_map(local_layer, mesh=mesh, in_specs=in_specs, out_specs=out_specs, check_vma=False)
```

```python
import jax
import jax.numpy as jnp
from jax import lax
from jax.experimental import pallas as pl
from jax.experimental.pallas import tpu as pltpu
from jax.sharding import PartitionSpec as P

EPS = 1e-6
MESH = pl.DeviceIdType.MESH
F32 = jnp.float32
BF16 = jnp.bfloat16
NZ = 4
NP = 8
A_LAG = 2
E_LAG = 3
COL = 384
DIRECT = 4


def remote(src, dst, send_sem, recv_sem, **where):
    return pltpu.make_async_remote_copy(src_ref=src, dst_ref=dst, send_sem=send_sem, recv_sem=recv_sem, device_id=where, device_id_type=MESH)


def partner(tp, k):
    if k == 1:
        return tp + 1 - 2 * lax.rem(tp, 2)
    return lax.rem(tp + 2, 4)


def pack_rows(col):
    rows = col.shape[0]
    lane = lax.broadcasted_iota(jnp.int32, (rows, 128), 1)
    row = lax.broadcasted_iota(jnp.int32, (rows, 128), 0)
    packed = jnp.sum(jnp.where(lane == row, col, 0.0), axis=0, keepdims=True)
    return jnp.broadcast_to(packed, (8, 128))


def unpack_rows(tile, rows):
    lane = lax.broadcasted_iota(jnp.int32, (rows, 128), 1)
    row = lax.broadcasted_iota(jnp.int32, (rows, 128), 0)
    wide = jnp.broadcast_to(tile[0:1], (rows, 128))
    return jnp.sum(jnp.where(lane == row, wide, 0.0), axis=1, keepdims=True)


def layer_kernel(hid_h, g1_h, g2_h, wq, wk, wv, wo, wg, wu, wd, kc, vc, lens_h, cos_h, sin_h,
                 out, k_out, v_out,
                 hid, g1, g2, lens, cos, sin, hid_p, len_v, rope, wbuf, wo_b, wg_b, wu_b, wd_b,
                 part, rbuf, lbuf, x_buf, o_x, o_cat, new_kv, red, r1, s_buf, r2, h_mid, h_fin, pbuf, rbuf2, lbuf2, mbuf,
                 cum_in, cum_out, own_sq, fac,
                 s_sem, w_sem, c_sem, b_sem, g_sem, rs, rr, ls, lr, o_s, o_r, a_s, a_r, b_s, b_r, c_s, c_r,
                 q_s, q_r, rs2, rr2, ls2, lr2, mr_s, mr_r, ml_s, ml_r, far_s):
    z = lax.axis_index('dm')
    tp = lax.axis_index('tp')
    rows, width = hid.shape
    full = width * NZ
    heads = wq.shape[0]
    hd = wq.shape[2]
    per = rows // NZ
    half = rows // 2
    side = half // 2
    slots = kc.shape[2]
    ff = wg.shape[1]
    n_pair = heads // 2
    n_a = 2 * n_pair
    n_col = ff // COL
    second = max(n_col, 9)
    n_e = second + n_col
    trip = E_LAG * (NZ - 1)
    n_grp = g_sem.shape[1]
    n_red = red.shape[1]
    rcol = width // n_red
    early = n_col * 2 // 3
    direct_from = n_e - DIRECT
    core = lax.rem(tp, 2)
    sib, across = partner(tp, 1), partner(tp, 2)
    nxt, prv = lax.rem(z + 1, NZ), lax.rem(z + NZ - 1, NZ)

    small = [pltpu.make_async_copy(a, b, s_sem.at[i]) for i, (a, b) in enumerate(((hid_h, hid), (g1_h, g1), (g2_h, g2), (cos_h, cos), (sin_h, sin), (lens_h, lens)))]
    load_o = pltpu.make_async_copy(wo, wo_b, b_sem.at[0])
    load_d = pltpu.make_async_copy(wd, wd_b, b_sem.at[1])

    def load_w(i, h):
        return pltpu.make_async_copy((wq, wk, wv)[i].at[h], wbuf.at[i, h], w_sem.at[i, h])

    def load_c(i, h):
        return pltpu.make_async_copy((kc, vc)[i].at[:, h], (k_out, v_out)[i].at[:, h], c_sem.at[i, h])

    def load(i, g):
        src, dst = ((wg, wg_b), (wu, wu_b))[i]
        cols = pl.ds(pl.multiple_of(g * COL, COL), COL)
        return pltpu.make_async_copy(src.at[:, cols], dst.at[:, cols], g_sem.at[i, g])

    for cp in small:
        cp.start()
    for h in range(heads):
        for i in range(3):
            load_w(i, h).start()
        if h >= 2:
            load_c(0, h - 2).start()
            load_c(1, h - 2).start()
    for h in range(max(heads - 2, 0), heads):
        load_c(0, h).start()
        load_c(1, h).start()
    load_o.start()
    for g in range(n_grp):
        load(0, g).start()
        load(1, g).start()
    load_d.start()

    sem = pltpu.get_barrier_semaphore()
    for k in range(1, NZ):
        pl.semaphore_signal(sem, inc=1, device_id={'dm': lax.rem(z + k, NZ)}, device_id_type=MESH)
    for k in (1, 2):
        pl.semaphore_signal(sem, inc=1, device_id={'tp': partner(tp, k)}, device_id_type=MESH)

    for cp in small:
        cp.wait()

    def inv(tile):
        return lax.rsqrt(tile / full + EPS)

    def local_norm(x, gain, step, lo):
        col = jnp.sum(x * x, axis=-1, keepdims=True)
        own_sq[step] = pack_rows(col)
        x_buf[lo:lo + x.shape[0]] = (x * lax.rsqrt(col / full + EPS) * gain).astype(BF16)

    def place(b, d):
        return d * per + b * NP

    x0 = hid[...].astype(F32)
    x0 = jnp.concatenate([x0[place(b, d):place(b, d) + NP] for b in range(2) for d in range(NZ)], axis=0)
    hid_p[...] = x0.astype(BF16)
    local_norm(x0, g1[...].astype(F32).reshape(1, width), 0, 0)
    cs, sn = cos[...], sin[...]
    row = lax.broadcasted_iota(jnp.int32, (2 * NP, slots), 0)
    pos = lax.broadcasted_iota(jnp.int32, (2 * NP, slots), 1)
    for b in range(2):
        part_cs, part_sn = [jnp.concatenate([t[b * NP:(b + 1) * NP]] * 2, axis=0) for t in (cs, sn)]
        rope[0, b] = jnp.concatenate([part_cs, part_cs], axis=-1)
        rope[1, b] = jnp.concatenate([-part_sn, part_sn], axis=-1)
        length = jnp.zeros((2 * NP, slots), jnp.int32)
        for r in range(NP):
            length = jnp.where((row == r) | (row == NP + r), lens[b * NP + r], length)
        len_v[b] = length

    def stat(step, way):
        return remote(cum_out.at[step, way], cum_in.at[step, way], q_s.at[step, way], q_r.at[step, way], dm=(nxt, prv)[way])

    def put_fac(i, tile, halves):
        n = len(halves) * half
        wide = jnp.broadcast_to(unpack_rows(tile, n), (n, 128))
        for k, b in enumerate(halves):
            for d in range(NZ):
                lo = (k * NZ + d) * NP
                fac[i, b, d] = wide[lo:lo + NP]

    def relay_stat(step, way, halves):
        has_in = (z > 0) if way == 0 else (z < NZ - 1)
        has_out = (z < NZ - 1) if way == 0 else (z > 0)

        @pl.when(has_in)
        def _():
            stat(step, way).wait_recv()

        @pl.when(jnp.logical_not(has_in))
        def _():
            cum_in[step, way] = jnp.zeros((8, 128), F32)

        before, own = cum_in[step, way], own_sq[step]
        cum = before + own
        cum_out[step, way] = cum

        @pl.when(has_out)
        def _():
            stat(step, way).start()

        scale = inv(cum)
        put_fac(2 * way, scale / inv(own), halves)
        put_fac(2 * way + 1, scale / inv(before), halves)

    @pl.when(z == 0)
    def _():
        rbuf[0] = jnp.zeros(rbuf.shape[1:], F32)

    @pl.when(z == NZ - 1)
    def _():
        lbuf[NZ - 1] = jnp.zeros(lbuf.shape[1:], F32)

    pl.semaphore_wait(sem, NZ + 1)

    def right(d, p):
        return remote(part.at[d, p], rbuf.at[d, p], rs.at[d, p], rr.at[d, p], dm=nxt)

    def left(d, p):
        return remote(part.at[d, p], lbuf.at[d, p], ls.at[d, p], lr.at[d, p], dm=prv)

    def split(it):
        b = it // n_pair
        return b, it - b * n_pair

    def o_copy(src, to, it):
        b, p = split(it)
        view = o_x.at[b, src, pl.ds(2 * p, 2)]
        return remote(view, view, o_s.at[it, to], o_r.at[it, src], dm=to)

    def repeat(f, n):
        return jnp.concatenate([f] * n, axis=1)

    def attend(it):
        b, p = split(it)
        y = part[z, it] * repeat(fac[4, b, z], 6) + (rbuf[z, it] * repeat(fac[5, b, z], 6) + lbuf[z, it] * repeat(fac[6, b, z], 6))

        @pl.when(b == 0)
        def _():
            for e in range(2):
                load_c(0, 2 * p + e).wait()
                load_c(1, 2 * p + e).wait()

        q, k, v_new = [jnp.concatenate([y[:, i * hd:(i + 1) * hd], y[:, (3 + i) * hd:(4 + i) * hd]], axis=0) for i in range(3)]
        cos2, sin2 = rope[0, b], rope[1, b]
        at_len = pos == len_v[b]
        seen = pos <= len_v[b]
        q = (q * cos2 + pltpu.roll(q, hd // 2, 1) * sin2).astype(BF16)
        k_new = (k * cos2 + pltpu.roll(k, hd // 2, 1) * sin2).astype(BF16).astype(F32)
        v_new = v_new.astype(BF16).astype(F32)
        s = jnp.zeros((2 * NP, slots), F32)
        for e in range(2):
            for r in range(NP):
                t = lax.dot_general(q, k_out[b * NP + r, 2 * p + e], (((1,), (1,)), ((), ())), preferred_element_type=F32)
                s = jnp.where(row == e * NP + r, t, s)
        s_new = jnp.sum(q.astype(F32) * k_new, axis=-1, keepdims=True)
        s = jnp.where(at_len, s_new, s) * (hd ** -0.5)
        s = jnp.where(seen, s, -1e30)
        ex = jnp.exp(s - jnp.max(s, axis=-1, keepdims=True))
        prob = (ex / jnp.sum(ex, axis=-1, keepdims=True)).astype(BF16).astype(F32)
        p_new = jnp.sum(jnp.where(at_len, prob, 0.0), axis=-1, keepdims=True)
        p_old = jnp.where(at_len, 0.0, prob).astype(BF16)
        acc = jnp.zeros((2 * NP, hd), F32)
        for e in range(2):
            for r in range(NP):
                t = jnp.dot(p_old, v_out[b * NP + r, 2 * p + e], preferred_element_type=F32)
                acc = jnp.where(row == e * NP + r, t, acc)
        acc = acc + p_new * v_new
        for e in range(2):
            h, at = 2 * p + e, slice(e * NP, (e + 1) * NP)
            new_kv[0, h, b] = k_new[at]
            new_kv[1, h, b] = v_new[at]
            o_x[b, z, h] = acc[at].astype(BF16)
        for k in (2, 1, 3):
            o_copy(z, lax.rem(z + k, NZ), it).start()

    where = lax.broadcasted_iota(jnp.int32, (slots, hd), 0)

    def patch(h, b):
        for r in range(NP):
            hit = where == lens[b * NP + r]
            for i, ref in enumerate((k_out, v_out)):
                fresh = jnp.broadcast_to(new_kv[i, h, b, r:r + 1, :], (slots, hd))
                ref[b * NP + r, h] = jnp.where(hit, fresh, ref[b * NP + r, h].astype(F32)).astype(BF16)

    mine = pl.ds(pl.multiple_of(core * side, side), side)
    other = pl.ds(pl.multiple_of((1 - core) * side, side), side)

    def a_copy(key, j):
        return remote(red.at[key, j, other], r1.at[key, j], a_s.at[key, j], a_r.at[key, j], tp=sib)

    def b_copy(key, j):
        return remote(s_buf.at[key, j], r2.at[key, j], b_s.at[key, j], b_r.at[key, j], tp=across)

    def c_copy(key, j, who):
        view = (h_mid, h_fin)[key // 2].at[key % 2, j, pl.ds(pl.multiple_of(who * side, side), side)]
        return remote(view, view, c_s.at[key, j], c_r.at[key, j], tp=sib)

    def o_gather(b):
        def wait(p, carry):
            it = b * n_pair + p
            for k in (1, 3, 2):
                o_copy(lax.rem(z + k, NZ), lax.rem(z + k, NZ), it).wait_recv()
            return carry

        lax.fori_loop(0, n_pair, wait, 0)
        o_cat[...] = jnp.concatenate([jnp.concatenate([o_x[b, d, h].astype(F32) for h in range(heads)], axis=1) for d in range(NZ)], axis=0).astype(BF16)

    def o_product(b, j):
        red[b, j] = jnp.dot(o_cat[...], wo_b[:, j * rcol:(j + 1) * rcol], preferred_element_type=F32)
        a_copy(b, j).start()

    def m_rows(b):
        return pl.ds(b * half, half)

    def stage_b(key):
        for j in range(n_red):
            a_copy(key, j).wait_recv()
            s_buf[key, j] = red[key, j, mine] + r1[key, j]
            b_copy(key, j).start()

    def stage_c(key):
        b = key % 2
        for j in range(n_red):
            b_copy(key, j).wait_recv()
            total = (s_buf[key, j] + r2[key, j]).astype(BF16).astype(F32)
            if key < 2:
                base = hid_p[pl.ds(pl.multiple_of(b * half + core * side, side), side), pl.ds(j * rcol, rcol)]
                h_mid[b, j, mine] = (base.astype(F32) + total).astype(BF16)
            else:
                h_fin[b, j, mine] = (h_mid[b, j, mine].astype(F32) + total).astype(BF16)
            c_copy(key, j, core).start()

    def stage_d(key):
        for j in range(n_red):
            c_copy(key, j, 1 - core).wait_recv()
        if key < 2:
            x = jnp.concatenate([h_mid[key, j].astype(F32) for j in range(n_red)], axis=1)
            local_norm(x, g2[...].astype(F32).reshape(1, width), 1 + key, key * half)

    def a_slot(t, carry):
        @pl.when(t < n_pair)
        def _():
            for e in range(2):
                for i in range(3):
                    load_w(i, 2 * t + e).wait()
            for e in range(2):
                h = 2 * t + e
                for i in range(3):
                    y = jnp.dot(x_buf[...], wbuf[i, h], preferred_element_type=F32)
                    for b in range(2):
                        for d in range(NZ):
                            lo = (b * NZ + d) * NP
                            part[d, b * n_pair + t, :, (3 * e + i) * hd:(3 * e + i + 1) * hd] = y[lo:lo + NP]

        @pl.when(t == A_LAG * z)
        def _():
            relay_stat(0, 0, (0, 1))

        for d in (3, 2, 1):
            p = t - A_LAG * z - (NZ - 1 - d)

            @pl.when((p >= 0) & (p < n_a))
            def _(d=d, p=p):
                b = p // n_pair

                @pl.when((z > 0) & (z <= d))
                def _():
                    right(d, p).wait_recv()

                @pl.when((z > 0) & (z < d))
                def _():
                    part[d, p] = part[d, p] * repeat(fac[0, b, d], 6) + rbuf[d, p] * repeat(fac[1, b, d], 6)

                @pl.when(z < d)
                def _():
                    right(d, p).start()

        @pl.when(t == A_LAG * (NZ - 1 - z))
        def _():
            relay_stat(0, 1, (0, 1))

        for d in (0, 1, 2):
            q = t - A_LAG * (NZ - 1 - z) - d

            @pl.when((q >= 0) & (q < n_a))
            def _(d=d, q=q):
                b = q // n_pair

                @pl.when((z < NZ - 1) & (z >= d))
                def _():
                    left(d, q).wait_recv()

                @pl.when((z < NZ - 1) & (z > d))
                def _():
                    part[d, q] = part[d, q] * repeat(fac[2, b, d], 6) + lbuf[d, q] * repeat(fac[3, b, d], 6)

                @pl.when(z > d)
                def _():
                    left(d, q).start()

        f = t - jnp.maximum(A_LAG * z + NZ - 1 - z, A_LAG * (NZ - 1 - z) + z)

        @pl.when(f == 0)
        def _():
            own = own_sq[0]
            scale = inv((cum_in[0, 0] + own) + cum_in[0, 1])
            put_fac(4, scale / inv(own), (0, 1))
            put_fac(5, scale / inv(cum_in[0, 0]), (0, 1))
            put_fac(6, scale / inv(cum_in[0, 1]), (0, 1))

        @pl.when((f >= 0) & (f < n_a))
        def _():
            attend(f)

        o_at = n_pair - 1 + A_LAG * (NZ - 1) + 2

        @pl.when(t == o_at)
        def _():
            load_o.wait()
            o_gather(0)
            for j in range(n_red):
                o_product(0, j)

        @pl.when(t == o_at + 1)
        def _():
            stage_b(0)

        return carry

    a_end = max(n_a + A_LAG * (NZ - 1), n_pair + A_LAG * (NZ - 1) + 3)
    lax.fori_loop(0, a_end, a_slot, 0)

    def patch_x(h, carry):
        patch(h, 0)
        return carry

    lax.fori_loop(0, heads, patch_x, 0)
    stage_c(0)
    stage_d(0)

    def right2(c):
        return remote(pbuf.at[c, 1], rbuf2.at[c], rs2.at[c], rr2.at[c], dm=nxt)

    def left2(c):
        return remote(pbuf.at[c, 0], lbuf2.at[c], ls2.at[c], lr2.at[c], dm=prv)

    def valid(c):
        return ((c >= 0) & (c < n_col)) | ((c >= second) & (c < n_e))

    def half_of(c):
        b = c // second
        return b, c - b * second

    def m_view(c, high):
        b, k = half_of(c)
        return mbuf.at[pl.ds(pl.multiple_of(b * half + high * side, side), side), pl.ds(pl.multiple_of(k * COL, COL), COL)]

    def m_left(c):
        return remote(m_view(c, 1), m_view(c, 1), mr_s.at[c], mr_r.at[c], dm=prv)

    def m_right(c):
        return remote(m_view(c, 0), m_view(c, 0), ml_s.at[c], ml_r.at[c], dm=nxt)

    def m_far(c, high, k):
        to = (NZ - 1 - k) if high else k
        recv = mr_r if high else ml_r
        return remote(m_view(c, high), m_view(c, high), far_s.at[high, c - direct_from, k - 2], recv.at[c], dm=to)

    def gated(a):
        g, u = a[:, :COL], a[:, COL:]
        return (g * (1.0 / (1.0 + jnp.exp(-g))) * u).astype(BF16)

    def wide(i, b, first):
        f = jnp.concatenate([fac[i, b, first], fac[i, b, first + 1]], axis=0)
        return repeat(f, 2 * COL // 128)

    def finish(c, high):
        b, k = half_of(c)
        mbuf[pl.ds(pl.multiple_of(b * half + high * side, side), side), pl.ds(pl.multiple_of(k * COL, COL), COL)] = gated(pbuf[c, high])

        @pl.when(c >= direct_from)
        def _():
            m_far(c, high, 3).start()
            m_far(c, high, 2).start()

        (m_left if high else m_right)(c).start()

    def e_slot(t, carry):
        @pl.when(valid(t))
        def _():
            b, k = half_of(t)

            @pl.when(b == 0)
            def _():
                load(0, k).wait()
                load(1, k).wait()

            cols = pl.ds(pl.multiple_of(k * COL, COL), COL)
            x = x_buf[pl.ds(pl.multiple_of(b * half, half), half), :]
            g = jnp.dot(x, wg_b[:, cols], preferred_element_type=F32)
            u = jnp.dot(x, wu_b[:, cols], preferred_element_type=F32)
            for s in range(2):
                pbuf[t, s, :, 0:COL] = g[s * side:(s + 1) * side]
                pbuf[t, s, :, COL:] = u[s * side:(s + 1) * side]

        c = t - E_LAG * z
        for step, first in ((1, 0), (2, second)):
            @pl.when(c == first)
            def _(step=step):
                relay_stat(step, 0, (step - 1,))

        @pl.when(valid(c))
        def _():
            b = c // second

            @pl.when(z > 0)
            def _():
                right2(c).wait_recv()
                pbuf[c, 1] = pbuf[c, 1] * wide(0, b, 2) + rbuf2[c] * wide(1, b, 2)

            @pl.when(z < NZ - 1)
            def _():
                right2(c).start()

            @pl.when(z == NZ - 1)
            def _():
                finish(c, 1)

        d = t - E_LAG * (NZ - 1 - z)
        for step, first in ((1, 0), (2, second)):
            @pl.when(d == first)
            def _(step=step):
                relay_stat(step, 1, (step - 1,))

        @pl.when(valid(d))
        def _():
            b = d // second

            @pl.when(z < NZ - 1)
            def _():
                left2(d).wait_recv()
                pbuf[d, 0] = pbuf[d, 0] * wide(2, b, 0) + lbuf2[d] * wide(3, b, 0)

            @pl.when(z > 0)
            def _():
                left2(d).start()

            @pl.when(z == 0)
            def _():
                finish(d, 0)

        e = t - E_LAG * (2 * NZ - 2 - z)

        @pl.when(valid(e) & (z < NZ - 1))
        def _():
            m_left(e).wait_recv()

            @pl.when((z > 0) & (e < direct_from))
            def _():
                m_left(e).start()

        f = t - E_LAG * (NZ - 1 + z)

        @pl.when(valid(f) & (z > 0))
        def _():
            m_right(f).wait_recv()

            @pl.when((z < NZ - 1) & (f < direct_from))
            def _():
                m_right(f).start()

        @pl.when(t == 1)
        def _():
            o_gather(1)
            for j in range(n_red):
                o_product(1, j)

        @pl.when(t == 2)
        def _():
            stage_b(1)

        @pl.when(t == 6)
        def _():
            stage_c(1)

        @pl.when(t == 8)
        def _():
            stage_d(1)

        @pl.when((t >= n_e) & (t < n_e + heads))
        def _():
            patch(t - n_e, 1)

        down = n_col + 2 * trip
        for j in range(n_red):
            @pl.when(t == down + j)
            def _(j=j):
                if j == 0:
                    load_d.wait()
                red[2, j] = jnp.dot(mbuf[m_rows(0), :], wd_b[:, j * rcol:(j + 1) * rcol], preferred_element_type=F32)
                a_copy(2, j).start()

        @pl.when(t == down + 2)
        def _():
            stage_b(2)

        late = second + early + 2 * trip
        for j in range(n_red):
            @pl.when(t == late + j)
            def _(j=j):
                red[3, j] = jnp.dot(mbuf[m_rows(1), 0:early * COL], wd_b[0:early * COL, j * rcol:(j + 1) * rcol], preferred_element_type=F32)

        return carry

    lax.fori_loop(0, max(n_e + 2 * trip, second + early + n_red + 2 * trip, n_e + heads, n_col + 2 * trip + 3), e_slot, 0)
    for j in range(n_red):
        red[3, j] = red[3, j] + jnp.dot(mbuf[m_rows(1), early * COL:], wd_b[early * COL:, j * rcol:(j + 1) * rcol], preferred_element_type=F32)
        a_copy(3, j).start()
    stage_c(2)
    stage_b(3)
    stage_d(2)

    def drain_a(p, carry):
        for d in range(NZ):
            @pl.when(z < d)
            def _(d=d):
                right(d, p).wait_send()

            @pl.when(z > d)
            def _(d=d):
                left(d, p).wait_send()

        for k in range(1, NZ):
            o_copy(z, lax.rem(z + k, NZ), p).wait_send()
        return carry

    lax.fori_loop(0, n_a, drain_a, 0)

    def drain_e(c, carry):
        @pl.when(valid(c))
        def _():
            @pl.when(z < NZ - 1)
            def _():
                right2(c).wait_send()

            @pl.when((z == 0) | ((z < NZ - 1) & (c < direct_from)))
            def _():
                m_right(c).wait_send()

            @pl.when(z > 0)
            def _():
                left2(c).wait_send()

            @pl.when((z == NZ - 1) | ((z > 0) & (c < direct_from)))
            def _():
                m_left(c).wait_send()

            for high in range(2):
                @pl.when((c >= direct_from) & (z == (NZ - 1) * high))
                def _(high=high):
                    m_far(c, high, 2).wait_send()
                    m_far(c, high, 3).wait_send()

        return carry

    lax.fori_loop(0, n_e, drain_e, 0)
    for step in range(3):
        @pl.when(z < NZ - 1)
        def _(step=step):
            stat(step, 0).wait_send()

        @pl.when(z > 0)
        def _(step=step):
            stat(step, 1).wait_send()

    stage_c(3)
    stage_d(3)
    for b in range(2):
        y = jnp.concatenate([h_fin[b, j].astype(F32) for j in range(n_red)], axis=1)
        if b == 0:
            ys = [y]
        else:
            ys.append(y)
    out[...] = jnp.concatenate([ys[b][d * NP:(d + 1) * NP] for d in range(NZ) for b in range(2)], axis=0).astype(BF16)
    for key in range(4):
        for j in range(n_red):
            a_copy(key, j).wait_send()
            b_copy(key, j).wait_send()
            c_copy(key, j, core).wait_send()


def layer_call(hid, g1, g2, wq, wk, wv, wo, wg, wu, wd, kc, vc, lens, cos, sin):
    rows, width = hid.shape
    heads, hd = wq.shape[0], wq.shape[2]
    slots = kc.shape[2]
    ff = wg.shape[1]
    half = rows // 2
    side = half // 2
    n_a = heads
    n_col = ff // COL
    n_e = max(n_col, 9) + n_col
    n_red = 2
    rcol = width // n_red
    hbm = pl.BlockSpec(memory_space=pl.ANY)
    vm = pl.BlockSpec(memory_space=pltpu.VMEM)
    dma = pltpu.SemaphoreType.DMA
    sums = pltpu.VMEM((NZ, n_a, NP, 6 * hd), F32)
    act = pltpu.VMEM((rows, width), BF16)
    half_red = pltpu.VMEM((4, n_red, side, rcol), F32)
    h_halves = pltpu.VMEM((2, n_red, half, rcol), BF16)
    return pl.pallas_call(
        layer_kernel,
        name='layer',
        out_shape=[pltpu.VMEM((rows, width), BF16), pltpu.VMEM(kc.shape, BF16), pltpu.VMEM(vc.shape, BF16)],
        in_specs=[hbm] * 15,
        out_specs=[vm, vm, vm],
        scratch_shapes=[
            act, pltpu.VMEM(g1.shape, g1.dtype), pltpu.VMEM(g2.shape, g2.dtype), pltpu.SMEM(lens.shape, jnp.int32), pltpu.VMEM(cos.shape, F32), pltpu.VMEM(sin.shape, F32),
            act, pltpu.VMEM((2, 2 * NP, slots), jnp.int32), pltpu.VMEM((2, 2, 2 * NP, hd), F32),
            pltpu.VMEM((3, heads, width, hd), BF16),
            pltpu.VMEM(wo.shape, BF16), pltpu.VMEM(wg.shape, BF16), pltpu.VMEM(wu.shape, BF16), pltpu.VMEM(wd.shape, BF16),
            sums, sums, sums,
            act, pltpu.VMEM((2, NZ, heads, NP, hd), BF16), pltpu.VMEM((half, width), BF16),
            pltpu.VMEM((2, heads, 2, NP, hd), F32),
            pltpu.VMEM((4, n_red, half, rcol), F32),
            half_red, half_red, half_red,
            h_halves, h_halves,
            pltpu.VMEM((n_e, 2, side, 2 * COL), F32),
            pltpu.VMEM((n_e, side, 2 * COL), F32),
            pltpu.VMEM((n_e, side, 2 * COL), F32),
            pltpu.VMEM((rows, ff), BF16),
            pltpu.VMEM((3, 2, 8, 128), F32), pltpu.VMEM((3, 2, 8, 128), F32), pltpu.VMEM((3, 8, 128), F32),
            pltpu.VMEM((7, 2, NZ, NP, 128), F32),
            dma((6,)), dma((3, heads)), dma((2, heads)), dma((2,)), dma((2, n_col)),
            dma((NZ, n_a)), dma((NZ, n_a)), dma((NZ, n_a)), dma((NZ, n_a)),
            dma((n_a, NZ)), dma((n_a, NZ)),
            dma((4, n_red)), dma((4, n_red)), dma((4, n_red)), dma((4, n_red)), dma((4, n_red)), dma((4, n_red)),
            dma((3, 2)), dma((3, 2)),
            dma((n_e,)), dma((n_e,)), dma((n_e,)), dma((n_e,)),
            dma((n_e,)), dma((n_e,)), dma((n_e,)), dma((n_e,)),
            dma((2, DIRECT, 2)),
        ],
        compiler_params=pltpu.CompilerParams(collective_id=0, has_side_effects=True, vmem_limit_bytes=VMEM_KIB * 1024),
    )(hid, g1, g2, wq, wk, wv, wo, wg, wu, wd, kc, vc, lens, cos, sin)


VMEM_KIB = 49 * 1024


def solution(mesh):
    row_spec = P('dp', 'dm')
    cache_spec = P(('dp', 'dm'), None, 'tp', None)
    batch_spec = P(('dp', 'dm'))
    rope_spec = P(('dp', 'dm'), None)
    in_specs = (row_spec, P('dm', 'tp', None), P('dm', 'tp', None), P('dm', 'tp', None), P('tp', None, 'dm'), P('dm', 'tp'), P('dm', 'tp'), P('tp', 'dm'), P('dm'), P('dm'), cache_spec, cache_spec, batch_spec, rope_spec, rope_spec)
    out_specs = (row_spec, cache_spec, cache_spec)

    def local_layer(hidden, w_q, w_k, w_v, w_o, w_gate, w_up, w_down, norm_attn, norm_mlp, k_cache, v_cache, seq_lens, rope_cos, rope_sin):
        by_head = [w.transpose(1, 0, 2) for w in (w_q, w_k, w_v)]
        caches = [c.transpose(0, 2, 1, 3) for c in (k_cache, v_cache)]
        h_out, k_out, v_out = layer_call(hidden, norm_attn, norm_mlp, *by_head, w_o.reshape(-1, w_o.shape[-1]), w_gate, w_up, w_down, *caches, seq_lens, rope_cos, rope_sin)
        return h_out, k_out.transpose(0, 2, 1, 3), v_out.transpose(0, 2, 1, 3)

    return jax.shard_map(local_layer, mesh=mesh, in_specs=in_specs, out_specs=out_specs, check_vma=False)
```

```python
import jax
import jax.numpy as jnp
from jax import lax
from jax.experimental import pallas as pl
from jax.experimental.pallas import tpu as pltpu
from jax.sharding import PartitionSpec as P

EPS = 1e-6
MESH = pl.DeviceIdType.MESH
F32 = jnp.float32
BF16 = jnp.bfloat16
NZ = 4
NP = 8
A_LAG = 2
FAR = 2
X_LAG = 5
E_LAG = 3
COL = 384
DIRECT = 4


def remote(src, dst, send_sem, recv_sem, **where):
    return pltpu.make_async_remote_copy(src_ref=src, dst_ref=dst, send_sem=send_sem, recv_sem=recv_sem, device_id=where, device_id_type=MESH)


def partner(tp, k):
    if k == 1:
        return tp + 1 - 2 * lax.rem(tp, 2)
    return lax.rem(tp + 2, 4)


def pack_rows(col):
    rows = col.shape[0]
    lane = lax.broadcasted_iota(jnp.int32, (rows, 128), 1)
    row = lax.broadcasted_iota(jnp.int32, (rows, 128), 0)
    packed = jnp.sum(jnp.where(lane == row, col, 0.0), axis=0, keepdims=True)
    return jnp.broadcast_to(packed, (8, 128))


def unpack_rows(tile, rows, first=0):
    lane = lax.broadcasted_iota(jnp.int32, (rows, 128), 1)
    row = lax.broadcasted_iota(jnp.int32, (rows, 128), 0)
    wide = jnp.broadcast_to(tile[0:1], (rows, 128))
    return jnp.sum(jnp.where(lane == row + first, wide, 0.0), axis=1, keepdims=True)


def layer_kernel(hid_h, g1_h, g2_h, wq, wk, wv, wo, wg, wu, wd, kc, vc, lens_h, cos_h, sin_h,
                 out, k_out, v_out,
                 hid, g1, g2, lens, cos, sin, hid_p, len_v, rope, wbuf, wo_b, wg_b, wu_b, wd_b,
                 part, rbuf, lbuf, dbuf, x_buf, o_x, o_cat, new_kv, red, r1, s_buf, r2, h_mid, h_fin, pbuf, rbuf2, lbuf2, mbuf,
                 cum_in, cum_out, own_sq, sq_all, fac,
                 s_sem, w_sem, c_sem, b_sem, g_sem, rs, rr, ls, lr, dx_s, dx_r, sq_s, sq_r, o_s, o_r, a_s, a_r, b_s, b_r, c_s, c_r,
                 q_s, q_r, rs2, rr2, ls2, lr2, mr_s, mr_r, ml_s, ml_r, far_s):
    z = lax.axis_index('dm')
    tp = lax.axis_index('tp')
    rows, width = hid.shape
    full = width * NZ
    heads = wq.shape[0]
    hd = wq.shape[2]
    per = rows // NZ
    half = rows // 2
    side = half // 2
    slots = kc.shape[2]
    ff = wg.shape[1]
    n_pair = heads // 2
    n_a = 2 * n_pair
    n_col = ff // COL
    second = max(n_col, 9)
    n_e = second + n_col
    trip = E_LAG * (NZ - 1)
    n_grp = g_sem.shape[1]
    n_red = red.shape[1]
    rcol = width // n_red
    early = n_col * 2 // 3
    direct_from = n_e - DIRECT
    core = lax.rem(tp, 2)
    sib, across = partner(tp, 1), partner(tp, 2)
    nxt, prv = lax.rem(z + 1, NZ), lax.rem(z + NZ - 1, NZ)

    small = [pltpu.make_async_copy(a, b, s_sem.at[i]) for i, (a, b) in enumerate(((hid_h, hid), (g1_h, g1), (g2_h, g2), (cos_h, cos), (sin_h, sin), (lens_h, lens)))]
    load_o = pltpu.make_async_copy(wo, wo_b, b_sem.at[0])
    load_d = pltpu.make_async_copy(wd, wd_b, b_sem.at[1])

    def load_w(i, h):
        return pltpu.make_async_copy((wq, wk, wv)[i].at[h], wbuf.at[i, h], w_sem.at[i, h])

    def load_c(i, h):
        return pltpu.make_async_copy((kc, vc)[i].at[:, h], (k_out, v_out)[i].at[:, h], c_sem.at[i, h])

    def load(i, g):
        src, dst = ((wg, wg_b), (wu, wu_b))[i]
        cols = pl.ds(pl.multiple_of(g * COL, COL), COL)
        return pltpu.make_async_copy(src.at[:, cols], dst.at[:, cols], g_sem.at[i, g])

    for cp in small:
        cp.start()
    for h in range(heads):
        for i in range(3):
            load_w(i, h).start()
        if h >= 2:
            load_c(0, h - 2).start()
            load_c(1, h - 2).start()
    for h in range(max(heads - 2, 0), heads):
        load_c(0, h).start()
        load_c(1, h).start()
    load_o.start()
    for g in range(n_grp):
        load(0, g).start()
        load(1, g).start()
    load_d.start()

    sem = pltpu.get_barrier_semaphore()
    for k in range(1, NZ):
        pl.semaphore_signal(sem, inc=1, device_id={'dm': lax.rem(z + k, NZ)}, device_id_type=MESH)
    for k in (1, 2):
        pl.semaphore_signal(sem, inc=1, device_id={'tp': partner(tp, k)}, device_id_type=MESH)

    for cp in small:
        cp.wait()

    def inv(tile):
        return lax.rsqrt(tile / full + EPS)

    def local_norm(x, gain, step, lo):
        col = jnp.sum(x * x, axis=-1, keepdims=True)
        own_sq[step] = pack_rows(col)
        x_buf[lo:lo + x.shape[0]] = (x * lax.rsqrt(col / full + EPS) * gain).astype(BF16)

    def place(b, d):
        return d * per + b * NP

    x0 = hid[...].astype(F32)
    x0 = jnp.concatenate([x0[place(b, d):place(b, d) + NP] for b in range(2) for d in range(NZ)], axis=0)
    hid_p[...] = x0.astype(BF16)
    local_norm(x0, g1[...].astype(F32).reshape(1, width), 0, 0)
    cs, sn = cos[...], sin[...]
    row = lax.broadcasted_iota(jnp.int32, (2 * NP, slots), 0)
    pos = lax.broadcasted_iota(jnp.int32, (2 * NP, slots), 1)
    for b in range(2):
        part_cs, part_sn = [jnp.concatenate([t[b * NP:(b + 1) * NP]] * 2, axis=0) for t in (cs, sn)]
        rope[0, b] = jnp.concatenate([part_cs, part_cs], axis=-1)
        rope[1, b] = jnp.concatenate([-part_sn, part_sn], axis=-1)
        length = jnp.zeros((2 * NP, slots), jnp.int32)
        for r in range(NP):
            length = jnp.where((row == r) | (row == NP + r), lens[b * NP + r], length)
        len_v[b] = length

    def stat(step, way):
        return remote(cum_out.at[step, way], cum_in.at[step, way], q_s.at[step, way], q_r.at[step, way], dm=(nxt, prv)[way])

    def put_fac(i, tile, halves, first=0):
        n = len(halves) * half
        wide = jnp.broadcast_to(unpack_rows(tile, n, first), (n, 128))
        for k, b in enumerate(halves):
            for d in range(NZ):
                lo = (k * NZ + d) * NP
                fac[i, b, d] = wide[lo:lo + NP]

    def relay_stat(step, way, halves):
        has_in = (z > 0) if way == 0 else (z < NZ - 1)
        has_out = (z < NZ - 1) if way == 0 else (z > 0)

        @pl.when(has_in)
        def _():
            stat(step, way).wait_recv()

        @pl.when(jnp.logical_not(has_in))
        def _():
            cum_in[step, way] = jnp.zeros((8, 128), F32)

        before, own = cum_in[step, way], own_sq[step]
        cum = before + own
        cum_out[step, way] = cum

        @pl.when(has_out)
        def _():
            stat(step, way).start()

        scale = inv(cum)
        put_fac(2 * way, scale / inv(own), halves)
        put_fac(2 * way + 1, scale / inv(before), halves)

    @pl.when(z == 0)
    def _():
        rbuf[0] = jnp.zeros(rbuf.shape[1:], F32)

    @pl.when(z == NZ - 1)
    def _():
        lbuf[NZ - 1] = jnp.zeros(lbuf.shape[1:], F32)

    def sq_copy(src, to):
        return remote(sq_all.at[src], sq_all.at[src], sq_s.at[to], sq_r.at[src], dm=to)

    sq_all[z] = own_sq[0]
    pl.semaphore_wait(sem, NZ + 1)
    for k in (2, 1, 3):
        sq_copy(z, lax.rem(z + k, NZ)).start()

    def a_stats():
        for k in (1, 3, 2):
            sq_copy(lax.rem(z + k, NZ), lax.rem(z + k, NZ)).wait_recv()
        none = jnp.zeros((8, 128), F32)
        before, after, own = none, none, own_sq[0]
        for j in range(NZ):
            before = before + jnp.where(j < z, sq_all[j], 0.0)
            after = after + jnp.where(j > z, sq_all[j], 0.0)
        total = inv((before + own) + after)
        for i, other_side in enumerate((before, after)):
            scale = inv(other_side + own)
            put_fac(2 * i, scale / inv(own), (1,), half)
            put_fac(2 * i + 1, scale / inv(other_side), (1,), half)
            put_fac(5 + i, total / inv(other_side), (1,), half)
        put_fac(4, total / inv(own), (1,), half)
        for j in range(NZ):
            put_fac(7 + j, total / inv(sq_all[j]), (0,))

    def x_copy(src, to, p):
        return remote(part.at[to, p], dbuf.at[src, p], dx_s.at[p, to], dx_r.at[p, src], dm=to)

    def right(d, p):
        return remote(part.at[d, p], rbuf.at[d, p], rs.at[d, p], rr.at[d, p], dm=nxt)

    def left(d, p):
        return remote(part.at[d, p], lbuf.at[d, p], ls.at[d, p], lr.at[d, p], dm=prv)

    def split(it):
        b = it // n_pair
        return b, it - b * n_pair

    def o_copy(src, to, it):
        b, p = split(it)
        view = o_x.at[b, src, pl.ds(2 * p, 2)]
        return remote(view, view, o_s.at[it, to], o_r.at[it, src], dm=to)

    def repeat(f, n):
        return jnp.concatenate([f] * n, axis=1)

    def attend_x(it):
        for k in (1, 3, 2):
            x_copy(lax.rem(z + k, NZ), lax.rem(z + k, NZ), it).wait_recv()
        for e in range(2):
            load_c(0, 2 * it + e).wait()
            load_c(1, 2 * it + e).wait()
        dbuf[z, it] = part[z, it]
        terms = [dbuf[j, it] * repeat(fac[7 + j, 0, z], 6) for j in range(NZ)]
        attend(it, (terms[0] + terms[1]) + (terms[2] + terms[3]))

    def attend_y(it):
        attend(it, part[z, it] * repeat(fac[4, 1, z], 6) + (rbuf[z, it] * repeat(fac[5, 1, z], 6) + lbuf[z, it] * repeat(fac[6, 1, z], 6)))

    def attend(it, y):
        b, p = split(it)
        q, k, v_new = [jnp.concatenate([y[:, i * hd:(i + 1) * hd], y[:, (3 + i) * hd:(4 + i) * hd]], axis=0) for i in range(3)]
        cos2, sin2 = rope[0, b], rope[1, b]
        at_len = pos == len_v[b]
        seen = pos <= len_v[b]
        q = (q * cos2 + pltpu.roll(q, hd // 2, 1) * sin2).astype(BF16)
        k_new = (k * cos2 + pltpu.roll(k, hd // 2, 1) * sin2).astype(BF16).astype(F32)
        v_new = v_new.astype(BF16).astype(F32)
        s = jnp.zeros((2 * NP, slots), F32)
        for e in range(2):
            for r in range(NP):
                t = lax.dot_general(q, k_out[b * NP + r, 2 * p + e], (((1,), (1,)), ((), ())), preferred_element_type=F32)
                s = jnp.where(row == e * NP + r, t, s)
        s_new = jnp.sum(q.astype(F32) * k_new, axis=-1, keepdims=True)
        s = jnp.where(at_len, s_new, s) * (hd ** -0.5)
        s = jnp.where(seen, s, -1e30)
        ex = jnp.exp(s - jnp.max(s, axis=-1, keepdims=True))
        prob = (ex / jnp.sum(ex, axis=-1, keepdims=True)).astype(BF16).astype(F32)
        p_new = jnp.sum(jnp.where(at_len, prob, 0.0), axis=-1, keepdims=True)
        p_old = jnp.where(at_len, 0.0, prob).astype(BF16)
        acc = jnp.zeros((2 * NP, hd), F32)
        for e in range(2):
            for r in range(NP):
                t = jnp.dot(p_old, v_out[b * NP + r, 2 * p + e], preferred_element_type=F32)
                acc = jnp.where(row == e * NP + r, t, acc)
        acc = acc + p_new * v_new
        for e in range(2):
            h, at = 2 * p + e, slice(e * NP, (e + 1) * NP)
            new_kv[0, h, b] = k_new[at]
            new_kv[1, h, b] = v_new[at]
            o_x[b, z, h] = acc[at].astype(BF16)
        for k in (2, 1, 3):
            o_copy(z, lax.rem(z + k, NZ), it).start()

    where = lax.broadcasted_iota(jnp.int32, (slots, hd), 0)

    def patch(h, b):
        for r in range(NP):
            hit = where == lens[b * NP + r]
            for i, ref in enumerate((k_out, v_out)):
                fresh = jnp.broadcast_to(new_kv[i, h, b, r:r + 1, :], (slots, hd))
                ref[b * NP + r, h] = jnp.where(hit, fresh, ref[b * NP + r, h].astype(F32)).astype(BF16)

    mine = pl.ds(pl.multiple_of(core * side, side), side)
    other = pl.ds(pl.multiple_of((1 - core) * side, side), side)

    def a_copy(key, j):
        return remote(red.at[key, j, other], r1.at[key, j], a_s.at[key, j], a_r.at[key, j], tp=sib)

    def b_copy(key, j):
        return remote(s_buf.at[key, j], r2.at[key, j], b_s.at[key, j], b_r.at[key, j], tp=across)

    def c_copy(key, j, who):
        view = (h_mid, h_fin)[key // 2].at[key % 2, j, pl.ds(pl.multiple_of(who * side, side), side)]
        return remote(view, view, c_s.at[key, j], c_r.at[key, j], tp=sib)

    def o_gather(b):
        def wait(p, carry):
            it = b * n_pair + p
            for k in (1, 3, 2):
                o_copy(lax.rem(z + k, NZ), lax.rem(z + k, NZ), it).wait_recv()
            return carry

        lax.fori_loop(0, n_pair, wait, 0)
        o_cat[...] = jnp.concatenate([jnp.concatenate([o_x[b, d, h].astype(F32) for h in range(heads)], axis=1) for d in range(NZ)], axis=0).astype(BF16)

    def o_product(b, j):
        red[b, j] = jnp.dot(o_cat[...], wo_b[:, j * rcol:(j + 1) * rcol], preferred_element_type=F32)
        a_copy(b, j).start()

    def m_rows(b):
        return pl.ds(b * half, half)

    def stage_b(key):
        for j in range(n_red):
            a_copy(key, j).wait_recv()
            s_buf[key, j] = red[key, j, mine] + r1[key, j]
            b_copy(key, j).start()

    def stage_c(key):
        b = key % 2
        for j in range(n_red):
            b_copy(key, j).wait_recv()
            total = (s_buf[key, j] + r2[key, j]).astype(BF16).astype(F32)
            if key < 2:
                base = hid_p[pl.ds(pl.multiple_of(b * half + core * side, side), side), pl.ds(j * rcol, rcol)]
                h_mid[b, j, mine] = (base.astype(F32) + total).astype(BF16)
            else:
                h_fin[b, j, mine] = (h_mid[b, j, mine].astype(F32) + total).astype(BF16)
            c_copy(key, j, core).start()

    def stage_d(key):
        for j in range(n_red):
            c_copy(key, j, 1 - core).wait_recv()
        if key < 2:
            x = jnp.concatenate([h_mid[key, j].astype(F32) for j in range(n_red)], axis=1)
            local_norm(x, g2[...].astype(F32).reshape(1, width), 1 + key, key * half)

    def a_slot(t, carry):
        @pl.when(t < n_pair)
        def _():
            for e in range(2):
                for i in range(3):
                    load_w(i, 2 * t + e).wait()
            for e in range(2):
                h = 2 * t + e
                for i in range(3):
                    y = jnp.dot(x_buf[...], wbuf[i, h], preferred_element_type=F32)
                    for b in range(2):
                        for d in range(NZ):
                            lo = (b * NZ + d) * NP
                            part[d, b * n_pair + t, :, (3 * e + i) * hd:(3 * e + i + 1) * hd] = y[lo:lo + NP]

            for d in (3, 0, 2, 1):
                @pl.when(z != d)
                def _(d=d):
                    x_copy(z, d, t).start()

        @pl.when(t == n_pair)
        def _():
            a_stats()

        for d in (3, 2, 1):
            p = t - A_LAG * z - FAR * (NZ - 1 - d)

            @pl.when((p >= n_pair) & (p < n_a))
            def _(d=d, p=p):
                b = p // n_pair

                @pl.when((z > 0) & (z <= d))
                def _():
                    right(d, p).wait_recv()

                @pl.when((z > 0) & (z < d))
                def _():
                    part[d, p] = part[d, p] * repeat(fac[0, b, d], 6) + rbuf[d, p] * repeat(fac[1, b, d], 6)

                @pl.when(z < d)
                def _():
                    right(d, p).start()

        for d in (0, 1, 2):
            q = t - A_LAG * (NZ - 1 - z) - FAR * d

            @pl.when((q >= n_pair) & (q < n_a))
            def _(d=d, q=q):
                b = q // n_pair

                @pl.when((z < NZ - 1) & (z >= d))
                def _():
                    left(d, q).wait_recv()

                @pl.when((z < NZ - 1) & (z > d))
                def _():
                    part[d, q] = part[d, q] * repeat(fac[2, b, d], 6) + lbuf[d, q] * repeat(fac[3, b, d], 6)

                @pl.when(z > d)
                def _():
                    left(d, q).start()

        g = t - X_LAG

        @pl.when((g >= 0) & (g < n_pair))
        def _():
            attend_x(g)

        f = t - jnp.maximum(A_LAG * z + FAR * (NZ - 1 - z), A_LAG * (NZ - 1 - z) + FAR * z)

        @pl.when((f >= n_pair) & (f < n_a))
        def _():
            attend_y(f)

        o_at = n_pair - 1 + X_LAG + 2

        @pl.when(t == o_at)
        def _():
            load_o.wait()
            o_gather(0)
            for j in range(n_red):
                o_product(0, j)

        @pl.when(t == o_at + 2)
        def _():
            stage_b(0)

        return carry

    a_end = max(n_a + max(A_LAG, FAR) * (NZ - 1), n_pair + X_LAG + 4)
    lax.fori_loop(0, a_end, a_slot, 0)

    def patch_x(h, carry):
        patch(h, 0)
        return carry

    lax.fori_loop(0, heads, patch_x, 0)
    stage_c(0)
    stage_d(0)

    def right2(c):
        return remote(pbuf.at[c, 1], rbuf2.at[c], rs2.at[c], rr2.at[c], dm=nxt)

    def left2(c):
        return remote(pbuf.at[c, 0], lbuf2.at[c], ls2.at[c], lr2.at[c], dm=prv)

    def valid(c):
        return ((c >= 0) & (c < n_col)) | ((c >= second) & (c < n_e))

    def half_of(c):
        b = c // second
        return b, c - b * second

    def m_view(c, high):
        b, k = half_of(c)
        return mbuf.at[pl.ds(pl.multiple_of(b * half + high * side, side), side), pl.ds(pl.multiple_of(k * COL, COL), COL)]

    def m_left(c):
        return remote(m_view(c, 1), m_view(c, 1), mr_s.at[c], mr_r.at[c], dm=prv)

    def m_right(c):
        return remote(m_view(c, 0), m_view(c, 0), ml_s.at[c], ml_r.at[c], dm=nxt)

    def m_far(c, high, k):
        to = (NZ - 1 - k) if high else k
        recv = mr_r if high else ml_r
        return remote(m_view(c, high), m_view(c, high), far_s.at[high, c - direct_from, k - 2], recv.at[c], dm=to)

    def gated(a):
        g, u = a[:, :COL], a[:, COL:]
        return (g * (1.0 / (1.0 + jnp.exp(-g))) * u).astype(BF16)

    def wide(i, b, first):
        f = jnp.concatenate([fac[i, b, first], fac[i, b, first + 1]], axis=0)
        return repeat(f, 2 * COL // 128)

    def finish(c, high):
        b, k = half_of(c)
        mbuf[pl.ds(pl.multiple_of(b * half + high * side, side), side), pl.ds(pl.multiple_of(k * COL, COL), COL)] = gated(pbuf[c, high])

        @pl.when(c >= direct_from)
        def _():
            m_far(c, high, 3).start()
            m_far(c, high, 2).start()

        (m_left if high else m_right)(c).start()

    def e_slot(t, carry):
        @pl.when(valid(t))
        def _():
            b, k = half_of(t)

            @pl.when(b == 0)
            def _():
                load(0, k).wait()
                load(1, k).wait()

            cols = pl.ds(pl.multiple_of(k * COL, COL), COL)
            x = x_buf[pl.ds(pl.multiple_of(b * half, half), half), :]
            g = jnp.dot(x, wg_b[:, cols], preferred_element_type=F32)
            u = jnp.dot(x, wu_b[:, cols], preferred_element_type=F32)
            for s in range(2):
                pbuf[t, s, :, 0:COL] = g[s * side:(s + 1) * side]
                pbuf[t, s, :, COL:] = u[s * side:(s + 1) * side]

        c = t - E_LAG * z
        for step, first in ((1, 0), (2, second)):
            @pl.when(c == first)
            def _(step=step):
                relay_stat(step, 0, (step - 1,))

        @pl.when(valid(c))
        def _():
            b = c // second

            @pl.when(z > 0)
            def _():
                right2(c).wait_recv()
                pbuf[c, 1] = pbuf[c, 1] * wide(0, b, 2) + rbuf2[c] * wide(1, b, 2)

            @pl.when(z < NZ - 1)
            def _():
                right2(c).start()

            @pl.when(z == NZ - 1)
            def _():
                finish(c, 1)

        d = t - E_LAG * (NZ - 1 - z)
        for step, first in ((1, 0), (2, second)):
            @pl.when(d == first)
            def _(step=step):
                relay_stat(step, 1, (step - 1,))

        @pl.when(valid(d))
        def _():
            b = d // second

            @pl.when(z < NZ - 1)
            def _():
                left2(d).wait_recv()
                pbuf[d, 0] = pbuf[d, 0] * wide(2, b, 0) + lbuf2[d] * wide(3, b, 0)

            @pl.when(z > 0)
            def _():
                left2(d).start()

            @pl.when(z == 0)
            def _():
                finish(d, 0)

        e = t - E_LAG * (2 * NZ - 2 - z)

        @pl.when(valid(e) & (z < NZ - 1))
        def _():
            m_left(e).wait_recv()

            @pl.when((z > 0) & (e < direct_from))
            def _():
                m_left(e).start()

        f = t - E_LAG * (NZ - 1 + z)

        @pl.when(valid(f) & (z > 0))
        def _():
            m_right(f).wait_recv()

            @pl.when((z < NZ - 1) & (f < direct_from))
            def _():
                m_right(f).start()

        @pl.when(t == 1)
        def _():
            o_gather(1)
            for j in range(n_red):
                o_product(1, j)

        @pl.when(t == 2)
        def _():
            stage_b(1)

        @pl.when(t == 6)
        def _():
            stage_c(1)

        @pl.when(t == 8)
        def _():
            stage_d(1)

        @pl.when((t >= n_e) & (t < n_e + heads))
        def _():
            patch(t - n_e, 1)

        down = n_col + 2 * trip
        for j in range(n_red):
            @pl.when(t == down + j)
            def _(j=j):
                if j == 0:
                    load_d.wait()
                red[2, j] = jnp.dot(mbuf[m_rows(0), :], wd_b[:, j * rcol:(j + 1) * rcol], preferred_element_type=F32)
                a_copy(2, j).start()

        @pl.when(t == down + 2)
        def _():
            stage_b(2)

        late = second + early + 2 * trip
        for j in range(n_red):
            @pl.when(t == late + j)
            def _(j=j):
                red[3, j] = jnp.dot(mbuf[m_rows(1), 0:early * COL], wd_b[0:early * COL, j * rcol:(j + 1) * rcol], preferred_element_type=F32)

        return carry

    lax.fori_loop(0, max(n_e + 2 * trip, second + early + n_red + 2 * trip, n_e + heads, n_col + 2 * trip + 3), e_slot, 0)
    for j in range(n_red):
        red[3, j] = red[3, j] + jnp.dot(mbuf[m_rows(1), early * COL:], wd_b[early * COL:, j * rcol:(j + 1) * rcol], preferred_element_type=F32)
        a_copy(3, j).start()
    stage_c(2)
    stage_b(3)
    stage_d(2)

    def drain_a(p, carry):
        for d in range(NZ):
            @pl.when((p >= n_pair) & (z < d))
            def _(d=d):
                right(d, p).wait_send()

            @pl.when((p >= n_pair) & (z > d))
            def _(d=d):
                left(d, p).wait_send()

            @pl.when((p < n_pair) & (z != d))
            def _(d=d):
                x_copy(z, d, p).wait_send()

        for k in range(1, NZ):
            o_copy(z, lax.rem(z + k, NZ), p).wait_send()
        return carry

    lax.fori_loop(0, n_a, drain_a, 0)

    def drain_e(c, carry):
        @pl.when(valid(c))
        def _():
            @pl.when(z < NZ - 1)
            def _():
                right2(c).wait_send()

            @pl.when((z == 0) | ((z < NZ - 1) & (c < direct_from)))
            def _():
                m_right(c).wait_send()

            @pl.when(z > 0)
            def _():
                left2(c).wait_send()

            @pl.when((z == NZ - 1) | ((z > 0) & (c < direct_from)))
            def _():
                m_left(c).wait_send()

            for high in range(2):
                @pl.when((c >= direct_from) & (z == (NZ - 1) * high))
                def _(high=high):
                    m_far(c, high, 2).wait_send()
                    m_far(c, high, 3).wait_send()

        return carry

    lax.fori_loop(0, n_e, drain_e, 0)
    for k in range(1, NZ):
        sq_copy(z, lax.rem(z + k, NZ)).wait_send()
    for step in (1, 2):
        @pl.when(z < NZ - 1)
        def _(step=step):
            stat(step, 0).wait_send()

        @pl.when(z > 0)
        def _(step=step):
            stat(step, 1).wait_send()

    stage_c(3)
    stage_d(3)
    for b in range(2):
        y = jnp.concatenate([h_fin[b, j].astype(F32) for j in range(n_red)], axis=1)
        if b == 0:
            ys = [y]
        else:
            ys.append(y)
    out[...] = jnp.concatenate([ys[b][d * NP:(d + 1) * NP] for d in range(NZ) for b in range(2)], axis=0).astype(BF16)
    for key in range(4):
        for j in range(n_red):
            a_copy(key, j).wait_send()
            b_copy(key, j).wait_send()
            c_copy(key, j, core).wait_send()


def layer_call(hid, g1, g2, wq, wk, wv, wo, wg, wu, wd, kc, vc, lens, cos, sin):
    rows, width = hid.shape
    heads, hd = wq.shape[0], wq.shape[2]
    slots = kc.shape[2]
    ff = wg.shape[1]
    half = rows // 2
    side = half // 2
    n_a = heads
    n_col = ff // COL
    n_e = max(n_col, 9) + n_col
    n_red = 2
    rcol = width // n_red
    hbm = pl.BlockSpec(memory_space=pl.ANY)
    vm = pl.BlockSpec(memory_space=pltpu.VMEM)
    dma = pltpu.SemaphoreType.DMA
    sums = pltpu.VMEM((NZ, n_a, NP, 6 * hd), F32)
    act = pltpu.VMEM((rows, width), BF16)
    half_red = pltpu.VMEM((4, n_red, side, rcol), F32)
    h_halves = pltpu.VMEM((2, n_red, half, rcol), BF16)
    return pl.pallas_call(
        layer_kernel,
        name='layer',
        out_shape=[pltpu.VMEM((rows, width), BF16), pltpu.VMEM(kc.shape, BF16), pltpu.VMEM(vc.shape, BF16)],
        in_specs=[hbm] * 15,
        out_specs=[vm, vm, vm],
        scratch_shapes=[
            act, pltpu.VMEM(g1.shape, g1.dtype), pltpu.VMEM(g2.shape, g2.dtype), pltpu.SMEM(lens.shape, jnp.int32), pltpu.VMEM(cos.shape, F32), pltpu.VMEM(sin.shape, F32),
            act, pltpu.VMEM((2, 2 * NP, slots), jnp.int32), pltpu.VMEM((2, 2, 2 * NP, hd), F32),
            pltpu.VMEM((3, heads, width, hd), BF16),
            pltpu.VMEM(wo.shape, BF16), pltpu.VMEM(wg.shape, BF16), pltpu.VMEM(wu.shape, BF16), pltpu.VMEM(wd.shape, BF16),
            sums, sums, sums, pltpu.VMEM((NZ, heads // 2, NP, 6 * hd), F32),
            act, pltpu.VMEM((2, NZ, heads, NP, hd), BF16), pltpu.VMEM((half, width), BF16),
            pltpu.VMEM((2, heads, 2, NP, hd), F32),
            pltpu.VMEM((4, n_red, half, rcol), F32),
            half_red, half_red, half_red,
            h_halves, h_halves,
            pltpu.VMEM((n_e, 2, side, 2 * COL), F32),
            pltpu.VMEM((n_e, side, 2 * COL), F32),
            pltpu.VMEM((n_e, side, 2 * COL), F32),
            pltpu.VMEM((rows, ff), BF16),
            pltpu.VMEM((3, 2, 8, 128), F32), pltpu.VMEM((3, 2, 8, 128), F32), pltpu.VMEM((3, 8, 128), F32), pltpu.VMEM((NZ, 8, 128), F32),
            pltpu.VMEM((7 + NZ, 2, NZ, NP, 128), F32),
            dma((6,)), dma((3, heads)), dma((2, heads)), dma((2,)), dma((2, n_col)),
            dma((NZ, n_a)), dma((NZ, n_a)), dma((NZ, n_a)), dma((NZ, n_a)),
            dma((heads // 2, NZ)), dma((heads // 2, NZ)), dma((NZ,)), dma((NZ,)),
            dma((n_a, NZ)), dma((n_a, NZ)),
            dma((4, n_red)), dma((4, n_red)), dma((4, n_red)), dma((4, n_red)), dma((4, n_red)), dma((4, n_red)),
            dma((3, 2)), dma((3, 2)),
            dma((n_e,)), dma((n_e,)), dma((n_e,)), dma((n_e,)),
            dma((n_e,)), dma((n_e,)), dma((n_e,)), dma((n_e,)),
            dma((2, DIRECT, 2)),
        ],
        compiler_params=pltpu.CompilerParams(collective_id=0, has_side_effects=True, vmem_limit_bytes=VMEM_KIB * 1024),
    )(hid, g1, g2, wq, wk, wv, wo, wg, wu, wd, kc, vc, lens, cos, sin)


VMEM_KIB = 49 * 1024


def flush_kernel(h_in, k_in, v_in, h_out, k_out, v_out, sem):
    rows = k_in.shape[0] // FLUSH
    copies = [pltpu.make_async_copy(h_in, h_out, sem.at[2, 0])]
    for i in range(FLUSH):
        at = pl.ds(i * rows, rows)
        copies.append(pltpu.make_async_copy(k_in.at[at], k_out.at[at], sem.at[0, i]))
        copies.append(pltpu.make_async_copy(v_in.at[at], v_out.at[at], sem.at[1, i]))
    for cp in copies:
        cp.start()
    for cp in copies:
        cp.wait()


def flush_call(h, k, v):
    vm = pl.BlockSpec(memory_space=pltpu.VMEM)
    hbm = pl.BlockSpec(memory_space=pl.ANY)
    return pl.pallas_call(
        flush_kernel,
        name='flush',
        out_shape=[pltpu.HBM(a.shape, a.dtype) for a in (h, k, v)],
        in_specs=[vm] * 3,
        out_specs=[hbm] * 3,
        scratch_shapes=[pltpu.SemaphoreType.DMA((3, FLUSH))],
        compiler_params=pltpu.CompilerParams(vmem_limit_bytes=2**20),
    )(h, k, v)


FLUSH = 4


def solution(mesh):
    row_spec = P('dp', 'dm')
    cache_spec = P(('dp', 'dm'), None, 'tp', None)
    batch_spec = P(('dp', 'dm'))
    rope_spec = P(('dp', 'dm'), None)
    in_specs = (row_spec, P('dm', 'tp', None), P('dm', 'tp', None), P('dm', 'tp', None), P('tp', None, 'dm'), P('dm', 'tp'), P('dm', 'tp'), P('tp', 'dm'), P('dm'), P('dm'), cache_spec, cache_spec, batch_spec, rope_spec, rope_spec)
    out_specs = (row_spec, cache_spec, cache_spec)

    def local_layer(hidden, w_q, w_k, w_v, w_o, w_gate, w_up, w_down, norm_attn, norm_mlp, k_cache, v_cache, seq_lens, rope_cos, rope_sin):
        by_head = [w.transpose(1, 0, 2) for w in (w_q, w_k, w_v)]
        caches = [c.transpose(0, 2, 1, 3) for c in (k_cache, v_cache)]
        h_out, k_out, v_out = layer_call(hidden, norm_attn, norm_mlp, *by_head, w_o.reshape(-1, w_o.shape[-1]), w_gate, w_up, w_down, *caches, seq_lens, rope_cos, rope_sin)
        h_out, k_out, v_out = flush_call(h_out, k_out, v_out)
        return h_out, k_out.transpose(0, 2, 1, 3), v_out.transpose(0, 2, 1, 3)

    return jax.shard_map(local_layer, mesh=mesh, in_specs=in_specs, out_specs=out_specs, check_vma=False)
```

```python
import jax
import jax.numpy as jnp
from jax import lax
from jax.experimental import pallas as pl
from jax.experimental.pallas import tpu as pltpu
from jax.sharding import PartitionSpec as P

EPS = 1e-6
MESH = pl.DeviceIdType.MESH
F32 = jnp.float32
BF16 = jnp.bfloat16
NZ = 4
NP = 8
A_LAG = 2
E_LAG = 3
COL = 384
DIRECT = 4


def remote(src, dst, send_sem, recv_sem, **where):
    return pltpu.make_async_remote_copy(src_ref=src, dst_ref=dst, send_sem=send_sem, recv_sem=recv_sem, device_id=where, device_id_type=MESH)


def partner(tp, k):
    if k == 1:
        return tp + 1 - 2 * lax.rem(tp, 2)
    return lax.rem(tp + 2, 4)


def pack_rows(col):
    rows = col.shape[0]
    lane = lax.broadcasted_iota(jnp.int32, (rows, 128), 1)
    row = lax.broadcasted_iota(jnp.int32, (rows, 128), 0)
    packed = jnp.sum(jnp.where(lane == row, col, 0.0), axis=0, keepdims=True)
    return jnp.broadcast_to(packed, (8, 128))


def unpack_rows(tile, rows):
    lane = lax.broadcasted_iota(jnp.int32, (rows, 128), 1)
    row = lax.broadcasted_iota(jnp.int32, (rows, 128), 0)
    wide = jnp.broadcast_to(tile[0:1], (rows, 128))
    return jnp.sum(jnp.where(lane == row, wide, 0.0), axis=1, keepdims=True)


def layer_kernel(hid_h, g1_h, g2_h, wq, wk, wv, wo, wg, wu, wd, kc, vc, lens_h, cos_h, sin_h,
                 out, k_out, v_out,
                 hid, g1, g2, lens, cos, sin, hid_p, len_v, rope, wbuf, wo_b, wg_b, wu_b, wd_b,
                 part, rbuf, lbuf, x_buf, o_x, o_cat, new_kv, red, r1, s_buf, r2, h_mid, h_fin, pbuf, rbuf2, lbuf2, mbuf,
                 cum_in, cum_out, own_sq, fac,
                 s_sem, w_sem, c_sem, b_sem, g_sem, rs, rr, ls, lr, o_s, o_r, a_s, a_r, b_s, b_r, c_s, c_r,
                 q_s, q_r, rs2, rr2, ls2, lr2, mr_s, mr_r, ml_s, ml_r, far_s):
    z = lax.axis_index('dm')
    tp = lax.axis_index('tp')
    rows, width = hid.shape
    full = width * NZ
    heads = wq.shape[0]
    hd = wq.shape[2]
    per = rows // NZ
    half = rows // 2
    side = half // 2
    slots = kc.shape[2]
    ff = wg.shape[1]
    n_pair = heads // 2
    n_a = 2 * n_pair
    n_col = ff // COL
    second = max(n_col, 9)
    n_e = second + n_col
    trip = E_LAG * (NZ - 1)
    n_grp = g_sem.shape[1]
    n_red = red.shape[1]
    rcol = width // n_red
    early = n_col * 2 // 3
    direct_from = n_e - DIRECT
    core = lax.rem(tp, 2)
    sib, across = partner(tp, 1), partner(tp, 2)
    nxt, prv = lax.rem(z + 1, NZ), lax.rem(z + NZ - 1, NZ)

    small = [pltpu.make_async_copy(a, b, s_sem.at[i]) for i, (a, b) in enumerate(((hid_h, hid), (g1_h, g1), (g2_h, g2), (cos_h, cos), (sin_h, sin), (lens_h, lens)))]
    load_o = pltpu.make_async_copy(wo, wo_b, b_sem.at[0])
    load_d = pltpu.make_async_copy(wd, wd_b, b_sem.at[1])

    def load_w(i, h):
        return pltpu.make_async_copy((wq, wk, wv)[i].at[h], wbuf.at[i, h], w_sem.at[i, h])

    def load_c(i, h):
        return pltpu.make_async_copy((kc, vc)[i].at[:, h], (k_out, v_out)[i].at[:, h], c_sem.at[i, h])

    def load(i, g):
        src, dst = ((wg, wg_b), (wu, wu_b))[i]
        cols = pl.ds(pl.multiple_of(g * COL, COL), COL)
        return pltpu.make_async_copy(src.at[:, cols], dst.at[:, cols], g_sem.at[i, g])

    for cp in small:
        cp.start()
    def load_pair(p):
        for e in range(2):
            for i in range(3):
                load_w(i, 2 * p + e).start()

    for p in range(min(n_pair, 2)):
        load_pair(p)

    sem = pltpu.get_barrier_semaphore()
    for k in range(1, NZ):
        pl.semaphore_signal(sem, inc=1, device_id={'dm': lax.rem(z + k, NZ)}, device_id_type=MESH)
    for k in (1, 2):
        pl.semaphore_signal(sem, inc=1, device_id={'tp': partner(tp, k)}, device_id_type=MESH)

    for cp in small:
        cp.wait()

    def inv(tile):
        return lax.rsqrt(tile / full + EPS)

    def local_norm(x, gain, step, lo):
        col = jnp.sum(x * x, axis=-1, keepdims=True)
        own_sq[step] = pack_rows(col)
        x_buf[lo:lo + x.shape[0]] = (x * lax.rsqrt(col / full + EPS) * gain).astype(BF16)

    def place(b, d):
        return d * per + b * NP

    x0 = hid[...].astype(F32)
    x0 = jnp.concatenate([x0[place(b, d):place(b, d) + NP] for b in range(2) for d in range(NZ)], axis=0)
    hid_p[...] = x0.astype(BF16)
    local_norm(x0, g1[...].astype(F32).reshape(1, width), 0, 0)
    cs, sn = cos[...], sin[...]
    row = lax.broadcasted_iota(jnp.int32, (2 * NP, slots), 0)
    pos = lax.broadcasted_iota(jnp.int32, (2 * NP, slots), 1)
    for b in range(2):
        part_cs, part_sn = [jnp.concatenate([t[b * NP:(b + 1) * NP]] * 2, axis=0) for t in (cs, sn)]
        rope[0, b] = jnp.concatenate([part_cs, part_cs], axis=-1)
        rope[1, b] = jnp.concatenate([-part_sn, part_sn], axis=-1)
        length = jnp.zeros((2 * NP, slots), jnp.int32)
        for r in range(NP):
            length = jnp.where((row == r) | (row == NP + r), lens[b * NP + r], length)
        len_v[b] = length

    def stat(step, way):
        return remote(cum_out.at[step, way], cum_in.at[step, way], q_s.at[step, way], q_r.at[step, way], dm=(nxt, prv)[way])

    def put_fac(i, tile, halves):
        n = len(halves) * half
        wide = jnp.broadcast_to(unpack_rows(tile, n), (n, 128))
        for k, b in enumerate(halves):
            for d in range(NZ):
                lo = (k * NZ + d) * NP
                fac[i, b, d] = wide[lo:lo + NP]

    def relay_stat(step, way, halves):
        has_in = (z > 0) if way == 0 else (z < NZ - 1)
        has_out = (z < NZ - 1) if way == 0 else (z > 0)

        @pl.when(has_in)
        def _():
            stat(step, way).wait_recv()

        @pl.when(jnp.logical_not(has_in))
        def _():
            cum_in[step, way] = jnp.zeros((8, 128), F32)

        before, own = cum_in[step, way], own_sq[step]
        cum = before + own
        cum_out[step, way] = cum

        @pl.when(has_out)
        def _():
            stat(step, way).start()

        scale = inv(cum)
        put_fac(2 * way, scale / inv(own), halves)
        put_fac(2 * way + 1, scale / inv(before), halves)

    @pl.when(z == 0)
    def _():
        rbuf[0] = jnp.zeros(rbuf.shape[1:], F32)

    @pl.when(z == NZ - 1)
    def _():
        lbuf[NZ - 1] = jnp.zeros(lbuf.shape[1:], F32)

    pl.semaphore_wait(sem, NZ + 1)

    def right(d, p):
        return remote(part.at[d, p], rbuf.at[d, p], rs.at[d, p], rr.at[d, p], dm=nxt)

    def left(d, p):
        return remote(part.at[d, p], lbuf.at[d, p], ls.at[d, p], lr.at[d, p], dm=prv)

    def split(it):
        b = it // n_pair
        return b, it - b * n_pair

    def o_copy(src, to, it):
        b, p = split(it)
        view = o_x.at[b, src, pl.ds(2 * p, 2)]
        return remote(view, view, o_s.at[it, to], o_r.at[it, src], dm=to)

    def repeat(f, n):
        return jnp.concatenate([f] * n, axis=1)

    def attend(it):
        b, p = split(it)
        y = part[z, it] * repeat(fac[4, b, z], 6) + (rbuf[z, it] * repeat(fac[5, b, z], 6) + lbuf[z, it] * repeat(fac[6, b, z], 6))

        @pl.when(b == 0)
        def _():
            for e in range(2):
                load_c(0, 2 * p + e).wait()
                load_c(1, 2 * p + e).wait()

        q, k, v_new = [jnp.concatenate([y[:, i * hd:(i + 1) * hd], y[:, (3 + i) * hd:(4 + i) * hd]], axis=0) for i in range(3)]
        cos2, sin2 = rope[0, b], rope[1, b]
        at_len = pos == len_v[b]
        seen = pos <= len_v[b]
        q = (q * cos2 + pltpu.roll(q, hd // 2, 1) * sin2).astype(BF16)
        k_new = (k * cos2 + pltpu.roll(k, hd // 2, 1) * sin2).astype(BF16).astype(F32)
        v_new = v_new.astype(BF16).astype(F32)
        s = jnp.zeros((2 * NP, slots), F32)
        for e in range(2):
            for r in range(NP):
                t = lax.dot_general(q, k_out[b * NP + r, 2 * p + e], (((1,), (1,)), ((), ())), preferred_element_type=F32)
                s = jnp.where(row == e * NP + r, t, s)
        s_new = jnp.sum(q.astype(F32) * k_new, axis=-1, keepdims=True)
        s = jnp.where(at_len, s_new, s) * (hd ** -0.5)
        s = jnp.where(seen, s, -1e30)
        ex = jnp.exp(s - jnp.max(s, axis=-1, keepdims=True))
        prob = (ex / jnp.sum(ex, axis=-1, keepdims=True)).astype(BF16).astype(F32)
        p_new = jnp.sum(jnp.where(at_len, prob, 0.0), axis=-1, keepdims=True)
        p_old = jnp.where(at_len, 0.0, prob).astype(BF16)
        acc = jnp.zeros((2 * NP, hd), F32)
        for e in range(2):
            for r in range(NP):
                t = jnp.dot(p_old, v_out[b * NP + r, 2 * p + e], preferred_element_type=F32)
                acc = jnp.where(row == e * NP + r, t, acc)
        acc = acc + p_new * v_new
        for e in range(2):
            h, at = 2 * p + e, slice(e * NP, (e + 1) * NP)
            new_kv[0, h, b] = k_new[at]
            new_kv[1, h, b] = v_new[at]
            o_x[b, z, h] = acc[at].astype(BF16)
        for k in (2, 1, 3):
            o_copy(z, lax.rem(z + k, NZ), it).start()

    where = lax.broadcasted_iota(jnp.int32, (slots, hd), 0)

    def patch(h, b):
        for r in range(NP):
            hit = where == lens[b * NP + r]
            for i, ref in enumerate((k_out, v_out)):
                fresh = jnp.broadcast_to(new_kv[i, h, b, r:r + 1, :], (slots, hd))
                ref[b * NP + r, h] = jnp.where(hit, fresh, ref[b * NP + r, h].astype(F32)).astype(BF16)

    mine = pl.ds(pl.multiple_of(core * side, side), side)
    other = pl.ds(pl.multiple_of((1 - core) * side, side), side)

    def a_copy(key, j):
        return remote(red.at[key, j, other], r1.at[key, j], a_s.at[key, j], a_r.at[key, j], tp=sib)

    def b_copy(key, j):
        return remote(s_buf.at[key, j], r2.at[key, j], b_s.at[key, j], b_r.at[key, j], tp=across)

    def c_copy(key, j, who):
        view = (h_mid, h_fin)[key // 2].at[key % 2, j, pl.ds(pl.multiple_of(who * side, side), side)]
        return remote(view, view, c_s.at[key, j], c_r.at[key, j], tp=sib)

    def o_gather(b):
        def wait(p, carry):
            it = b * n_pair + p
            for k in (1, 3, 2):
                o_copy(lax.rem(z + k, NZ), lax.rem(z + k, NZ), it).wait_recv()
            return carry

        lax.fori_loop(0, n_pair, wait, 0)
        o_cat[...] = jnp.concatenate([jnp.concatenate([o_x[b, d, h].astype(F32) for h in range(heads)], axis=1) for d in range(NZ)], axis=0).astype(BF16)

    def o_product(b, j):
        red[b, j] = jnp.dot(o_cat[...], wo_b[:, j * rcol:(j + 1) * rcol], preferred_element_type=F32)
        a_copy(b, j).start()

    def m_rows(b):
        return pl.ds(b * half, half)

    def stage_b(key):
        for j in range(n_red):
            a_copy(key, j).wait_recv()
            s_buf[key, j] = red[key, j, mine] + r1[key, j]
            b_copy(key, j).start()

    def stage_c(key):
        b = key % 2
        for j in range(n_red):
            b_copy(key, j).wait_recv()
            total = (s_buf[key, j] + r2[key, j]).astype(BF16).astype(F32)
            if key < 2:
                base = hid_p[pl.ds(pl.multiple_of(b * half + core * side, side), side), pl.ds(j * rcol, rcol)]
                h_mid[b, j, mine] = (base.astype(F32) + total).astype(BF16)
            else:
                h_fin[b, j, mine] = (h_mid[b, j, mine].astype(F32) + total).astype(BF16)
            c_copy(key, j, core).start()

    def stage_d(key):
        for j in range(n_red):
            c_copy(key, j, 1 - core).wait_recv()
        if key < 2:
            x = jnp.concatenate([h_mid[key, j].astype(F32) for j in range(n_red)], axis=1)
            local_norm(x, g2[...].astype(F32).reshape(1, width), 1 + key, key * half)

    a_end = max(n_a + A_LAG * (NZ - 1), n_pair + A_LAG * (NZ - 1) + 3, n_col + 7)

    def a_slot(t, carry):
        @pl.when(t + 2 < n_pair)
        def _():
            load_pair(t + 2)

        @pl.when((t >= 3) & (t < 3 + n_pair))
        def _():
            for e in range(2):
                load_c(0, 2 * (t - 3) + e).start()
                load_c(1, 2 * (t - 3) + e).start()

        @pl.when(t == 7)
        def _():
            load_o.start()

        @pl.when((t >= 7) & (t < 7 + n_col))
        def _():
            load(0, t - 7).start()
            load(1, t - 7).start()

        @pl.when(t == a_end - 1)
        def _():
            load_d.start()

        @pl.when(t < n_pair)
        def _():
            for e in range(2):
                for i in range(3):
                    load_w(i, 2 * t + e).wait()
            for e in range(2):
                h = 2 * t + e
                for i in range(3):
                    y = jnp.dot(x_buf[...], wbuf[i, h], preferred_element_type=F32)
                    for b in range(2):
                        for d in range(NZ):
                            lo = (b * NZ + d) * NP
                            part[d, b * n_pair + t, :, (3 * e + i) * hd:(3 * e + i + 1) * hd] = y[lo:lo + NP]

        @pl.when(t == A_LAG * z)
        def _():
            relay_stat(0, 0, (0, 1))

        for d in (3, 2, 1):
            p = t - A_LAG * z - (NZ - 1 - d)

            @pl.when((p >= 0) & (p < n_a))
            def _(d=d, p=p):
                b = p // n_pair

                @pl.when((z > 0) & (z <= d))
                def _():
                    right(d, p).wait_recv()

                @pl.when((z > 0) & (z < d))
                def _():
                    part[d, p] = part[d, p] * repeat(fac[0, b, d], 6) + rbuf[d, p] * repeat(fac[1, b, d], 6)

                @pl.when(z < d)
                def _():
                    right(d, p).start()

        @pl.when(t == A_LAG * (NZ - 1 - z))
        def _():
            relay_stat(0, 1, (0, 1))

        for d in (0, 1, 2):
            q = t - A_LAG * (NZ - 1 - z) - d

            @pl.when((q >= 0) & (q < n_a))
            def _(d=d, q=q):
                b = q // n_pair

                @pl.when((z < NZ - 1) & (z >= d))
                def _():
                    left(d, q).wait_recv()

                @pl.when((z < NZ - 1) & (z > d))
                def _():
                    part[d, q] = part[d, q] * repeat(fac[2, b, d], 6) + lbuf[d, q] * repeat(fac[3, b, d], 6)

                @pl.when(z > d)
                def _():
                    left(d, q).start()

        f = t - jnp.maximum(A_LAG * z + NZ - 1 - z, A_LAG * (NZ - 1 - z) + z)

        @pl.when(f == 0)
        def _():
            own = own_sq[0]
            scale = inv((cum_in[0, 0] + own) + cum_in[0, 1])
            put_fac(4, scale / inv(own), (0, 1))
            put_fac(5, scale / inv(cum_in[0, 0]), (0, 1))
            put_fac(6, scale / inv(cum_in[0, 1]), (0, 1))

        @pl.when((f >= 0) & (f < n_a))
        def _():
            attend(f)

        o_at = n_pair - 1 + A_LAG * (NZ - 1) + 2

        @pl.when(t == o_at)
        def _():
            load_o.wait()
            o_gather(0)
            for j in range(n_red):
                o_product(0, j)

        @pl.when(t == o_at + 1)
        def _():
            stage_b(0)

        return carry

    lax.fori_loop(0, a_end, a_slot, 0)

    def patch_x(h, carry):
        patch(h, 0)
        return carry

    lax.fori_loop(0, heads, patch_x, 0)
    stage_c(0)
    stage_d(0)

    def right2(c):
        return remote(pbuf.at[c, 1], rbuf2.at[c], rs2.at[c], rr2.at[c], dm=nxt)

    def left2(c):
        return remote(pbuf.at[c, 0], lbuf2.at[c], ls2.at[c], lr2.at[c], dm=prv)

    def valid(c):
        return ((c >= 0) & (c < n_col)) | ((c >= second) & (c < n_e))

    def half_of(c):
        b = c // second
        return b, c - b * second

    def m_view(c, high):
        b, k = half_of(c)
        return mbuf.at[pl.ds(pl.multiple_of(b * half + high * side, side), side), pl.ds(pl.multiple_of(k * COL, COL), COL)]

    def m_left(c):
        return remote(m_view(c, 1), m_view(c, 1), mr_s.at[c], mr_r.at[c], dm=prv)

    def m_right(c):
        return remote(m_view(c, 0), m_view(c, 0), ml_s.at[c], ml_r.at[c], dm=nxt)

    def m_far(c, high, k):
        to = (NZ - 1 - k) if high else k
        recv = mr_r if high else ml_r
        return remote(m_view(c, high), m_view(c, high), far_s.at[high, c - direct_from, k - 2], recv.at[c], dm=to)

    def gated(a):
        g, u = a[:, :COL], a[:, COL:]
        return (g * (1.0 / (1.0 + jnp.exp(-g))) * u).astype(BF16)

    def wide(i, b, first):
        f = jnp.concatenate([fac[i, b, first], fac[i, b, first + 1]], axis=0)
        return repeat(f, 2 * COL // 128)

    def finish(c, high):
        b, k = half_of(c)
        mbuf[pl.ds(pl.multiple_of(b * half + high * side, side), side), pl.ds(pl.multiple_of(k * COL, COL), COL)] = gated(pbuf[c, high])

        @pl.when(c >= direct_from)
        def _():
            m_far(c, high, 3).start()
            m_far(c, high, 2).start()

        (m_left if high else m_right)(c).start()

    def e_slot(t, carry):
        @pl.when(valid(t))
        def _():
            b, k = half_of(t)

            @pl.when(b == 0)
            def _():
                load(0, k).wait()
                load(1, k).wait()

            cols = pl.ds(pl.multiple_of(k * COL, COL), COL)
            x = x_buf[pl.ds(pl.multiple_of(b * half, half), half), :]
            g = jnp.dot(x, wg_b[:, cols], preferred_element_type=F32)
            u = jnp.dot(x, wu_b[:, cols], preferred_element_type=F32)
            for s in range(2):
                pbuf[t, s, :, 0:COL] = g[s * side:(s + 1) * side]
                pbuf[t, s, :, COL:] = u[s * side:(s + 1) * side]

        c = t - E_LAG * z
        for step, first in ((1, 0), (2, second)):
            @pl.when(c == first)
            def _(step=step):
                relay_stat(step, 0, (step - 1,))

        @pl.when(valid(c))
        def _():
            b = c // second

            @pl.when(z > 0)
            def _():
                right2(c).wait_recv()
                pbuf[c, 1] = pbuf[c, 1] * wide(0, b, 2) + rbuf2[c] * wide(1, b, 2)

            @pl.when(z < NZ - 1)
            def _():
                right2(c).start()

            @pl.when(z == NZ - 1)
            def _():
                finish(c, 1)

        d = t - E_LAG * (NZ - 1 - z)
        for step, first in ((1, 0), (2, second)):
            @pl.when(d == first)
            def _(step=step):
                relay_stat(step, 1, (step - 1,))

        @pl.when(valid(d))
        def _():
            b = d // second

            @pl.when(z < NZ - 1)
            def _():
                left2(d).wait_recv()
                pbuf[d, 0] = pbuf[d, 0] * wide(2, b, 0) + lbuf2[d] * wide(3, b, 0)

            @pl.when(z > 0)
            def _():
                left2(d).start()

            @pl.when(z == 0)
            def _():
                finish(d, 0)

        e = t - E_LAG * (2 * NZ - 2 - z)

        @pl.when(valid(e) & (z < NZ - 1))
        def _():
            m_left(e).wait_recv()

            @pl.when((z > 0) & (e < direct_from))
            def _():
                m_left(e).start()

        f = t - E_LAG * (NZ - 1 + z)

        @pl.when(valid(f) & (z > 0))
        def _():
            m_right(f).wait_recv()

            @pl.when((z < NZ - 1) & (f < direct_from))
            def _():
                m_right(f).start()

        @pl.when(t == 1)
        def _():
            o_gather(1)
            for j in range(n_red):
                o_product(1, j)

        @pl.when(t == 2)
        def _():
            stage_b(1)

        @pl.when(t == 6)
        def _():
            stage_c(1)

        @pl.when(t == 8)
        def _():
            stage_d(1)

        @pl.when((t >= n_e) & (t < n_e + heads))
        def _():
            patch(t - n_e, 1)

        down = n_col + 2 * trip
        for j in range(n_red):
            @pl.when(t == down + j)
            def _(j=j):
                if j == 0:
                    load_d.wait()
                red[2, j] = jnp.dot(mbuf[m_rows(0), :], wd_b[:, j * rcol:(j + 1) * rcol], preferred_element_type=F32)
                a_copy(2, j).start()

        @pl.when(t == down + 2)
        def _():
            stage_b(2)

        late = second + early + 2 * trip
        for j in range(n_red):
            @pl.when(t == late + j)
            def _(j=j):
                red[3, j] = jnp.dot(mbuf[m_rows(1), 0:early * COL], wd_b[0:early * COL, j * rcol:(j + 1) * rcol], preferred_element_type=F32)

        return carry

    lax.fori_loop(0, max(n_e + 2 * trip, second + early + n_red + 2 * trip, n_e + heads, n_col + 2 * trip + 3), e_slot, 0)
    for j in range(n_red):
        red[3, j] = red[3, j] + jnp.dot(mbuf[m_rows(1), early * COL:], wd_b[early * COL:, j * rcol:(j + 1) * rcol], preferred_element_type=F32)
        a_copy(3, j).start()
    stage_c(2)
    stage_b(3)
    stage_d(2)

    def drain_a(p, carry):
        for d in range(NZ):
            @pl.when(z < d)
            def _(d=d):
                right(d, p).wait_send()

            @pl.when(z > d)
            def _(d=d):
                left(d, p).wait_send()

        for k in range(1, NZ):
            o_copy(z, lax.rem(z + k, NZ), p).wait_send()
        return carry

    lax.fori_loop(0, n_a, drain_a, 0)

    def drain_e(c, carry):
        @pl.when(valid(c))
        def _():
            @pl.when(z < NZ - 1)
            def _():
                right2(c).wait_send()

            @pl.when((z == 0) | ((z < NZ - 1) & (c < direct_from)))
            def _():
                m_right(c).wait_send()

            @pl.when(z > 0)
            def _():
                left2(c).wait_send()

            @pl.when((z == NZ - 1) | ((z > 0) & (c < direct_from)))
            def _():
                m_left(c).wait_send()

            for high in range(2):
                @pl.when((c >= direct_from) & (z == (NZ - 1) * high))
                def _(high=high):
                    m_far(c, high, 2).wait_send()
                    m_far(c, high, 3).wait_send()

        return carry

    lax.fori_loop(0, n_e, drain_e, 0)
    for step in range(3):
        @pl.when(z < NZ - 1)
        def _(step=step):
            stat(step, 0).wait_send()

        @pl.when(z > 0)
        def _(step=step):
            stat(step, 1).wait_send()

    stage_c(3)
    stage_d(3)
    for b in range(2):
        y = jnp.concatenate([h_fin[b, j].astype(F32) for j in range(n_red)], axis=1)
        if b == 0:
            ys = [y]
        else:
            ys.append(y)
    out[...] = jnp.concatenate([ys[b][d * NP:(d + 1) * NP] for d in range(NZ) for b in range(2)], axis=0).astype(BF16)
    for key in range(4):
        for j in range(n_red):
            a_copy(key, j).wait_send()
            b_copy(key, j).wait_send()
            c_copy(key, j, core).wait_send()


def layer_call(hid, g1, g2, wq, wk, wv, wo, wg, wu, wd, kc, vc, lens, cos, sin):
    rows, width = hid.shape
    heads, hd = wq.shape[0], wq.shape[2]
    slots = kc.shape[2]
    ff = wg.shape[1]
    half = rows // 2
    side = half // 2
    n_a = heads
    n_col = ff // COL
    n_e = max(n_col, 9) + n_col
    n_red = 2
    rcol = width // n_red
    hbm = pl.BlockSpec(memory_space=pl.ANY)
    vm = pl.BlockSpec(memory_space=pltpu.VMEM)
    dma = pltpu.SemaphoreType.DMA
    sums = pltpu.VMEM((NZ, n_a, NP, 6 * hd), F32)
    act = pltpu.VMEM((rows, width), BF16)
    half_red = pltpu.VMEM((4, n_red, side, rcol), F32)
    h_halves = pltpu.VMEM((2, n_red, half, rcol), BF16)
    return pl.pallas_call(
        layer_kernel,
        name='layer',
        out_shape=[pltpu.VMEM((rows, width), BF16), pltpu.VMEM(kc.shape, BF16), pltpu.VMEM(vc.shape, BF16)],
        in_specs=[hbm] * 15,
        out_specs=[vm, vm, vm],
        scratch_shapes=[
            act, pltpu.VMEM(g1.shape, g1.dtype), pltpu.VMEM(g2.shape, g2.dtype), pltpu.SMEM(lens.shape, jnp.int32), pltpu.VMEM(cos.shape, F32), pltpu.VMEM(sin.shape, F32),
            act, pltpu.VMEM((2, 2 * NP, slots), jnp.int32), pltpu.VMEM((2, 2, 2 * NP, hd), F32),
            pltpu.VMEM((3, heads, width, hd), BF16),
            pltpu.VMEM(wo.shape, BF16), pltpu.VMEM(wg.shape, BF16), pltpu.VMEM(wu.shape, BF16), pltpu.VMEM(wd.shape, BF16),
            sums, sums, sums,
            act, pltpu.VMEM((2, NZ, heads, NP, hd), BF16), pltpu.VMEM((half, width), BF16),
            pltpu.VMEM((2, heads, 2, NP, hd), F32),
            pltpu.VMEM((4, n_red, half, rcol), F32),
            half_red, half_red, half_red,
            h_halves, h_halves,
            pltpu.VMEM((n_e, 2, side, 2 * COL), F32),
            pltpu.VMEM((n_e, side, 2 * COL), F32),
            pltpu.VMEM((n_e, side, 2 * COL), F32),
            pltpu.VMEM((rows, ff), BF16),
            pltpu.VMEM((3, 2, 8, 128), F32), pltpu.VMEM((3, 2, 8, 128), F32), pltpu.VMEM((3, 8, 128), F32),
            pltpu.VMEM((7, 2, NZ, NP, 128), F32),
            dma((6,)), dma((3, heads)), dma((2, heads)), dma((2,)), dma((2, n_col)),
            dma((NZ, n_a)), dma((NZ, n_a)), dma((NZ, n_a)), dma((NZ, n_a)),
            dma((n_a, NZ)), dma((n_a, NZ)),
            dma((4, n_red)), dma((4, n_red)), dma((4, n_red)), dma((4, n_red)), dma((4, n_red)), dma((4, n_red)),
            dma((3, 2)), dma((3, 2)),
            dma((n_e,)), dma((n_e,)), dma((n_e,)), dma((n_e,)),
            dma((n_e,)), dma((n_e,)), dma((n_e,)), dma((n_e,)),
            dma((2, DIRECT, 2)),
        ],
        compiler_params=pltpu.CompilerParams(collective_id=0, has_side_effects=True, vmem_limit_bytes=VMEM_KIB * 1024),
    )(hid, g1, g2, wq, wk, wv, wo, wg, wu, wd, kc, vc, lens, cos, sin)


VMEM_KIB = 49 * 1024


def flush_kernel(h_in, k_in, v_in, h_out, k_out, v_out, sem):
    rows = k_in.shape[0] // FLUSH
    copies = [pltpu.make_async_copy(h_in, h_out, sem.at[2, 0])]
    for i in range(FLUSH):
        at = pl.ds(i * rows, rows)
        copies.append(pltpu.make_async_copy(k_in.at[at], k_out.at[at], sem.at[0, i]))
        copies.append(pltpu.make_async_copy(v_in.at[at], v_out.at[at], sem.at[1, i]))
    for cp in copies:
        cp.start()
    for cp in copies:
        cp.wait()


def flush_call(h, k, v):
    vm = pl.BlockSpec(memory_space=pltpu.VMEM)
    hbm = pl.BlockSpec(memory_space=pl.ANY)
    return pl.pallas_call(
        flush_kernel,
        name='flush',
        out_shape=[pltpu.HBM(a.shape, a.dtype) for a in (h, k, v)],
        in_specs=[vm] * 3,
        out_specs=[hbm] * 3,
        scratch_shapes=[pltpu.SemaphoreType.DMA((3, FLUSH))],
        compiler_params=pltpu.CompilerParams(vmem_limit_bytes=2**20),
    )(h, k, v)


FLUSH = 4


def solution(mesh):
    row_spec = P('dp', 'dm')
    cache_spec = P(('dp', 'dm'), None, 'tp', None)
    batch_spec = P(('dp', 'dm'))
    rope_spec = P(('dp', 'dm'), None)
    in_specs = (row_spec, P('dm', 'tp', None), P('dm', 'tp', None), P('dm', 'tp', None), P('tp', None, 'dm'), P('dm', 'tp'), P('dm', 'tp'), P('tp', 'dm'), P('dm'), P('dm'), cache_spec, cache_spec, batch_spec, rope_spec, rope_spec)
    out_specs = (row_spec, cache_spec, cache_spec)

    def local_layer(hidden, w_q, w_k, w_v, w_o, w_gate, w_up, w_down, norm_attn, norm_mlp, k_cache, v_cache, seq_lens, rope_cos, rope_sin):
        by_head = [w.transpose(1, 0, 2) for w in (w_q, w_k, w_v)]
        caches = [c.transpose(0, 2, 1, 3) for c in (k_cache, v_cache)]
        h_out, k_out, v_out = layer_call(hidden, norm_attn, norm_mlp, *by_head, w_o.reshape(-1, w_o.shape[-1]), w_gate, w_up, w_down, *caches, seq_lens, rope_cos, rope_sin)
        h_out, k_out, v_out = flush_call(h_out, k_out, v_out)
        return h_out, k_out.transpose(0, 2, 1, 3), v_out.transpose(0, 2, 1, 3)

    return jax.shard_map(local_layer, mesh=mesh, in_specs=in_specs, out_specs=out_specs, check_vma=False)
```

```python
import jax
import jax.numpy as jnp
from jax import lax
from jax.experimental import pallas as pl
from jax.experimental.pallas import tpu as pltpu
from jax.sharding import PartitionSpec as P

EPS = 1e-6
MESH = pl.DeviceIdType.MESH
F32 = jnp.float32
BF16 = jnp.bfloat16
NZ = 4
NP = 8
A_LAG = 2
FAR = 2
X_LAG = 5
E_LAG = 3
COL = 384
DIRECT = 4


def remote(src, dst, send_sem, recv_sem, **where):
    return pltpu.make_async_remote_copy(src_ref=src, dst_ref=dst, send_sem=send_sem, recv_sem=recv_sem, device_id=where, device_id_type=MESH)


def partner(tp, k):
    if k == 1:
        return tp + 1 - 2 * lax.rem(tp, 2)
    return lax.rem(tp + 2, 4)


def pack_rows(col):
    rows = col.shape[0]
    lane = lax.broadcasted_iota(jnp.int32, (rows, 128), 1)
    row = lax.broadcasted_iota(jnp.int32, (rows, 128), 0)
    packed = jnp.sum(jnp.where(lane == row, col, 0.0), axis=0, keepdims=True)
    return jnp.broadcast_to(packed, (8, 128))


def unpack_rows(tile, rows, first=0):
    lane = lax.broadcasted_iota(jnp.int32, (rows, 128), 1)
    row = lax.broadcasted_iota(jnp.int32, (rows, 128), 0)
    wide = jnp.broadcast_to(tile[0:1], (rows, 128))
    return jnp.sum(jnp.where(lane == row + first, wide, 0.0), axis=1, keepdims=True)


def layer_kernel(hid_h, g1_h, g2_h, wq, wk, wv, wo, wg, wu, wd, kc, vc, lens_h, cos_h, sin_h,
                 out, k_out, v_out,
                 hid, g1, g2, lens, cos, sin, hid_p, len_v, rope, wbuf, wo_b, wg_b, wu_b, wd_b,
                 part, rbuf, lbuf, dbuf, x_buf, o_x, o_cat, new_kv, red, r1, s_buf, r2, h_mid, h_fin, pbuf, rbuf2, lbuf2, mbuf,
                 cum_in, cum_out, own_sq, sq_all, fac,
                 s_sem, w_sem, c_sem, b_sem, g_sem, rs, rr, ls, lr, dx_s, dx_r, sq_s, sq_r, o_s, o_r, a_s, a_r, b_s, b_r, c_s, c_r,
                 q_s, q_r, rs2, rr2, ls2, lr2, mr_s, mr_r, ml_s, ml_r, far_s):
    z = lax.axis_index('dm')
    tp = lax.axis_index('tp')
    rows, width = hid.shape
    full = width * NZ
    heads = wq.shape[0]
    hd = wq.shape[2]
    per = rows // NZ
    half = rows // 2
    side = half // 2
    slots = kc.shape[2]
    ff = wg.shape[1]
    n_pair = heads // 2
    n_a = 2 * n_pair
    n_col = ff // COL
    second = max(n_col, 9)
    n_e = second + n_col
    trip = E_LAG * (NZ - 1)
    n_grp = g_sem.shape[1]
    n_red = red.shape[1]
    rcol = width // n_red
    early = n_col * 2 // 3
    direct_from = n_e - DIRECT
    core = lax.rem(tp, 2)
    sib, across = partner(tp, 1), partner(tp, 2)
    nxt, prv = lax.rem(z + 1, NZ), lax.rem(z + NZ - 1, NZ)

    small = [pltpu.make_async_copy(a, b, s_sem.at[i]) for i, (a, b) in enumerate(((hid_h, hid), (g1_h, g1), (g2_h, g2), (cos_h, cos), (sin_h, sin), (lens_h, lens)))]
    load_o = pltpu.make_async_copy(wo, wo_b, b_sem.at[0])
    load_d = pltpu.make_async_copy(wd, wd_b, b_sem.at[1])

    def load_w(i, h):
        return pltpu.make_async_copy((wq, wk, wv)[i].at[h], wbuf.at[i, h], w_sem.at[i, h])

    def load_c(i, h):
        return pltpu.make_async_copy((kc, vc)[i].at[:, h], (k_out, v_out)[i].at[:, h], c_sem.at[i, h])

    def load(i, g):
        src, dst = ((wg, wg_b), (wu, wu_b))[i]
        cols = pl.ds(pl.multiple_of(g * COL, COL), COL)
        return pltpu.make_async_copy(src.at[:, cols], dst.at[:, cols], g_sem.at[i, g])

    for cp in small:
        cp.start()
    def load_pair(p):
        for e in range(2):
            for i in range(3):
                load_w(i, 2 * p + e).start()

    for p in range(min(n_pair, 2)):
        load_pair(p)

    sem = pltpu.get_barrier_semaphore()
    for k in range(1, NZ):
        pl.semaphore_signal(sem, inc=1, device_id={'dm': lax.rem(z + k, NZ)}, device_id_type=MESH)
    for k in (1, 2):
        pl.semaphore_signal(sem, inc=1, device_id={'tp': partner(tp, k)}, device_id_type=MESH)

    for cp in small:
        cp.wait()

    def inv(tile):
        return lax.rsqrt(tile / full + EPS)

    def local_norm(x, gain, step, lo):
        col = jnp.sum(x * x, axis=-1, keepdims=True)
        own_sq[step] = pack_rows(col)
        x_buf[lo:lo + x.shape[0]] = (x * lax.rsqrt(col / full + EPS) * gain).astype(BF16)

    def place(b, d):
        return d * per + b * NP

    x0 = hid[...].astype(F32)
    x0 = jnp.concatenate([x0[place(b, d):place(b, d) + NP] for b in range(2) for d in range(NZ)], axis=0)
    hid_p[...] = x0.astype(BF16)
    local_norm(x0, g1[...].astype(F32).reshape(1, width), 0, 0)
    cs, sn = cos[...], sin[...]
    row = lax.broadcasted_iota(jnp.int32, (2 * NP, slots), 0)
    pos = lax.broadcasted_iota(jnp.int32, (2 * NP, slots), 1)
    for b in range(2):
        part_cs, part_sn = [jnp.concatenate([t[b * NP:(b + 1) * NP]] * 2, axis=0) for t in (cs, sn)]
        rope[0, b] = jnp.concatenate([part_cs, part_cs], axis=-1)
        rope[1, b] = jnp.concatenate([-part_sn, part_sn], axis=-1)
        length = jnp.zeros((2 * NP, slots), jnp.int32)
        for r in range(NP):
            length = jnp.where((row == r) | (row == NP + r), lens[b * NP + r], length)
        len_v[b] = length

    def stat(step, way):
        return remote(cum_out.at[step, way], cum_in.at[step, way], q_s.at[step, way], q_r.at[step, way], dm=(nxt, prv)[way])

    def put_fac(i, tile, halves, first=0):
        n = len(halves) * half
        wide = jnp.broadcast_to(unpack_rows(tile, n, first), (n, 128))
        for k, b in enumerate(halves):
            for d in range(NZ):
                lo = (k * NZ + d) * NP
                fac[i, b, d] = wide[lo:lo + NP]

    def relay_stat(step, way, halves):
        has_in = (z > 0) if way == 0 else (z < NZ - 1)
        has_out = (z < NZ - 1) if way == 0 else (z > 0)

        @pl.when(has_in)
        def _():
            stat(step, way).wait_recv()

        @pl.when(jnp.logical_not(has_in))
        def _():
            cum_in[step, way] = jnp.zeros((8, 128), F32)

        before, own = cum_in[step, way], own_sq[step]
        cum = before + own
        cum_out[step, way] = cum

        @pl.when(has_out)
        def _():
            stat(step, way).start()

        scale = inv(cum)
        put_fac(2 * way, scale / inv(own), halves)
        put_fac(2 * way + 1, scale / inv(before), halves)

    @pl.when(z == 0)
    def _():
        rbuf[0] = jnp.zeros(rbuf.shape[1:], F32)

    @pl.when(z == NZ - 1)
    def _():
        lbuf[NZ - 1] = jnp.zeros(lbuf.shape[1:], F32)

    def sq_copy(src, to):
        return remote(sq_all.at[src], sq_all.at[src], sq_s.at[to], sq_r.at[src], dm=to)

    sq_all[z] = own_sq[0]
    pl.semaphore_wait(sem, NZ + 1)
    for k in (2, 1, 3):
        sq_copy(z, lax.rem(z + k, NZ)).start()

    def a_stats():
        for k in (1, 3, 2):
            sq_copy(lax.rem(z + k, NZ), lax.rem(z + k, NZ)).wait_recv()
        none = jnp.zeros((8, 128), F32)
        before, after, own = none, none, own_sq[0]
        for j in range(NZ):
            before = before + jnp.where(j < z, sq_all[j], 0.0)
            after = after + jnp.where(j > z, sq_all[j], 0.0)
        total = inv((before + own) + after)
        for i, other_side in enumerate((before, after)):
            scale = inv(other_side + own)
            put_fac(2 * i, scale / inv(own), (1,), half)
            put_fac(2 * i + 1, scale / inv(other_side), (1,), half)
            put_fac(5 + i, total / inv(other_side), (1,), half)
        put_fac(4, total / inv(own), (1,), half)
        for j in range(NZ):
            put_fac(7 + j, total / inv(sq_all[j]), (0,))

    def x_copy(src, to, p):
        return remote(part.at[to, p], dbuf.at[src, p], dx_s.at[p, to], dx_r.at[p, src], dm=to)

    def right(d, p):
        return remote(part.at[d, p], rbuf.at[d, p], rs.at[d, p], rr.at[d, p], dm=nxt)

    def left(d, p):
        return remote(part.at[d, p], lbuf.at[d, p], ls.at[d, p], lr.at[d, p], dm=prv)

    def split(it):
        b = it // n_pair
        return b, it - b * n_pair

    def o_copy(src, to, it):
        b, p = split(it)
        view = o_x.at[b, src, pl.ds(2 * p, 2)]
        return remote(view, view, o_s.at[it, to], o_r.at[it, src], dm=to)

    def repeat(f, n):
        return jnp.concatenate([f] * n, axis=1)

    def attend_x(it):
        for k in (1, 3, 2):
            x_copy(lax.rem(z + k, NZ), lax.rem(z + k, NZ), it).wait_recv()
        for e in range(2):
            load_c(0, 2 * it + e).wait()
            load_c(1, 2 * it + e).wait()
        dbuf[z, it] = part[z, it]
        terms = [dbuf[j, it] * repeat(fac[7 + j, 0, z], 6) for j in range(NZ)]
        attend(it, (terms[0] + terms[1]) + (terms[2] + terms[3]))

    def attend_y(it):
        attend(it, part[z, it] * repeat(fac[4, 1, z], 6) + (rbuf[z, it] * repeat(fac[5, 1, z], 6) + lbuf[z, it] * repeat(fac[6, 1, z], 6)))

    def attend(it, y):
        b, p = split(it)
        q, k, v_new = [jnp.concatenate([y[:, i * hd:(i + 1) * hd], y[:, (3 + i) * hd:(4 + i) * hd]], axis=0) for i in range(3)]
        cos2, sin2 = rope[0, b], rope[1, b]
        at_len = pos == len_v[b]
        seen = pos <= len_v[b]
        q = (q * cos2 + pltpu.roll(q, hd // 2, 1) * sin2).astype(BF16)
        k_new = (k * cos2 + pltpu.roll(k, hd // 2, 1) * sin2).astype(BF16).astype(F32)
        v_new = v_new.astype(BF16).astype(F32)
        s = jnp.zeros((2 * NP, slots), F32)
        for e in range(2):
            for r in range(NP):
                t = lax.dot_general(q, k_out[b * NP + r, 2 * p + e], (((1,), (1,)), ((), ())), preferred_element_type=F32)
                s = jnp.where(row == e * NP + r, t, s)
        s_new = jnp.sum(q.astype(F32) * k_new, axis=-1, keepdims=True)
        s = jnp.where(at_len, s_new, s) * (hd ** -0.5)
        s = jnp.where(seen, s, -1e30)
        ex = jnp.exp(s - jnp.max(s, axis=-1, keepdims=True))
        prob = (ex / jnp.sum(ex, axis=-1, keepdims=True)).astype(BF16).astype(F32)
        p_new = jnp.sum(jnp.where(at_len, prob, 0.0), axis=-1, keepdims=True)
        p_old = jnp.where(at_len, 0.0, prob).astype(BF16)
        acc = jnp.zeros((2 * NP, hd), F32)
        for e in range(2):
            for r in range(NP):
                t = jnp.dot(p_old, v_out[b * NP + r, 2 * p + e], preferred_element_type=F32)
                acc = jnp.where(row == e * NP + r, t, acc)
        acc = acc + p_new * v_new
        for e in range(2):
            h, at = 2 * p + e, slice(e * NP, (e + 1) * NP)
            new_kv[0, h, b] = k_new[at]
            new_kv[1, h, b] = v_new[at]
            o_x[b, z, h] = acc[at].astype(BF16)
        for k in (2, 1, 3):
            o_copy(z, lax.rem(z + k, NZ), it).start()

    where = lax.broadcasted_iota(jnp.int32, (slots, hd), 0)

    def patch(h, b):
        for r in range(NP):
            hit = where == lens[b * NP + r]
            for i, ref in enumerate((k_out, v_out)):
                fresh = jnp.broadcast_to(new_kv[i, h, b, r:r + 1, :], (slots, hd))
                ref[b * NP + r, h] = jnp.where(hit, fresh, ref[b * NP + r, h].astype(F32)).astype(BF16)

    mine = pl.ds(pl.multiple_of(core * side, side), side)
    other = pl.ds(pl.multiple_of((1 - core) * side, side), side)

    def a_copy(key, j):
        return remote(red.at[key, j, other], r1.at[key, j], a_s.at[key, j], a_r.at[key, j], tp=sib)

    def b_copy(key, j):
        return remote(s_buf.at[key, j], r2.at[key, j], b_s.at[key, j], b_r.at[key, j], tp=across)

    def c_copy(key, j, who):
        view = (h_mid, h_fin)[key // 2].at[key % 2, j, pl.ds(pl.multiple_of(who * side, side), side)]
        return remote(view, view, c_s.at[key, j], c_r.at[key, j], tp=sib)

    def o_gather(b):
        def wait(p, carry):
            it = b * n_pair + p
            for k in (1, 3, 2):
                o_copy(lax.rem(z + k, NZ), lax.rem(z + k, NZ), it).wait_recv()
            return carry

        lax.fori_loop(0, n_pair, wait, 0)
        o_cat[...] = jnp.concatenate([jnp.concatenate([o_x[b, d, h].astype(F32) for h in range(heads)], axis=1) for d in range(NZ)], axis=0).astype(BF16)

    def o_product(b, j):
        red[b, j] = jnp.dot(o_cat[...], wo_b[:, j * rcol:(j + 1) * rcol], preferred_element_type=F32)
        a_copy(b, j).start()

    def m_rows(b):
        return pl.ds(b * half, half)

    def stage_b(key):
        for j in range(n_red):
            a_copy(key, j).wait_recv()
            s_buf[key, j] = red[key, j, mine] + r1[key, j]
            b_copy(key, j).start()

    def stage_c(key):
        b = key % 2
        for j in range(n_red):
            b_copy(key, j).wait_recv()
            total = (s_buf[key, j] + r2[key, j]).astype(BF16).astype(F32)
            if key < 2:
                base = hid_p[pl.ds(pl.multiple_of(b * half + core * side, side), side), pl.ds(j * rcol, rcol)]
                h_mid[b, j, mine] = (base.astype(F32) + total).astype(BF16)
            else:
                h_fin[b, j, mine] = (h_mid[b, j, mine].astype(F32) + total).astype(BF16)
            c_copy(key, j, core).start()

    def stage_d(key):
        for j in range(n_red):
            c_copy(key, j, 1 - core).wait_recv()
        if key < 2:
            x = jnp.concatenate([h_mid[key, j].astype(F32) for j in range(n_red)], axis=1)
            local_norm(x, g2[...].astype(F32).reshape(1, width), 1 + key, key * half)

    a_end = max(n_a + max(A_LAG, FAR) * (NZ - 1), n_pair + X_LAG + 4, n_col + 7)

    def a_slot(t, carry):
        @pl.when(t + 2 < n_pair)
        def _():
            load_pair(t + 2)

        @pl.when((t >= 3) & (t < 3 + n_pair))
        def _():
            for e in range(2):
                load_c(0, 2 * (t - 3) + e).start()
                load_c(1, 2 * (t - 3) + e).start()

        @pl.when(t == 7)
        def _():
            load_o.start()

        @pl.when((t >= 7) & (t < 7 + n_col))
        def _():
            load(0, t - 7).start()
            load(1, t - 7).start()

        @pl.when(t == a_end - 1)
        def _():
            load_d.start()

        @pl.when(t < n_pair)
        def _():
            for e in range(2):
                for i in range(3):
                    load_w(i, 2 * t + e).wait()
            for e in range(2):
                h = 2 * t + e
                for i in range(3):
                    y = jnp.dot(x_buf[...], wbuf[i, h], preferred_element_type=F32)
                    for b in range(2):
                        for d in range(NZ):
                            lo = (b * NZ + d) * NP
                            part[d, b * n_pair + t, :, (3 * e + i) * hd:(3 * e + i + 1) * hd] = y[lo:lo + NP]

            for d in (3, 0, 2, 1):
                @pl.when(z != d)
                def _(d=d):
                    x_copy(z, d, t).start()

        @pl.when(t == n_pair)
        def _():
            a_stats()

        for d in (3, 2, 1):
            p = t - A_LAG * z - FAR * (NZ - 1 - d)

            @pl.when((p >= n_pair) & (p < n_a))
            def _(d=d, p=p):
                b = p // n_pair

                @pl.when((z > 0) & (z <= d))
                def _():
                    right(d, p).wait_recv()

                @pl.when((z > 0) & (z < d))
                def _():
                    part[d, p] = part[d, p] * repeat(fac[0, b, d], 6) + rbuf[d, p] * repeat(fac[1, b, d], 6)

                @pl.when(z < d)
                def _():
                    right(d, p).start()

        for d in (0, 1, 2):
            q = t - A_LAG * (NZ - 1 - z) - FAR * d

            @pl.when((q >= n_pair) & (q < n_a))
            def _(d=d, q=q):
                b = q // n_pair

                @pl.when((z < NZ - 1) & (z >= d))
                def _():
                    left(d, q).wait_recv()

                @pl.when((z < NZ - 1) & (z > d))
                def _():
                    part[d, q] = part[d, q] * repeat(fac[2, b, d], 6) + lbuf[d, q] * repeat(fac[3, b, d], 6)

                @pl.when(z > d)
                def _():
                    left(d, q).start()

        g = t - X_LAG

        @pl.when((g >= 0) & (g < n_pair))
        def _():
            attend_x(g)

        f = t - jnp.maximum(A_LAG * z + FAR * (NZ - 1 - z), A_LAG * (NZ - 1 - z) + FAR * z)

        @pl.when((f >= n_pair) & (f < n_a))
        def _():
            attend_y(f)

        o_at = n_pair - 1 + X_LAG + 2

        @pl.when(t == o_at)
        def _():
            load_o.wait()
            o_gather(0)
            for j in range(n_red):
                o_product(0, j)

        @pl.when(t == o_at + 2)
        def _():
            stage_b(0)

        return carry

    lax.fori_loop(0, a_end, a_slot, 0)

    def patch_x(h, carry):
        patch(h, 0)
        return carry

    lax.fori_loop(0, heads, patch_x, 0)
    stage_c(0)
    stage_d(0)

    def right2(c):
        return remote(pbuf.at[c, 1], rbuf2.at[c], rs2.at[c], rr2.at[c], dm=nxt)

    def left2(c):
        return remote(pbuf.at[c, 0], lbuf2.at[c], ls2.at[c], lr2.at[c], dm=prv)

    def valid(c):
        return ((c >= 0) & (c < n_col)) | ((c >= second) & (c < n_e))

    def half_of(c):
        b = c // second
        return b, c - b * second

    def m_view(c, high):
        b, k = half_of(c)
        return mbuf.at[pl.ds(pl.multiple_of(b * half + high * side, side), side), pl.ds(pl.multiple_of(k * COL, COL), COL)]

    def m_left(c):
        return remote(m_view(c, 1), m_view(c, 1), mr_s.at[c], mr_r.at[c], dm=prv)

    def m_right(c):
        return remote(m_view(c, 0), m_view(c, 0), ml_s.at[c], ml_r.at[c], dm=nxt)

    def m_far(c, high, k):
        to = (NZ - 1 - k) if high else k
        recv = mr_r if high else ml_r
        return remote(m_view(c, high), m_view(c, high), far_s.at[high, c - direct_from, k - 2], recv.at[c], dm=to)

    def gated(a):
        g, u = a[:, :COL], a[:, COL:]
        return (g * (1.0 / (1.0 + jnp.exp(-g))) * u).astype(BF16)

    def wide(i, b, first):
        f = jnp.concatenate([fac[i, b, first], fac[i, b, first + 1]], axis=0)
        return repeat(f, 2 * COL // 128)

    def finish(c, high):
        b, k = half_of(c)
        mbuf[pl.ds(pl.multiple_of(b * half + high * side, side), side), pl.ds(pl.multiple_of(k * COL, COL), COL)] = gated(pbuf[c, high])

        @pl.when(c >= direct_from)
        def _():
            m_far(c, high, 3).start()
            m_far(c, high, 2).start()

        (m_left if high else m_right)(c).start()

    def e_slot(t, carry):
        @pl.when(valid(t))
        def _():
            b, k = half_of(t)

            @pl.when(b == 0)
            def _():
                load(0, k).wait()
                load(1, k).wait()

            cols = pl.ds(pl.multiple_of(k * COL, COL), COL)
            x = x_buf[pl.ds(pl.multiple_of(b * half, half), half), :]
            g = jnp.dot(x, wg_b[:, cols], preferred_element_type=F32)
            u = jnp.dot(x, wu_b[:, cols], preferred_element_type=F32)
            for s in range(2):
                pbuf[t, s, :, 0:COL] = g[s * side:(s + 1) * side]
                pbuf[t, s, :, COL:] = u[s * side:(s + 1) * side]

        c = t - E_LAG * z
        for step, first in ((1, 0), (2, second)):
            @pl.when(c == first)
            def _(step=step):
                relay_stat(step, 0, (step - 1,))

        @pl.when(valid(c))
        def _():
            b = c // second

            @pl.when(z > 0)
            def _():
                right2(c).wait_recv()
                pbuf[c, 1] = pbuf[c, 1] * wide(0, b, 2) + rbuf2[c] * wide(1, b, 2)

            @pl.when(z < NZ - 1)
            def _():
                right2(c).start()

            @pl.when(z == NZ - 1)
            def _():
                finish(c, 1)

        d = t - E_LAG * (NZ - 1 - z)
        for step, first in ((1, 0), (2, second)):
            @pl.when(d == first)
            def _(step=step):
                relay_stat(step, 1, (step - 1,))

        @pl.when(valid(d))
        def _():
            b = d // second

            @pl.when(z < NZ - 1)
            def _():
                left2(d).wait_recv()
                pbuf[d, 0] = pbuf[d, 0] * wide(2, b, 0) + lbuf2[d] * wide(3, b, 0)

            @pl.when(z > 0)
            def _():
                left2(d).start()

            @pl.when(z == 0)
            def _():
                finish(d, 0)

        e = t - E_LAG * (2 * NZ - 2 - z)

        @pl.when(valid(e) & (z < NZ - 1))
        def _():
            m_left(e).wait_recv()

            @pl.when((z > 0) & (e < direct_from))
            def _():
                m_left(e).start()

        f = t - E_LAG * (NZ - 1 + z)

        @pl.when(valid(f) & (z > 0))
        def _():
            m_right(f).wait_recv()

            @pl.when((z < NZ - 1) & (f < direct_from))
            def _():
                m_right(f).start()

        @pl.when(t == 1)
        def _():
            o_gather(1)
            for j in range(n_red):
                o_product(1, j)

        @pl.when(t == 2)
        def _():
            stage_b(1)

        @pl.when(t == 6)
        def _():
            stage_c(1)

        @pl.when(t == 8)
        def _():
            stage_d(1)

        @pl.when((t >= n_e) & (t < n_e + heads))
        def _():
            patch(t - n_e, 1)

        down = n_col + 2 * trip
        for j in range(n_red):
            @pl.when(t == down + j)
            def _(j=j):
                if j == 0:
                    load_d.wait()
                red[2, j] = jnp.dot(mbuf[m_rows(0), :], wd_b[:, j * rcol:(j + 1) * rcol], preferred_element_type=F32)
                a_copy(2, j).start()

        @pl.when(t == down + 2)
        def _():
            stage_b(2)

        late = second + early + 2 * trip
        for j in range(n_red):
            @pl.when(t == late + j)
            def _(j=j):
                red[3, j] = jnp.dot(mbuf[m_rows(1), 0:early * COL], wd_b[0:early * COL, j * rcol:(j + 1) * rcol], preferred_element_type=F32)

        return carry

    lax.fori_loop(0, max(n_e + 2 * trip, second + early + n_red + 2 * trip, n_e + heads, n_col + 2 * trip + 3), e_slot, 0)
    for j in range(n_red):
        red[3, j] = red[3, j] + jnp.dot(mbuf[m_rows(1), early * COL:], wd_b[early * COL:, j * rcol:(j + 1) * rcol], preferred_element_type=F32)
        a_copy(3, j).start()
    stage_c(2)
    stage_b(3)
    stage_d(2)

    def drain_a(p, carry):
        for d in range(NZ):
            @pl.when((p >= n_pair) & (z < d))
            def _(d=d):
                right(d, p).wait_send()

            @pl.when((p >= n_pair) & (z > d))
            def _(d=d):
                left(d, p).wait_send()

            @pl.when((p < n_pair) & (z != d))
            def _(d=d):
                x_copy(z, d, p).wait_send()

        for k in range(1, NZ):
            o_copy(z, lax.rem(z + k, NZ), p).wait_send()
        return carry

    lax.fori_loop(0, n_a, drain_a, 0)

    def drain_e(c, carry):
        @pl.when(valid(c))
        def _():
            @pl.when(z < NZ - 1)
            def _():
                right2(c).wait_send()

            @pl.when((z == 0) | ((z < NZ - 1) & (c < direct_from)))
            def _():
                m_right(c).wait_send()

            @pl.when(z > 0)
            def _():
                left2(c).wait_send()

            @pl.when((z == NZ - 1) | ((z > 0) & (c < direct_from)))
            def _():
                m_left(c).wait_send()

            for high in range(2):
                @pl.when((c >= direct_from) & (z == (NZ - 1) * high))
                def _(high=high):
                    m_far(c, high, 2).wait_send()
                    m_far(c, high, 3).wait_send()

        return carry

    lax.fori_loop(0, n_e, drain_e, 0)
    for k in range(1, NZ):
        sq_copy(z, lax.rem(z + k, NZ)).wait_send()
    for step in (1, 2):
        @pl.when(z < NZ - 1)
        def _(step=step):
            stat(step, 0).wait_send()

        @pl.when(z > 0)
        def _(step=step):
            stat(step, 1).wait_send()

    stage_c(3)
    stage_d(3)
    for b in range(2):
        y = jnp.concatenate([h_fin[b, j].astype(F32) for j in range(n_red)], axis=1)
        if b == 0:
            ys = [y]
        else:
            ys.append(y)
    out[...] = jnp.concatenate([ys[b][d * NP:(d + 1) * NP] for d in range(NZ) for b in range(2)], axis=0).astype(BF16)
    for key in range(4):
        for j in range(n_red):
            a_copy(key, j).wait_send()
            b_copy(key, j).wait_send()
            c_copy(key, j, core).wait_send()


def layer_call(hid, g1, g2, wq, wk, wv, wo, wg, wu, wd, kc, vc, lens, cos, sin):
    rows, width = hid.shape
    heads, hd = wq.shape[0], wq.shape[2]
    slots = kc.shape[2]
    ff = wg.shape[1]
    half = rows // 2
    side = half // 2
    n_a = heads
    n_col = ff // COL
    n_e = max(n_col, 9) + n_col
    n_red = 2
    rcol = width // n_red
    hbm = pl.BlockSpec(memory_space=pl.ANY)
    vm = pl.BlockSpec(memory_space=pltpu.VMEM)
    dma = pltpu.SemaphoreType.DMA
    sums = pltpu.VMEM((NZ, n_a, NP, 6 * hd), F32)
    act = pltpu.VMEM((rows, width), BF16)
    half_red = pltpu.VMEM((4, n_red, side, rcol), F32)
    h_halves = pltpu.VMEM((2, n_red, half, rcol), BF16)
    return pl.pallas_call(
        layer_kernel,
        name='layer',
        out_shape=[pltpu.VMEM((rows, width), BF16), pltpu.VMEM(kc.shape, BF16), pltpu.VMEM(vc.shape, BF16)],
        in_specs=[hbm] * 15,
        out_specs=[vm, vm, vm],
        scratch_shapes=[
            act, pltpu.VMEM(g1.shape, g1.dtype), pltpu.VMEM(g2.shape, g2.dtype), pltpu.SMEM(lens.shape, jnp.int32), pltpu.VMEM(cos.shape, F32), pltpu.VMEM(sin.shape, F32),
            act, pltpu.VMEM((2, 2 * NP, slots), jnp.int32), pltpu.VMEM((2, 2, 2 * NP, hd), F32),
            pltpu.VMEM((3, heads, width, hd), BF16),
            pltpu.VMEM(wo.shape, BF16), pltpu.VMEM(wg.shape, BF16), pltpu.VMEM(wu.shape, BF16), pltpu.VMEM(wd.shape, BF16),
            sums, sums, sums, pltpu.VMEM((NZ, heads // 2, NP, 6 * hd), F32),
            act, pltpu.VMEM((2, NZ, heads, NP, hd), BF16), pltpu.VMEM((half, width), BF16),
            pltpu.VMEM((2, heads, 2, NP, hd), F32),
            pltpu.VMEM((4, n_red, half, rcol), F32),
            half_red, half_red, half_red,
            h_halves, h_halves,
            pltpu.VMEM((n_e, 2, side, 2 * COL), F32),
            pltpu.VMEM((n_e, side, 2 * COL), F32),
            pltpu.VMEM((n_e, side, 2 * COL), F32),
            pltpu.VMEM((rows, ff), BF16),
            pltpu.VMEM((3, 2, 8, 128), F32), pltpu.VMEM((3, 2, 8, 128), F32), pltpu.VMEM((3, 8, 128), F32), pltpu.VMEM((NZ, 8, 128), F32),
            pltpu.VMEM((7 + NZ, 2, NZ, NP, 128), F32),
            dma((6,)), dma((3, heads)), dma((2, heads)), dma((2,)), dma((2, n_col)),
            dma((NZ, n_a)), dma((NZ, n_a)), dma((NZ, n_a)), dma((NZ, n_a)),
            dma((heads // 2, NZ)), dma((heads // 2, NZ)), dma((NZ,)), dma((NZ,)),
            dma((n_a, NZ)), dma((n_a, NZ)),
            dma((4, n_red)), dma((4, n_red)), dma((4, n_red)), dma((4, n_red)), dma((4, n_red)), dma((4, n_red)),
            dma((3, 2)), dma((3, 2)),
            dma((n_e,)), dma((n_e,)), dma((n_e,)), dma((n_e,)),
            dma((n_e,)), dma((n_e,)), dma((n_e,)), dma((n_e,)),
            dma((2, DIRECT, 2)),
        ],
        compiler_params=pltpu.CompilerParams(collective_id=0, has_side_effects=True, vmem_limit_bytes=VMEM_KIB * 1024),
    )(hid, g1, g2, wq, wk, wv, wo, wg, wu, wd, kc, vc, lens, cos, sin)


VMEM_KIB = 49 * 1024


def flush_kernel(h_in, k_in, v_in, h_out, k_out, v_out, sem):
    rows = k_in.shape[0] // FLUSH
    copies = [pltpu.make_async_copy(h_in, h_out, sem.at[2, 0])]
    for i in range(FLUSH):
        at = pl.ds(i * rows, rows)
        copies.append(pltpu.make_async_copy(k_in.at[at], k_out.at[at], sem.at[0, i]))
        copies.append(pltpu.make_async_copy(v_in.at[at], v_out.at[at], sem.at[1, i]))
    for cp in copies:
        cp.start()
    for cp in copies:
        cp.wait()


def flush_call(h, k, v):
    vm = pl.BlockSpec(memory_space=pltpu.VMEM)
    hbm = pl.BlockSpec(memory_space=pl.ANY)
    return pl.pallas_call(
        flush_kernel,
        name='flush',
        out_shape=[pltpu.HBM(a.shape, a.dtype) for a in (h, k, v)],
        in_specs=[vm] * 3,
        out_specs=[hbm] * 3,
        scratch_shapes=[pltpu.SemaphoreType.DMA((3, FLUSH))],
        compiler_params=pltpu.CompilerParams(vmem_limit_bytes=2**20),
    )(h, k, v)


FLUSH = 4


def solution(mesh):
    row_spec = P('dp', 'dm')
    cache_spec = P(('dp', 'dm'), None, 'tp', None)
    batch_spec = P(('dp', 'dm'))
    rope_spec = P(('dp', 'dm'), None)
    in_specs = (row_spec, P('dm', 'tp', None), P('dm', 'tp', None), P('dm', 'tp', None), P('tp', None, 'dm'), P('dm', 'tp'), P('dm', 'tp'), P('tp', 'dm'), P('dm'), P('dm'), cache_spec, cache_spec, batch_spec, rope_spec, rope_spec)
    out_specs = (row_spec, cache_spec, cache_spec)

    def local_layer(hidden, w_q, w_k, w_v, w_o, w_gate, w_up, w_down, norm_attn, norm_mlp, k_cache, v_cache, seq_lens, rope_cos, rope_sin):
        by_head = [w.transpose(1, 0, 2) for w in (w_q, w_k, w_v)]
        caches = [c.transpose(0, 2, 1, 3) for c in (k_cache, v_cache)]
        h_out, k_out, v_out = layer_call(hidden, norm_attn, norm_mlp, *by_head, w_o.reshape(-1, w_o.shape[-1]), w_gate, w_up, w_down, *caches, seq_lens, rope_cos, rope_sin)
        h_out, k_out, v_out = flush_call(h_out, k_out, v_out)
        return h_out, k_out.transpose(0, 2, 1, 3), v_out.transpose(0, 2, 1, 3)

    return jax.shard_map(local_layer, mesh=mesh, in_specs=in_specs, out_specs=out_specs, check_vma=False)
```
